32 devices in a mesh: dp: 8 (over y, x, core), ctx: 4 (over z).
Axes of the slice: x: 2, y: 2, z: 4, core: 2. Of those that a mesh axis runs over, the one named last changes fastest.
Arguments:
- layer_in: bfloat16 [2, 8192, 768], P(None, ('dp', 'ctx')), may hold values from -6 to 6
- seg_start: int32 [2, 8192], P(None, ('dp', 'ctx')), may hold values from 0 to 964, as said below
- out_grad: bfloat16 [2, 8192, 768], P(None, ('dp', 'ctx')), may hold values from -6 to 6
- w_qkv: bfloat16 [768, 2304], P(('dp', 'ctx')), may hold values from -0.3125 to 0.3125
- w_attn_out: bfloat16 [768, 768], P(('dp', 'ctx')), may hold values from -0.75 to 0.75
- w_in: bfloat16 [768, 2304], P(('dp', 'ctx')), may hold values from -0.21875 to 0.21875
- w_mlp_out: bfloat16 [768, 1152], P(('dp', 'ctx')), may hold values from -0.1875 to 0.1875
- norm_attn: bfloat16 [768], P(('dp', 'ctx')), may hold values from 0.099609375 to 1.8984375
- norm_mlp: bfloat16 [768], P(('dp', 'ctx')), may hold values from 0.099609375 to 1.8984375
Outputs:
- layer_out: bfloat16 [2, 8192, 768], P(None, ('dp', 'ctx'))
- grad_in: bfloat16 [2, 8192, 768], P(None, ('dp', 'ctx'))
- grad_w_qkv: float32 [768, 2304], P(('dp', 'ctx'))
- grad_w_attn_out: float32 [768, 768], P(('dp', 'ctx'))
- grad_w_in: float32 [768, 2304], P(('dp', 'ctx'))
- grad_w_mlp_out: float32 [768, 1152], P(('dp', 'ctx'))
- grad_norm_attn: float32 [768], P(('dp', 'ctx'))
- grad_norm_mlp: float32 [768], P(('dp', 'ctx'))
The draws below stay inside these ranges and needn't reach their ends.
Inputs may be any that keep to these rules, and one draw needn't show every extreme that they name: `seg_start`: documents are runs of 60 to 800 tokens that tile each sequence of 1024 tokens and never cross from one sequence to the next; every token of a document carries the position within its sequence of the document's first token, so the first token of each sequence carries 0.
All inputs are finite; a program needn't handle non-finite values.
Results may differ from the reference program's by a relative error of at most 0.017.
The reference program's roundings to bfloat16 on the way count: a program that leaves them out, or rounds other values in their place, can miss the bound.
Values may be sent and summed in bfloat16 or wider, within the bound.
A program may use at most 192 MiB of HBM per device.

```python
from functools import partial
import jax
import jax.numpy as jnp
from jax import lax

D = 768
HEADS = 12
HEAD_DIM = 64
FF = 1152
MICRO = 2
DOC_MIN = 60
DOC_MAX = 800
LEN = 1024
SEQ_TOKENS = 8192
N_DP = 8


def draw_seg_start(key, part):
    sequences = SEQ_TOKENS // LEN * MICRO
    candidates = LEN // DOC_MIN + 1
    lengths = jax.random.randint(key, (sequences, candidates), DOC_MIN, DOC_MAX - DOC_MIN + 1, dtype=jnp.int32)
    doc_ends = jnp.cumsum(lengths, axis=1)
    starts = jnp.concatenate([jnp.zeros((sequences, 1), jnp.int32), doc_ends[:, :-1]], axis=1)
    usable = starts <= LEN - DOC_MIN
    positions = jnp.arange(LEN, dtype=jnp.int32)
    covering = usable[:, None, :] & (starts[:, None, :] <= positions[None, :, None])
    first_token = jnp.max(jnp.where(covering, starts[:, None, :], 0), axis=2)
    return first_token.reshape(MICRO, SEQ_TOKENS).astype(jnp.int32)


def strengthened(array, rng, source, target, blocks, factor):
    def block_of(axis_at):
        return (jnp.arange(array.shape[axis_at]) // (array.shape[axis_at] // blocks)).reshape((-1,) + (1,) * (array.ndim - 1 - axis_at))

    one_side = jax.random.permutation(rng, blocks)[block_of(target)]
    far = (block_of(target) + blocks // 2) % blocks
    return jnp.where((block_of(source) == one_side) | (block_of(source) == far), factor * array, array)


def level_of(key, shape, pieces, low, high):
    def one(dim, shards_of):
        draws = jax.random.uniform(jax.random.fold_in(jax.random.fold_in(key, 6), dim), (shards_of,), jnp.float32, low / len(pieces), high / len(pieces))
        return jnp.repeat(jnp.exp(draws), shape[dim] // shards_of).reshape((-1,) + (1,) * (len(shape) - dim - 1))

    loudness = one(*pieces[0])
    for cut in pieces[1:]:
        loudness = loudness * one(*cut)
    return loudness


def noise(rng, dims, scale, most, cuts=(), kind=jnp.bfloat16):
    result = jax.random.normal(rng, dims, jnp.float32) * scale
    if len(cuts) > 0:
        result = level_of(rng, dims, cuts, -0.22, 0.18) * result
    return jnp.clip(result, min=-most, max=most).astype(kind)


def heavy_noise(stream_key, extent, deviation, limit, shards, heavy, kind=jnp.bfloat16):
    array = deviation * jax.random.normal(stream_key, extent, jnp.float32)
    if shards:
        array = array * level_of(stream_key, extent, shards, -0.22, 0.18)
    return jnp.clip(strengthened(array, jax.random.fold_in(stream_key, 3), *heavy), -limit, limit).astype(kind)


def setup_inputs(seed: int = 0) -> dict:
    key_list = jax.random.split(jax.random.key(seed), 10)
    layer_in = noise(key_list[0], (MICRO, SEQ_TOKENS, D), 1.0, 6.0, ((1, 32),))
    seg_start = draw_seg_start(jax.random.fold_in(key_list[9], 71), 0)
    out_grad = heavy_noise(key_list[2], (MICRO, SEQ_TOKENS, D), 1.0, 6.0, ((1, 32),), (1, 2, 32, 2.75))
    w_qkv = noise(key_list[3], (D, 3 * D), (D // 2) ** -0.5, 0.3125, ((0, 32),))
    w_attn_out = noise(key_list[4], (D, D), HEAD_DIM ** -0.5, 0.75, ((0, 32),))
    w_in = noise(key_list[5], (D, 2 * FF), D ** -0.5, 0.21875, ((0, 32),))
    w_mlp_out = noise(key_list[6], (D, FF), FF ** -0.5, 0.1875, ((0, 32),))
    norm_attn = jnp.clip(1.0 + 0.18 * jax.random.normal(key_list[7], (D,), jnp.float32), 0.099609375, 1.8984375).astype(jnp.bfloat16)
    norm_mlp = jnp.clip(1.0 + 0.18 * jax.random.normal(key_list[8], (D,), jnp.float32), 0.099609375, 1.8984375).astype(jnp.bfloat16)
    return {"layer_in": layer_in, "seg_start": seg_start, "out_grad": out_grad, "w_qkv": w_qkv, "w_attn_out": w_attn_out, "w_in": w_in, "w_mlp_out": w_mlp_out, "norm_attn": norm_attn, "norm_mlp": norm_mlp}


rope_base = 160000.0
norm_eps = 1e-05
neg_large = -1e+30

@jax.custom_vjp
def low(v):
    return lax.optimization_barrier(v.astype(jnp.bfloat16)).astype(jnp.float32)

@jax.custom_vjp
def low_back(v):
    return v

def low_keep(v):
    return (low(v), None)

def low_pass(kept, grad):
    return (grad,)

def back_keep(v):
    return (v, None)

def back_low(kept, grad):
    return (low(grad),)
low.defvjp(low_keep, low_pass)
low_back.defvjp(back_keep, back_low)

def matmul(left, right):
    return jnp.dot(left, right, precision=lax.Precision.HIGHEST, preferred_element_type=jnp.float32)

def normalize(values):
    centered = values - lax.optimization_barrier(jnp.mean(values, axis=-1, keepdims=True))
    spread = lax.optimization_barrier(jnp.mean(centered * centered, axis=-1, keepdims=True))
    return centered * lax.rsqrt(spread + norm_eps)

def rope_tables(positions):
    half_dim = HEAD_DIM // 2
    frequency = rope_base ** (-(jnp.arange(half_dim).astype(jnp.float32) * 2.0) / HEAD_DIM)
    angles = positions.astype(jnp.float32)[:, None] * frequency[None, :]
    angles = jnp.concatenate([angles, angles], axis=-1)
    return (jnp.cos(angles), jnp.sin(angles))

def rotate(values, cosine_table, sine_table):
    half_dim = values.shape[-1] // 2
    turned = jnp.concatenate([-values[..., half_dim:], values[..., :half_dim]], axis=-1)
    return values * cosine_table[:, None, :] + turned * sine_table[:, None, :]

def head_attention(query_head, key_head, value_head, same_doc):
    scores = low_back(matmul(query_head, key_head.T) * HEAD_DIM ** (-0.5))
    scores = jnp.where(same_doc, scores, neg_large)
    row_max = lax.optimization_barrier(jnp.max(scores, axis=-1, keepdims=True))
    shifted = jnp.exp(scores - row_max)
    row_sum = lax.optimization_barrier(jnp.sum(shifted, axis=-1, keepdims=True))
    attn_prob = shifted / row_sum
    return matmul(low(attn_prob), value_head)

def layer_forward(hidden_in, w_qkv, w_attn_out, w_in, w_mlp_out, gain_attn, gain_mlp, doc_starts):
    positions = jnp.arange(LEN, dtype=jnp.int32) - doc_starts
    cosine_table, sine_table = rope_tables(positions)
    normed = low(normalize(hidden_in) * gain_attn)
    qkv_all = low_back(matmul(normed, w_qkv)).reshape(LEN, 3, HEADS, HEAD_DIM)
    queries = low(rotate(qkv_all[:, 0], cosine_table, sine_table))
    keys_rot = low(rotate(qkv_all[:, 1], cosine_table, sine_table))
    values_all = low(qkv_all[:, 2])
    same_doc = doc_starts[:, None] == doc_starts[None, :]
    attend = jax.checkpoint(head_attention)
    mixed_out = lax.map(lambda head_in: attend(head_in[0], head_in[1], head_in[2], same_doc), (jnp.transpose(queries, (1, 0, 2)), jnp.transpose(keys_rot, (1, 0, 2)), jnp.transpose(values_all, (1, 0, 2))))
    attended = low(low_back(jnp.transpose(mixed_out, (1, 0, 2)).reshape(LEN, D)))
    middle = hidden_in + low_back(matmul(attended, w_attn_out))
    normed_mlp = low(normalize(middle) * gain_mlp)
    projected = low_back(matmul(normed_mlp, w_in))
    gated_out = low(jax.nn.gelu(projected[:, :FF], approximate=False) * projected[:, FF:])
    return middle + low_back(matmul(gated_out, w_mlp_out.T))

def reference(layer_in, seg_start, out_grad, w_qkv, w_attn_out, w_in, w_mlp_out, norm_attn, norm_mlp):
    params = tuple((weight_arg.astype(jnp.float32) for weight_arg in (w_qkv, w_attn_out, w_in, w_mlp_out, norm_attn, norm_mlp)))
    sequences = layer_in.astype(jnp.float32).reshape(MICRO * N_DP, LEN, D)
    starts = seg_start.reshape(MICRO * N_DP, LEN).astype(jnp.int32)
    cotangents = out_grad.astype(jnp.float32).reshape(MICRO * N_DP, LEN, D)

    def one_sequence(running, sequence_in):
        hidden_seq, start_seq, cot_seq = sequence_in
        out_seq, pullback = jax.vjp(partial(layer_forward, doc_starts=start_seq), hidden_seq, *params)
        new_grads = pullback(cot_seq)
        running = tuple((running_sum + addition for running_sum, addition in zip(running, new_grads[1:])))
        return (running, (out_seq.astype(jnp.bfloat16), new_grads[0].astype(jnp.bfloat16)))
    initial = tuple((jnp.zeros(weight_arg.shape, jnp.float32) for weight_arg in params))
    totals, (outputs, grad_inputs) = lax.scan(one_sequence, initial, (sequences, starts, cotangents))
    return (outputs.reshape(MICRO, SEQ_TOKENS, D), grad_inputs.reshape(MICRO, SEQ_TOKENS, D), totals[0], totals[1], totals[2], totals[3], totals[4], totals[5])
```

```python
import functools
import jax
import jax.numpy as jnp
from jax import lax
from jax.experimental import pallas as pl
from jax.experimental.pallas import tpu as pltpu
from jax.sharding import PartitionSpec as P

MESH = pl.DeviceIdType.MESH
bf16 = jnp.bfloat16
f32 = jnp.float32

HEADS = 12
HEAD_DIM = 64
FF = 1152
rope_base = 160000.0
norm_eps = 1e-05
neg_large = -1e30

WIDTH = 3456
GATHER = [(0, 512), (512, 768), (1280, 384), (1664, 640), (2304, 512), (2816, 640)]
PAIR = 128
ATTN = 1280
IN = 1664
MLP = 2816
REDUCE = {
    "m": (2816, 640),
    "i0": (1664, 640),
    "i1": (2304, 512),
    "a": (1280, 384),
    "q2": (896, 384),
    "q1": (512, 384),
    "q0": (128, 384),
    "g": (0, 128),
}


def dims(left, right, left_at, right_at):
    return lax.dot_general(
        left, right, (((left_at,), (right_at,)), ((), ())), preferred_element_type=f32
    )


def times(left, right):
    return jnp.dot(left, right, preferred_element_type=f32)


def step_kernel(
    x_in, dy_in, seg_in, wp, freq,
    lo_out, gi_out, gp_out, land, keep,
    xs, dys, sg, h1t, wq, wa, wi, wm, gains, cosr, sinr, qk, big, probs, otb, rl, x1, h2, hid, hidp,
    dgo, dgp, dx1b, dx1bp, dot_send, dot_own, f1r, lo, gi, grad, grow, dkb, dvb,
    ra, rb, ra2, rb2, zs, zp, zm, zx, fin,
    rs_, ls_, sends,
):
    dp = lax.axis_index("dp")
    z = lax.axis_index("ctx")
    q = dp // 2
    k = lax.rem(dp, 2)
    other = 1 - k
    pn = dp + 1 - 2 * k
    xn = dp + 2 - 4 * lax.rem(dp // 2, 2)
    yn = dp + 4 - 8 * (dp // 4)
    zn = z + 1 - 2 * lax.rem(z, 2)
    zb = jnp.where(z < 2, 2, 1)
    zh = z // 2
    qx = q + 1 - 2 * lax.rem(q, 2)
    qy = q + 2 - 4 * (q // 2)
    qd = qx + 2 - 4 * (qx // 2)
    inner = jnp.logical_or(z == 1, z == 2)
    outer = jnp.logical_or(z == 0, z == 3)
    names = {}
    count = {"send": 0, "local": 0}
    drains = []

    def rsem(name):
        return rs_.at[names.setdefault(name, len(names))]

    def send(src, dst, name, dev, when=None):
        i = count["send"]
        count["send"] += 1
        copy = pltpu.make_async_remote_copy(
            src_ref=src, dst_ref=dst, send_sem=sends.at[i], recv_sem=rsem(name),
            device_id=dev, device_id_type=MESH,
        )
        if when is None:
            copy.start()
            drains.append(copy.wait_send)
        else:
            pl.when(when)(copy.start)
            drains.append(lambda: pl.when(when)(copy.wait_send))

    def local(src, dst, name):
        copy = pltpu.make_async_copy(src, dst, rsem(name))
        copy.start()
        return copy

    def arrived(ref, name):
        pltpu.make_async_copy(ref, ref, rsem(name)).wait()

    def rows(start, size):
        return pl.ds(pl.multiple_of(start, 8), size)

    def lanes(start, size):
        return pl.ds(pl.multiple_of(start, 128), size)

    barrier = pltpu.get_barrier_semaphore()
    for dz in range(1, 4):
        for kk in range(2):
            pl.semaphore_signal(
                barrier, inc=1, device_id=(2 * q + kk, lax.rem(z + dz, 4)), device_id_type=MESH
            )
    for dev in (pn, xn, yn):
        pl.semaphore_signal(barrier, inc=1, device_id=(dev, z), device_id_type=MESH)
    pl.semaphore_wait(barrier, 9)

    def zstage(u):
        o, w = GATHER[u]
        cols = pl.ds(o, w)
        dst = land.at[rows(dp * 96 + z * 24, 24), cols]
        for c in range(2):
            src = wp.at[c, :, cols]
            send(src, dst, f"z{u}", (2 * q + c, zn))
            send(src, dst, f"z{u}", (2 * q + c, zb))
            send(src, dst, f"z{u}", (pn, z), when=k != c)
            pl.when(k == c)(lambda src=src: local(src, dst, f"z{u}") and None)

    def xystage(u):
        o, w = GATHER[u]
        cols = pl.ds(o, w)
        slab = land.at[rows(q * 192, 192), cols]
        arrived(slab, f"z{u}")
        send(slab, slab, f"x{u}", (xn, z))
        send(slab, slab, f"y{u}", (yn, z))
        for j in range(2):
            part = land.at[rows((2 * q + j) * 96 + lax.rem(4 - 2 * z + 4, 4) * 24, 48), cols]
            send(part, part, f"z{u}", (dp, zn), when=inner)

    def diag(u):
        o, w = GATHER[u]
        cols = pl.ds(o, w)
        arrived(land.at[rows(qx * 192, 192), cols], f"x{u}")
        part = land.at[rows(qx * 192, 96), cols]
        send(part, part, f"dx{u}", (yn, z))
        arrived(land.at[rows(qy * 192, 192), cols], f"y{u}")
        part = land.at[rows(qy * 192 + 96, 96), cols]
        send(part, part, f"dy{u}", (xn, z))

    def done(u):
        o, w = GATHER[u]
        cols = pl.ds(o, w)
        arrived(land.at[rows(qd * 192, 96), cols], f"dx{u}")
        arrived(land.at[rows(qd * 192 + 96, 96), cols], f"dy{u}")

    def activation(src_ref, dst_ref, name):
        for m in range(2):
            to = 2 * k + m
            src = src_ref.at[m]
            dst = dst_ref.at[rows(z * 256, 256), :]
            sem = rs_.at[base[name] + lax.rem(z, 2)]
            i = count["send"]
            count["send"] += 1
            copy = pltpu.make_async_remote_copy(
                src_ref=src, dst_ref=dst, send_sem=sends.at[i], recv_sem=sem,
                device_id=(2 * q + zh, to), device_id_type=MESH,
            )
            pl.when(to != z)(copy.start)
            pl.when(to == z)(pltpu.make_async_copy(src, dst, sem).start)
            drains.append(lambda copy=copy, to=to: pl.when(to != z)(copy.wait_send))

    base = {}
    for name in ("ax", "ay", "alo", "agi"):
        base[name] = len(names)
        names[name + "0"] = len(names)
        names[name + "1"] = len(names)

    def share_activation(ref, name):
        for j in range(2):
            r = rows(k * 512 + j * 256, 256)
            arrived(ref.at[r, :], f"{name}{j}")
            send(ref.at[r, :], ref.at[r, :], f"p{name}{j}", (pn, z))

    def shared_activation(ref, name):
        for j in range(2):
            arrived(ref.at[rows(other * 512 + j * 256, 256), :], f"p{name}{j}")

    def give_back(src_ref, out_ref, name):
        m = lax.rem(z, 2)
        for j in range(2):
            to = 2 * k + j
            src = src_ref.at[pl.ds(j * 256, 256), :]
            dst = out_ref.at[m]
            sem = rs_.at[base[name] + m]
            i = count["send"]
            count["send"] += 1
            copy = pltpu.make_async_remote_copy(
                src_ref=src, dst_ref=dst, send_sem=sends.at[i], recv_sem=sem,
                device_id=(2 * q + zh, to), device_id_type=MESH,
            )
            here = jnp.logical_and(to == z, zh == k)
            away = jnp.logical_not(here)
            pl.when(away)(copy.start)
            pl.when(here)(pltpu.make_async_copy(src, dst, sem).start)
            drains.append(lambda copy=copy, away=away: pl.when(away)(copy.wait_send))

    def given_back(out_ref, name):
        for m in range(2):
            arrived(out_ref.at[m], f"{name}{m}")

    def seg_send():
        for m in range(2):
            to = 2 * k + m
            src = seg_in.at[m]
            dst = sg.at[:, lanes(z * 256, 256)]
            for c in range(2):
                i = count["send"]
                count["send"] += 1
                copy = pltpu.make_async_remote_copy(
                    src_ref=src, dst_ref=dst, send_sem=sends.at[i], recv_sem=rsem("seg"),
                    device_id=(2 * q + c, to), device_id_type=MESH,
                )
                here = jnp.logical_and(to == z, k == c)
                away = jnp.logical_not(here)
                pl.when(away)(copy.start)
                pl.when(here)(pltpu.make_async_copy(src, dst, rsem("seg")).start)
                drains.append(lambda copy=copy, away=away: pl.when(away)(copy.wait_send))

    def s1(u):
        o, w = REDUCE[u]
        cols = pl.ds(o, w)
        for slot, quarter in enumerate((qx, qd)):
            send(grad.at[rows(quarter * 192, 96), cols], ra.at[slot, :, cols], f"ra{u}", (xn, z))
        for slot, quarter in enumerate((qy, qd)):
            send(grad.at[rows(quarter * 192 + 96, 96), cols], rb.at[slot, :, cols], f"rb{u}", (yn, z))

    def s2(u):
        o, w = REDUCE[u]
        cols = pl.ds(o, w)
        arrived(ra.at[:, :, cols], f"ra{u}")
        r = rows(qy * 192, 96)
        grad[r, cols] = (grad[r, cols].astype(f32) + ra[1, :, cols].astype(f32)).astype(bf16)
        send(grad.at[r, cols], ra2.at[:, cols], f"ra2{u}", (yn, z))
        arrived(rb.at[:, :, cols], f"rb{u}")
        r2 = rows(qx * 192 + 96, 96)
        grad[r2, cols] = (grad[r2, cols].astype(f32) + rb[1, :, cols].astype(f32)).astype(bf16)
        send(grad.at[r2, cols], rb2.at[:, cols], f"rb2{u}", (xn, z))

    def s3(u):
        o, w = REDUCE[u]
        cols = pl.ds(o, w)
        arrived(ra2.at[:, cols], f"ra2{u}")
        arrived(rb2.at[:, cols], f"rb2{u}")
        for j, (one, two) in enumerate(((ra, ra2), (rb, rb2))):
            total = (
                grad[rows(q * 192 + 96 * j, 96), cols].astype(f32)
                + one[0, :, cols].astype(f32)
                + two[:, cols].astype(f32)
            )
            for at in range(4):
                zs[j, at, :, cols] = total[24 * at : 24 * at + 24].astype(bf16)
        send(zs.at[:, zn, :, cols], zp.at[:, :, cols], f"zp{u}", (dp, zn))
        far = 2 * (1 - zh)
        send(zs.at[:, pl.ds(far, 2), :, cols], zm.at[:, :, :, cols], f"zm{u}", (dp, zn), when=outer)

    def s4(u):
        o, w = REDUCE[u]
        cols = pl.ds(o, w)
        far = 2 * (1 - zh)

        @pl.when(inner)
        def _():
            arrived(zm.at[:, :, :, cols], f"zm{u}")
            for j in range(2):
                for at in range(2):
                    zs[j, far + at, :, cols] = (
                        zs[j, far + at, :, cols].astype(f32) + zm[j, at, :, cols].astype(f32)
                    ).astype(bf16)

        for at in range(2):
            send(zs.at[:, far + at, :, cols], zx.at[:, :, cols], f"zx{u}", (dp, far + at), when=inner)

    def s5(u):
        o, w = REDUCE[u]
        cols = pl.ds(o, w)
        arrived(zp.at[:, :, cols], f"zp{u}")
        arrived(zx.at[:, :, cols], f"zx{u}")
        for j in range(2):
            fin[j, :, cols] = (
                zs[j, z, :, cols].astype(f32) + zp[j, :, cols].astype(f32) + zx[j, :, cols].astype(f32)
            )
        local(fin.at[k, :, cols], gp_out.at[k, :, cols], f"fl{u}")
        send(fin.at[other, :, cols], gp_out.at[k, :, cols], f"fr{u}", (pn, z))

    def s6(u):
        o, w = REDUCE[u]
        cols = pl.ds(o, w)
        arrived(gp_out.at[k, :, cols], f"fl{u}")
        arrived(gp_out.at[other, :, cols], f"fr{u}")

    zstage(0)
    activation(x_in, xs, "ax")
    seg_send()
    zstage(1)
    xystage(0)
    share_activation(xs, "ax")
    xystage(1)
    zstage(2)
    zstage(3)
    arrived(sg, "seg")
    positions = (lax.broadcasted_iota(jnp.int32, (1, 1024), 1) - sg[...]).astype(f32)
    angles = freq[:, 0:1] * positions
    cosr[...] = jnp.cos(angles)
    sinr[...] = jnp.sin(angles)
    starts = sg[...].astype(f32)
    column = jnp.broadcast_to(starts, (128, 1024)).T

    @pl.loop(0, 8)
    def _(i):
        r = lanes(i * 128, 128)
        here = jnp.broadcast_to(sg[:, r].astype(f32), (1024, 128))
        big[:, r] = jnp.where(column == here, 0.0, neg_large)

    diag(0)
    done(0)
    local(land.at[:, pl.ds(0, 128)], gains, "cg")
    local(land.at[:, pl.ds(128, 384)], wq.at[0], "cq0")
    diag(1)
    shared_activation(xs, "ax")
    arrived(gains, "cg")
    gain_rows = gains[...].astype(f32).T
    grow[...] = gain_rows[0:8]

    @pl.loop(0, 4)
    def _(i):
        xb = xs[rows(i * 256, 256), :].astype(f32)
        c = xb - jnp.mean(xb, -1, keepdims=True)
        n = c * lax.rsqrt(jnp.mean(c * c, -1, keepdims=True) + norm_eps)
        h1t[:, lanes(i * 256, 256)] = (n * grow[0:1, :]).astype(bf16).T

    xystage(2)
    xystage(3)
    zstage(4)
    zstage(5)
    done(1)
    local(land.at[:, pl.ds(512, 384)], wq.at[1], "cq1")
    local(land.at[:, pl.ds(896, 384)], wq.at[2], "cq2")
    for p in range(3):
        arrived(wq.at[p], f"cq{p}")

    @pl.loop(0, 3)
    def _(p):
        t = times(wq[p].T, h1t[...])
        c = cosr[...]
        s = sinr[...]
        for hh in range(4):
            u1 = t[hh * 64 : hh * 64 + 32]
            u2 = t[hh * 64 + 32 : hh * 64 + 64]
            scale = HEAD_DIM**-0.5 if hh < 2 else 1.0
            qk[p, hh * 64 : hh * 64 + 32, :] = ((u1 * c - u2 * s) * scale).astype(bf16)
            qk[p, hh * 64 + 32 : hh * 64 + 64, :] = ((u2 * c + u1 * s) * scale).astype(bf16)
        qk[p, 256:384, :] = t[256:384].astype(bf16)

    activation(dy_in, dys, "ay")

    def weight_done(u):
        done(u)
        o, w = GATHER[u]
        if u == 2:
            pieces = [(land.at[:, pl.ds(o, w)], wa.at[k], None)]
        elif u == 3:
            pieces = [(land.at[:, pl.ds(o, w)], wi.at[k, :, pl.ds(0, 640)], None)]
        elif u == 4:
            pieces = [(land.at[:, pl.ds(o, w)], wi.at[k, :, pl.ds(640, 512)], None)]
        else:
            pieces = [
                (land.at[:, pl.ds(o, 640)], wm.at[:, pl.ds(0, 640)], k == 0),
                (land.at[:, pl.ds(o + 128, 512)], wm.at[:, pl.ds(640, 512)], k == 1),
            ]
        for src, dst, when in pieces:
            if when is None:
                local(src, dst, f"cw{u}")
            else:
                pl.when(when)(lambda src=src, dst=dst: local(src, dst, f"cw{u}") and None)
            send(src, dst, f"pw{u}", (pn, z), when=when)

    def weight_here(u):
        if u == 2:
            mine, theirs = [(wa.at[k], None)], [(wa.at[other], None)]
        elif u == 3:
            mine, theirs = [(wi.at[k, :, pl.ds(0, 640)], None)], [(wi.at[other, :, pl.ds(0, 640)], None)]
        elif u == 4:
            mine, theirs = [(wi.at[k, :, pl.ds(640, 512)], None)], [(wi.at[other, :, pl.ds(640, 512)], None)]
        else:
            low, high = wm.at[:, pl.ds(0, 640)], wm.at[:, pl.ds(640, 512)]
            mine, theirs = [(low, k == 0), (high, k == 1)], [(low, k == 1), (high, k == 0)]
        for group, name in ((mine, "cw"), (theirs, "pw")):
            for ref, when in group:
                if when is None:
                    arrived(ref, f"{name}{u}")
                else:
                    pl.when(when)(lambda ref=ref, name=name: arrived(ref, f"{name}{u}"))

    forward_steps = [
        lambda: (diag(2), xystage(4)),
        lambda: (diag(3), xystage(5)),
        lambda: (weight_done(2), diag(4)),
        lambda: (weight_done(3), diag(5)),
        lambda: (weight_done(4), share_activation(dys, "ay")),
        lambda: weight_done(5),
    ]

    for h in range(6):
        p, hh, slot = h // 2, h % 2, h % 2
        kt = qk[p, 128 + hh * 64 : 192 + hh * 64, :]
        vt = qk[p, 256 + hh * 64 : 320 + hh * 64, :]
        if h >= 2:
            arrived(probs.at[slot], f"e{h - 2}")
        orow = rows(k * 384 + h * 64, 64)

        @pl.loop(0, 4)
        def _(i):
            cols = lanes(i * 256, 256)
            s = dims(kt, qk[p, hh * 64 : hh * 64 + 64, cols], 0, 0) + big[:, cols]
            e = jnp.exp(s - jnp.max(s, 0, keepdims=True))
            r = 1.0 / jnp.sum(e, 0, keepdims=True)
            eb = e.astype(bf16)
            probs[slot, :, cols] = eb
            otb[orow, cols] = (times(vt, eb) * r).astype(bf16)
            rl[h : h + 1, cols] = r

        local(probs.at[slot], keep.at[h], f"e{h}")
        send(otb.at[orow, :], otb.at[orow, :], f"o{h}", (pn, z))
        forward_steps[h]()

    for u in range(2, 6):
        weight_here(u)
    for h in range(6):
        arrived(otb.at[rows(other * 384 + h * 64, 64), :], f"o{h}")
    arrived(probs.at[0], "e4")
    arrived(probs.at[1], "e5")

    mine = rows(k * 512, 512)
    theirs = rows(other * 512, 512)
    my_lanes = lanes(k * 512, 512)
    ot_mine = otb[:, my_lanes]
    x1[:, 0:384] = xs[mine, 0:384].astype(f32) + dims(ot_mine, wa[0], 0, 0)
    x1[:, 384:768] = xs[mine, 384:768].astype(f32) + dims(ot_mine, wa[1], 0, 0)
    xx = x1[...]
    c = xx - jnp.mean(xx, -1, keepdims=True)
    n = c * lax.rsqrt(jnp.mean(c * c, -1, keepdims=True) + norm_eps)
    h2[mine, :] = (n * grow[1:2, :]).astype(bf16)
    send(h2.at[mine, :], h2.at[mine, :], "h2", (pn, z))
    for o, w in ((0, 512), (512, 512), (1024, 128)):
        cols = pl.ds(o, w)
        a = times(h2[mine, :], wi[0, :, cols])
        b = times(h2[mine, :], wi[1, :, cols])
        phi = 0.5 * (1.0 + lax.erf(a * 0.7071067811865476))
        gelu = a * phi
        hid[:, cols] = (gelu * b).astype(bf16)
        big[0:512, cols] = b * (phi + a * (jnp.exp(-0.5 * a * a) * 0.3989422804014327))
        big[512:1024, cols] = gelu
    send(hid.at[:, lanes(other * 512, 640)], hidp, "hid", (pn, z))
    lo[...] = (x1[...] + dims(hid[...], wm[...], 1, 1)).astype(bf16)
    give_back(lo, lo_out, "alo")

    for o, w in ((0, 512), (512, 512), (1024, 128)):
        cols = pl.ds(o, w)
        e = times(dys[mine, :], wm[:, cols])
        dgo[0, :, cols] = (e * big[0:512, cols]).astype(bf16)
        dgo[1, :, cols] = (e * big[512:1024, cols]).astype(bf16)
    send(dgo.at[other], dgp, "dg", (pn, z))
    f2 = dims(dgo[0], wi[0], 1, 1) + dims(dgo[1], wi[1], 1, 1)
    xx = x1[...]
    c = xx - jnp.mean(xx, -1, keepdims=True)
    r2 = lax.rsqrt(jnp.mean(c * c, -1, keepdims=True) + norm_eps)
    n = c * r2
    grow[3:4, :] = jnp.sum(f2 * n, 0, keepdims=True)
    cc = f2 * grow[1:2, :]
    dx = dys[mine, :].astype(f32) + r2 * (
        cc - jnp.mean(cc, -1, keepdims=True) - n * jnp.mean(cc * n, -1, keepdims=True)
    )
    x1[...] = dx
    dx1b[...] = dx.astype(bf16)
    send(dx1b.at[:, lanes(other * 384, 384)], dx1bp, "dx1b", (pn, z))
    for part in range(2):
        which = other if part == 0 else k
        col = lanes(which * 384, 384)
        feat = rows(which * 384, 384)
        left = jnp.concatenate([wa[0, feat, :], wa[1, feat, :]], axis=1)
        t = dims(left, dx1b[...], 1, 1).astype(bf16)
        if part == 0:
            dot_send[...] = t
            send(dot_send, dot_own.at[:, my_lanes], "do", (pn, z))
        else:
            dot_own[:, my_lanes] = t
    local(keep.at[5], probs.at[1], "b5")
    local(keep.at[4], probs.at[0], "b4")

    shared_activation(dys, "ay")
    arrived(hidp, "hid")
    grad[:, MLP : MLP + 640] = (
        dims(dys[mine, :], hid[:, lanes(k * 512, 640)], 0, 0) + dims(dys[theirs, :], hidp[...], 0, 0)
    ).astype(bf16)
    s1("m")
    arrived(h2.at[theirs, :], "h2")
    arrived(dgp, "dg")
    for name, o, w in (("i0", 0, 640), ("i1", 640, 512)):
        cols = pl.ds(o, w)
        grad[:, IN + o : IN + o + w] = (
            dims(h2[mine, :], dgo[k, :, cols], 0, 0) + dims(h2[theirs, :], dgp[:, cols], 0, 0)
        ).astype(bf16)
        s1(name)
    arrived(dx1bp, "dx1b")
    grad[:, ATTN : ATTN + 384] = (
        times(otb[:, my_lanes], dx1b[:, lanes(k * 384, 384)])
        + times(otb[:, lanes(other * 512, 512)], dx1bp[...])
    ).astype(bf16)
    s1("a")
    arrived(dot_own.at[:, lanes(other * 512, 512)], "do")

    backward_steps = {
        5: lambda: (s2("m"), s2("i0")),
        4: lambda: (s3("m"), s2("i1")),
        3: lambda: (s4("m"), s3("i0"), s2("a"), s2("q2")),
        2: lambda: (s5("m"), s4("i0"), s3("i1"), s3("a")),
        1: lambda: (s5("i0"), s4("i1"), s4("a"), s3("q2"), s2("q1")),
        0: lambda: (s5("i1"), s5("a"), s4("q2"), s3("q1")),
    }
    for h in (5, 4, 3, 2, 1, 0):
        p, hh, slot = h // 2, h % 2, h % 2
        kt = qk[p, 128 + hh * 64 : 192 + hh * 64, :]
        vt = qk[p, 256 + hh * 64 : 320 + hh * 64, :]
        qr = slice(hh * 64, hh * 64 + 64)
        arrived(probs.at[slot], f"b{h}")
        dkb[...] = jnp.zeros_like(dkb)
        dvb[...] = jnp.zeros_like(dvb)

        @pl.loop(0, 4)
        def _(i):
            cols = lanes(i * 256, 256)
            do = dot_own[h * 64 : h * 64 + 64, cols].astype(f32) * rl[h : h + 1, cols]
            delta = jnp.sum(do * otb[rows(k * 384 + h * 64, 64), cols].astype(f32), 0, keepdims=True)
            dob = do.astype(bf16)
            e = probs[slot, :, cols]
            ds = (e.astype(f32) * (dims(vt, dob, 0, 0) - delta)).astype(bf16)
            dkb[...] += dims(qk[p, qr, cols], ds, 1, 1)
            dvb[...] += dims(dob, e, 1, 1)
            dq = times(kt, ds) * HEAD_DIM**-0.5
            c = cosr[:, cols]
            s = sinr[:, cols]
            qk[p, hh * 64 : hh * 64 + 32, cols] = (dq[:32] * c + dq[32:] * s).astype(bf16)
            qk[p, hh * 64 + 32 : hh * 64 + 64, cols] = (dq[32:] * c - dq[:32] * s).astype(bf16)

        if h >= 2:
            local(keep.at[h - 2], probs.at[slot], f"b{h - 2}")
        d = dkb[...]
        c = cosr[...]
        s = sinr[...]
        qk[p, 128 + hh * 64 : 160 + hh * 64, :] = (d[:32] * c + d[32:] * s).astype(bf16)
        qk[p, 160 + hh * 64 : 192 + hh * 64, :] = (d[32:] * c - d[:32] * s).astype(bf16)
        qk[p, 256 + hh * 64 : 320 + hh * 64, :] = dvb[...].astype(bf16)
        if hh == 0:
            grad[:, PAIR + 384 * p : PAIR + 384 * p + 384] = dims(h1t[...], qk[p], 1, 1).astype(bf16)
            s1(f"q{p}")
        backward_steps[h]()

    def f1_part(cols):
        return times(wq[0], qk[0, :, cols]) + times(wq[1], qk[1, :, cols]) + times(wq[2], qk[2, :, cols])

    big[0:768, 0:512] = f1_part(lanes(other * 512, 512))
    send(big.at[pl.ds(0, 768), pl.ds(0, 512)], f1r, "f1", (pn, z))
    big[0:768, 512:1024] = f1_part(my_lanes)
    s2("q0")
    s5("q2")
    s4("q1")
    arrived(f1r, "f1")
    f1 = (big[0:768, 512:1024] + f1r[...]).T
    xx = xs[mine, :].astype(f32)
    c = xx - jnp.mean(xx, -1, keepdims=True)
    r1 = lax.rsqrt(jnp.mean(c * c, -1, keepdims=True) + norm_eps)
    n = c * r1
    grow[2:3, :] = jnp.sum(f1 * n, 0, keepdims=True)
    cc = f1 * grow[0:1, :]
    gi[...] = (
        x1[...] + r1 * (cc - jnp.mean(cc, -1, keepdims=True) - n * jnp.mean(cc * n, -1, keepdims=True))
    ).astype(bf16)
    give_back(gi, gi_out, "agi")
    two = jnp.concatenate([grow[2:4, :], jnp.zeros((126, 768), f32)], axis=0)
    grad[:, 0:128] = two.T.astype(bf16)
    s1("g")
    s3("q0")
    s5("q1")
    s2("g")
    s4("q0")
    s3("g")
    s5("q0")
    s4("g")
    s5("g")
    for u in REDUCE:
        s6(u)
    given_back(lo_out, "alo")
    given_back(gi_out, "agi")
    for drain in drains:
        drain()


def pack(w_qkv, w_attn, w_in, w_mlp, g1, g2):
    r = w_qkv.shape[0]
    g = jnp.concatenate([g1[:, None], g2[:, None], jnp.zeros((r, 126), bf16)], axis=1)
    g = jnp.broadcast_to(g[None], (2, r, 128))
    qkv = w_qkv.reshape(r, 3, 2, 3, 128).transpose(2, 0, 3, 1, 4).reshape(2, r, 1152)
    a = w_attn.reshape(r, 2, 384).transpose(1, 0, 2)
    i = w_in.reshape(r, 2, 1152).transpose(1, 0, 2)
    m = jnp.stack([w_mlp[:, :640], w_mlp[:, 512:]])
    return jnp.concatenate([g, qkv, a, i, m], axis=2)


def unpack(gp):
    r = gp.shape[1]
    gains = gp[0, :, 0:2] + gp[1, :, 0:2]
    qkv = gp[:, :, 128:1280].reshape(2, r, 3, 3, 128).transpose(1, 3, 0, 2, 4).reshape(r, 2304)
    a = gp[:, :, 1280:1664].transpose(1, 0, 2).reshape(r, 768)
    i = gp[:, :, 1664:2816].transpose(1, 0, 2).reshape(r, 2304)
    m = jnp.concatenate([gp[0, :, 2816:3456], gp[1, :, 2944:3456]], axis=1)
    return qkv, a, i, m, gains[:, 0], gains[:, 1]


def fast(layer_in, seg_start, out_grad, w_qkv, w_attn_out, w_in, w_mlp_out, norm_attn, norm_mlp):
    wp = pack(w_qkv, w_attn_out, w_in, w_mlp_out, norm_attn, norm_mlp)
    frequency = rope_base ** (-(jnp.arange(32).astype(f32) * 2.0) / HEAD_DIM)
    freq = jnp.broadcast_to(frequency[:, None], (32, 128))
    hbm = pl.BlockSpec(memory_space=pltpu.HBM)
    vmem = pl.BlockSpec(memory_space=pltpu.VMEM)
    V = pltpu.VMEM
    outs = pl.pallas_call(
        step_kernel,
        name="layer",
        out_shape=[
            jax.ShapeDtypeStruct((2, 256, 768), bf16),
            jax.ShapeDtypeStruct((2, 256, 768), bf16),
            jax.ShapeDtypeStruct((2, 24, WIDTH), f32),
            jax.ShapeDtypeStruct((768, WIDTH), bf16),
            jax.ShapeDtypeStruct((6, 1024, 1024), bf16),
        ],
        in_specs=[hbm, hbm, hbm, vmem, vmem],
        out_specs=[hbm] * 5,
        scratch_shapes=[
            V((1024, 768), bf16),
            V((1024, 768), bf16),
            V((1, 1024), jnp.int32),
            V((768, 1024), bf16),
            V((3, 768, 384), bf16),
            V((2, 768, 384), bf16),
            V((2, 768, 1152), bf16),
            V((768, 1152), bf16),
            V((768, 128), bf16),
            V((32, 1024), f32),
            V((32, 1024), f32),
            V((3, 384, 1024), bf16),
            V((1024, 1152), f32),
            V((2, 1024, 1024), bf16),
            V((768, 1024), bf16),
            V((8, 1024), f32),
            V((512, 768), f32),
            V((1024, 768), bf16),
            V((512, 1152), bf16),
            V((512, 640), bf16),
            V((2, 512, 1152), bf16),
            V((512, 1152), bf16),
            V((512, 768), bf16),
            V((512, 384), bf16),
            V((384, 512), bf16),
            V((384, 1024), bf16),
            V((768, 512), f32),
            V((512, 768), bf16),
            V((512, 768), bf16),
            V((768, WIDTH), bf16),
            V((8, 768), f32),
            V((64, 1024), f32),
            V((64, 1024), f32),
            V((2, 96, WIDTH), bf16),
            V((2, 96, WIDTH), bf16),
            V((96, WIDTH), bf16),
            V((96, WIDTH), bf16),
            V((2, 4, 24, WIDTH), bf16),
            V((2, 24, WIDTH), bf16),
            V((2, 2, 24, WIDTH), bf16),
            V((2, 24, WIDTH), bf16),
            V((2, 24, WIDTH), f32),
            pltpu.SemaphoreType.DMA((160,)),
            pltpu.SemaphoreType.DMA((1,)),
            pltpu.SemaphoreType.DMA((220,)),
        ],
        compiler_params=pltpu.CompilerParams(
            collective_id=0, has_side_effects=True, vmem_limit_bytes=67043328
        ),
    )(layer_in, out_grad, seg_start[:, None, :], wp, freq)
    return (outs[0], outs[1], *unpack(outs[2]))


def normalize(values):
    centered = values - jnp.mean(values, axis=-1, keepdims=True)
    spread = jnp.mean(centered * centered, axis=-1, keepdims=True)
    return centered * lax.rsqrt(spread + norm_eps)


def rope_tables(positions):
    half_dim = HEAD_DIM // 2
    frequency = rope_base ** (-(jnp.arange(half_dim).astype(jnp.float32) * 2.0) / HEAD_DIM)
    angles = positions.astype(jnp.float32)[:, None] * frequency[None, :]
    angles = jnp.concatenate([angles, angles], axis=-1)
    return (jnp.cos(angles), jnp.sin(angles))


def turn_half(values):
    half_dim = values.shape[-1] // 2
    return jnp.concatenate([-values[..., half_dim:], values[..., :half_dim]], axis=-1)


def rotate(values, cosine_table, sine_table):
    return values * cosine_table[:, None, :] + turn_half(values) * sine_table[:, None, :]


def unrotate(values, cosine_table, sine_table):
    return values * cosine_table[:, None, :] - turn_half(values) * sine_table[:, None, :]


def product(left, right):
    return jnp.dot(left, right, preferred_element_type=jnp.float32)


def left_transposed(left, right):
    return lax.dot_general(
        left, right, (((0,), (0,)), ((), ())), preferred_element_type=jnp.float32
    )


def right_transposed(left, right):
    return lax.dot_general(
        left, right, (((1,), (1,)), ((), ())), preferred_element_type=jnp.float32
    )


def to_groups(array):
    row_count, head_count, head_size = array.shape
    return array.reshape(row_count, head_count // 4, 4, head_size).transpose(1, 0, 2, 3)


def from_groups(array):
    group_count, row_count, group_heads, head_size = array.shape
    return array.transpose(1, 0, 2, 3).reshape(row_count, group_count * group_heads, head_size)


def attend_group(group_in, same_doc):
    query_part, key_part, value_part = group_in
    scores = jnp.einsum(
        "qhd,khd->hqk", query_part, key_part, preferred_element_type=jnp.float32
    ) * HEAD_DIM ** (-0.5)
    masked = jnp.where(same_doc[None], scores, neg_large)
    highest = jnp.max(masked, axis=-1, keepdims=True)
    shifted = jnp.exp(masked - highest)
    totals = jnp.sum(shifted, axis=-1, keepdims=True)
    attn_prob = shifted / totals
    log_total = highest + jnp.log(totals)
    mixed_out = jnp.einsum(
        "hqk,khd->qhd",
        attn_prob.astype(jnp.bfloat16),
        value_part,
        preferred_element_type=jnp.float32,
    )
    return (mixed_out, log_total[..., 0])


def attend_back(group_in, same_doc):
    query_part, key_part, value_part, grad_part, log_total = group_in
    scores = jnp.einsum(
        "qhd,khd->hqk", query_part, key_part, preferred_element_type=jnp.float32
    ) * HEAD_DIM ** (-0.5)
    attn_prob = jnp.where(same_doc[None], jnp.exp(scores - log_total[..., None]), 0.0)
    grad_prob = jnp.einsum(
        "qhd,khd->hqk", grad_part, value_part, preferred_element_type=jnp.float32
    )
    inner_sum = jnp.sum(attn_prob * grad_prob, axis=-1, keepdims=True)
    grad_score = (attn_prob * (grad_prob - inner_sum)).astype(jnp.bfloat16)
    grad_query = jnp.einsum(
        "hqk,khd->qhd", grad_score, key_part, preferred_element_type=jnp.float32
    ) * HEAD_DIM ** (-0.5)
    grad_key = jnp.einsum(
        "hqk,qhd->khd", grad_score, query_part, preferred_element_type=jnp.float32
    ) * HEAD_DIM ** (-0.5)
    grad_value = jnp.einsum(
        "hqk,qhd->khd",
        attn_prob.astype(jnp.bfloat16),
        grad_part,
        preferred_element_type=jnp.float32,
    )
    return (grad_query, grad_key, grad_value)


def scaled_norm(values_in, gain_row):
    return normalize(values_in) * gain_row


def geglu(first_half, second_half):
    return jax.nn.gelu(first_half, approximate=False) * second_half


def local(layer_in, seg_start, out_grad, w_qkv, w_attn_out, w_in, w_mlp_out, norm_attn, norm_mlp):
    micro_count = layer_in.shape[0]
    span_len = layer_in.shape[1]
    model_width = layer_in.shape[2]
    ctx_rank = lax.axis_index("ctx")
    grad_sums = (
        jnp.zeros((model_width, 3 * model_width), jnp.float32),
        jnp.zeros((model_width, model_width), jnp.float32),
        jnp.zeros((model_width, 2 * FF), jnp.float32),
        jnp.zeros((model_width, FF), jnp.float32),
        jnp.zeros((model_width,), jnp.float32),
        jnp.zeros((model_width,), jnp.float32),
    )
    offsets = ctx_rank * span_len + jnp.arange(span_len, dtype=jnp.int32)
    outputs = []
    grad_inputs = []
    for micro_step in range(micro_count):
        gathered = (
            lax.all_gather(w_qkv, ("dp", "ctx"), axis=0, tiled=True),
            lax.all_gather(w_attn_out, ("dp", "ctx"), axis=0, tiled=True),
            lax.all_gather(w_in, ("dp", "ctx"), axis=0, tiled=True),
            lax.all_gather(w_mlp_out, ("dp", "ctx"), axis=0, tiled=True),
            lax.all_gather(norm_attn, ("dp", "ctx"), axis=0, tiled=True),
            lax.all_gather(norm_mlp, ("dp", "ctx"), axis=0, tiled=True),
        )
        qkv_full, attn_full, in_full, mlp_full, gain_attn, gain_mlp = gathered
        starts_here = seg_start[micro_step]
        hidden = layer_in[micro_step].astype(jnp.float32)
        cosine_table, sine_table = rope_tables(offsets - starts_here)
        normed, norm_back = jax.vjp(scaled_norm, hidden, gain_attn.astype(jnp.float32))
        normed_low = normed.astype(jnp.bfloat16)
        qkv_local = product(normed_low, qkv_full).reshape(span_len, 3, HEADS, HEAD_DIM)
        queries = rotate(qkv_local[:, 0], cosine_table, sine_table).astype(jnp.bfloat16)
        keys_here = rotate(qkv_local[:, 1], cosine_table, sine_table).astype(jnp.bfloat16)
        values_here = qkv_local[:, 2].astype(jnp.bfloat16)
        keys_all, values_all, starts_all = (
            lax.all_gather(keys_here, "ctx", axis=0, tiled=True),
            lax.all_gather(values_here, "ctx", axis=0, tiled=True),
            lax.all_gather(starts_here, "ctx", axis=0, tiled=True),
        )
        same_doc = starts_here[:, None] == starts_all[None, :]
        query_groups = to_groups(queries)
        key_groups = to_groups(keys_all)
        value_groups = to_groups(values_all)
        mixed_out, log_total = lax.map(
            lambda group_in: attend_group(group_in, same_doc),
            (query_groups, key_groups, value_groups),
        )
        attended = from_groups(mixed_out).reshape(span_len, model_width).astype(jnp.bfloat16)
        middle = hidden + product(attended, attn_full)
        normed_mlp, norm_mlp_back = jax.vjp(scaled_norm, middle, gain_mlp.astype(jnp.float32))
        normed_mlp_low = normed_mlp.astype(jnp.bfloat16)
        projected = product(normed_mlp_low, in_full)
        gated_out, geglu_back = jax.vjp(geglu, projected[:, :FF], projected[:, FF:])
        gated_low = gated_out.astype(jnp.bfloat16)
        result = middle + right_transposed(gated_low, mlp_full)
        outputs.append(result.astype(jnp.bfloat16))
        qkv_full, attn_full, in_full, mlp_full = (
            lax.all_gather(w_qkv, ("dp", "ctx"), axis=0, tiled=True),
            lax.all_gather(w_attn_out, ("dp", "ctx"), axis=0, tiled=True),
            lax.all_gather(w_in, ("dp", "ctx"), axis=0, tiled=True),
            lax.all_gather(w_mlp_out, ("dp", "ctx"), axis=0, tiled=True),
        )
        grad_out = out_grad[micro_step].astype(jnp.float32)
        grad_out_low = out_grad[micro_step]
        grad_mlp_weight = left_transposed(grad_out_low, gated_low)
        grad_gated = product(grad_out_low, mlp_full)
        grad_first, grad_second = geglu_back(grad_gated)
        grad_projected = jnp.concatenate([grad_first, grad_second], axis=1).astype(jnp.bfloat16)
        grad_in_weight = left_transposed(normed_mlp_low, grad_projected)
        grad_normed_mlp = right_transposed(grad_projected, in_full)
        grad_middle_norm, grad_gain_mlp = norm_mlp_back(grad_normed_mlp)
        grad_middle = grad_out + grad_middle_norm
        grad_middle_low = grad_middle.astype(jnp.bfloat16)
        grad_attn_weight = left_transposed(attended, grad_middle_low)
        grad_attended = (
            right_transposed(grad_middle_low, attn_full)
            .astype(jnp.bfloat16)
            .reshape(span_len, HEADS, HEAD_DIM)
        )
        grad_groups = to_groups(grad_attended)
        grad_query_groups, grad_key_groups, grad_value_groups = lax.map(
            lambda group_in: attend_back(group_in, same_doc),
            (query_groups, key_groups, value_groups, grad_groups, log_total),
        )
        keys_total = keys_all.shape[0]
        grad_keys, grad_values = (
            lax.psum_scatter(
                from_groups(grad_key_groups).reshape(keys_total, model_width).astype(jnp.bfloat16),
                "ctx",
                scatter_dimension=0,
                tiled=True,
            ).astype(jnp.float32),
            lax.psum_scatter(
                from_groups(grad_value_groups)
                .reshape(keys_total, model_width)
                .astype(jnp.bfloat16),
                "ctx",
                scatter_dimension=0,
                tiled=True,
            ).astype(jnp.float32),
        )
        grad_qkv = jnp.stack(
            [
                unrotate(from_groups(grad_query_groups), cosine_table, sine_table),
                unrotate(grad_keys.reshape(span_len, HEADS, HEAD_DIM), cosine_table, sine_table),
                grad_values.reshape(span_len, HEADS, HEAD_DIM),
            ],
            axis=1,
        )
        grad_qkv = grad_qkv.reshape(span_len, 3 * model_width).astype(jnp.bfloat16)
        grad_qkv_weight = left_transposed(normed_low, grad_qkv)
        grad_normed = right_transposed(grad_qkv, qkv_full)
        grad_hidden_norm, grad_gain_attn = norm_back(grad_normed)
        grad_inputs.append((grad_middle + grad_hidden_norm).astype(jnp.bfloat16))
        grad_sums = (
            grad_sums[0] + grad_qkv_weight,
            grad_sums[1] + grad_attn_weight,
            grad_sums[2] + grad_in_weight,
            grad_sums[3] + grad_mlp_weight,
            grad_sums[4] + grad_gain_attn,
            grad_sums[5] + grad_gain_mlp,
        )
    shares = (
        lax.psum_scatter(grad_sums[0], ("dp", "ctx"), scatter_dimension=0, tiled=True),
        lax.psum_scatter(grad_sums[1], ("dp", "ctx"), scatter_dimension=0, tiled=True),
        lax.psum_scatter(grad_sums[2], ("dp", "ctx"), scatter_dimension=0, tiled=True),
        lax.psum_scatter(grad_sums[3], ("dp", "ctx"), scatter_dimension=0, tiled=True),
        lax.psum_scatter(grad_sums[4], ("dp", "ctx"), scatter_dimension=0, tiled=True),
        lax.psum_scatter(grad_sums[5], ("dp", "ctx"), scatter_dimension=0, tiled=True),
    )
    return (
        jnp.stack(outputs),
        jnp.stack(grad_inputs),
        shares[0],
        shares[1],
        shares[2],
        shares[3],
        shares[4],
        shares[5],
    )


def solution(mesh):
    A = P(None, ("dp", "ctx"), None)
    S = P(None, ("dp", "ctx"))
    W = P(("dp", "ctx"), None)
    G = P(("dp", "ctx"))
    return jax.shard_map(
        fast if dict(mesh.shape) == {"dp": 8, "ctx": 4} else local,
        mesh=mesh,
        in_specs=(A, S, A, W, W, W, W, G, G),
        out_specs=(A, A, W, W, W, W, G, G),
        check_vma=False,
    )
```

```python
import contextlib

import jax
import jax.numpy as jnp
import numpy as np
from jax import lax
from jax.experimental import pallas as pl
from jax.experimental.pallas import tpu as pltpu
from jax.sharding import PartitionSpec as P

MESH = pl.DeviceIdType.MESH
bf16 = jnp.bfloat16
f32 = jnp.float32

HEADS = 12
HEAD_DIM = 64
FF = 1152
rope_base = 160000.0
norm_eps = 1e-05
neg_large = -1e30

WIDTH = 3456
GATHER = [(0, 512), (512, 768), (1280, 384), (1664, 640), (2304, 512), (2816, 640)]
PAIR = 128
ATTN = 1280
IN = 1664
MLP = 2816
REDUCE = {
    "m": (2816, 640),
    "i0": (1664, 640),
    "i1": (2304, 512),
    "a": (1280, 384),
    "q2": (896, 384),
    "q1": (512, 384),
    "q0": (128, 384),
    "g": (0, 128),
}


TRACE = False


def scope(name):
    return jax.named_scope(name) if TRACE else contextlib.nullcontext()


def scoped(fn):
    def inner(*args):
        with scope(f"{fn.__name__}_{args[0] if args and isinstance(args[0], (int, str)) else ''}"):
            return fn(*args)

    return inner


def dims(left, right, left_at, right_at):
    return lax.dot_general(
        left, right, (((left_at,), (right_at,)), ((), ())), preferred_element_type=f32
    )


def times(left, right):
    return jnp.dot(left, right, preferred_element_type=f32)


def step_kernel(
    x_in, dy_in, seg_in, w_qkv, w_attn, w_in, w_mlp, g_attn, g_mlp, freq,
    lo_out, gi_out, gp_out, land, keep,
    wp, gcol,
    xs, dys, sg, h1t, wq, wa, wi, wm, gains, cosr, sinr, qk, big, probs, otb, rl, x1, h2, hid, hidp,
    dgo, dgp, dx1b, dx1bp, dot_send, dot_own, f1r, lo, gi, grad, grow, dkb, dvb,
    ra, rb, ra2, rb2, zs, zp, zm, zx, fin,
    rs_, ls_, sends,
):
    dp = lax.axis_index("dp")
    z = lax.axis_index("ctx")
    q = dp // 2
    k = lax.rem(dp, 2)
    other = 1 - k
    pn = dp + 1 - 2 * k
    xn = dp + 2 - 4 * lax.rem(dp // 2, 2)
    yn = dp + 4 - 8 * (dp // 4)
    zn = z + 1 - 2 * lax.rem(z, 2)
    zb = jnp.where(z < 2, 2, 1)
    zh = z // 2
    qx = q + 1 - 2 * lax.rem(q, 2)
    qy = q + 2 - 4 * (q // 2)
    qd = qx + 2 - 4 * (qx // 2)
    inner = jnp.logical_or(z == 1, z == 2)
    outer = jnp.logical_or(z == 0, z == 3)
    names = {}
    count = {"send": 0, "local": 0}
    drains = []

    def rsem(name):
        return rs_.at[names.setdefault(name, len(names))]

    def still(view):
        index = view.transforms[0].indices
        return view.ref.at[tuple(pl.ds(0, at.size) if hasattr(at, "size") else 0 for at in index)]

    def send(src, dst, name, dev, when=None, sem=None):
        i = count["send"]
        count["send"] += 1
        copy = pltpu.make_async_remote_copy(
            src_ref=src, dst_ref=dst, send_sem=sends.at[i], recv_sem=rsem(name) if sem is None else sem,
            device_id=dev, device_id_type=MESH,
        )
        if when is None:
            copy.start()
        else:
            pl.when(when())(copy.start)
        drains.append((i, src, when))

    def drain_all():
        for i, src, when in drains:
            view = still(src) if hasattr(src, "transforms") else src

            def wait(view=view, i=i):
                pltpu.make_async_copy(view, view, sends.at[i]).wait()

            if when is None:
                wait()
            else:
                pl.when(when())(wait)

    def local(src, dst, name):
        copy = pltpu.make_async_copy(src, dst, rsem(name))
        copy.start()
        return copy

    def arrived(ref, name):
        pltpu.make_async_copy(ref, ref, rsem(name)).wait()

    def rows(start, size):
        return pl.ds(pl.multiple_of(start, 8), size)

    def lanes(start, size):
        return pl.ds(pl.multiple_of(start, 128), size)

    barrier = pltpu.get_barrier_semaphore()
    for dz in range(1, 4):
        for kk in range(2):
            pl.semaphore_signal(
                barrier, inc=1, device_id=(2 * q + kk, lax.rem(z + dz, 4)), device_id_type=MESH
            )
    for dev in (pn, xn, yn):
        pl.semaphore_signal(barrier, inc=1, device_id=(dev, z), device_id_type=MESH)

    packs = []
    for c in range(2):
        for p in range(3):
            for t in range(3):
                packs.append((w_qkv, 768 * t + 384 * c + 128 * p, c, PAIR + 384 * p + 128 * t, 128))
        packs.append((w_attn, 384 * c, c, ATTN, 384))
        packs.append((w_in, 1152 * c, c, IN, 1152))
        packs.append((w_mlp, 512 * c, c, MLP, 640))
    packing = [
        pltpu.make_async_copy(w.at[:, pl.ds(o, n)], wp.at[c, :, pl.ds(at, n)], ls_.at[i])
        for i, (w, o, c, at, n) in enumerate(packs)
    ]
    for copy in packing:
        copy.start()
    gcol[...] = jnp.zeros_like(gcol)
    gcol[0:1, 0:24] = g_attn[...].astype(f32)
    gcol[1:2, 0:24] = g_mlp[...].astype(f32)
    columns = jnp.concatenate([gcol[...], jnp.zeros((120, 128), f32)], axis=0).T[0:24].astype(bf16)
    wp[0, :, 0:128] = columns
    wp[1, :, 0:128] = columns

    @scoped
    def zstage(u):
        o, w = GATHER[u]
        cols = pl.ds(o, w)
        dst = land.at[rows(dp * 96 + z * 24, 24), cols]
        for c in range(2):
            src = wp.at[c, :, cols]
            send(src, dst, f"z{u}", (2 * q + c, zn))
            send(src, dst, f"z{u}", (2 * q + c, zb))
            send(src, dst, f"z{u}", (pn, z), when=lambda c=c: k != c)
            pl.when(k == c)(lambda src=src: local(src, dst, f"z{u}") and None)

    @scoped
    def xystage(u):
        o, w = GATHER[u]
        cols = pl.ds(o, w)
        slab = land.at[rows(q * 192, 192), cols]
        arrived(slab, f"z{u}")
        send(slab, slab, f"x{u}", (xn, z))
        send(slab, slab, f"y{u}", (yn, z))
        for j in range(2):
            part = land.at[rows((2 * q + j) * 96 + lax.rem(4 - 2 * z + 4, 4) * 24, 48), cols]
            send(part, part, f"z{u}", (dp, zn), when=lambda: inner)

    @scoped
    def diag(u):
        o, w = GATHER[u]
        cols = pl.ds(o, w)
        arrived(land.at[rows(qx * 192, 192), cols], f"x{u}")
        part = land.at[rows(qx * 192, 96), cols]
        send(part, part, f"dx{u}", (yn, z))
        arrived(land.at[rows(qy * 192, 192), cols], f"y{u}")
        part = land.at[rows(qy * 192 + 96, 96), cols]
        send(part, part, f"dy{u}", (xn, z))

    @scoped
    def done(u):
        o, w = GATHER[u]
        cols = pl.ds(o, w)
        arrived(land.at[rows(qd * 192, 96), cols], f"dx{u}")
        arrived(land.at[rows(qd * 192 + 96, 96), cols], f"dy{u}")

    def activation(src_ref, dst_ref, name, turn=None):
        for m in range(2):
            src = src_ref.at[m]
            dst = dst_ref.at[rows(z * 256, 256), :]
            sem = rs_.at[base[name] + lax.rem(z, 2)]

            def away(m=m):
                there = 2 * k + m != z
                return there if turn is None else jnp.logical_and(turn, there)

            here = 2 * k + m == z
            if turn is not None:
                here = jnp.logical_and(turn, here)
            send(src, dst, None, (2 * q + zh, 2 * k + m), when=away, sem=sem)
            pl.when(here)(pltpu.make_async_copy(src, dst, sem).start)

    base = {}
    for name in ("ax", "ay", "alo", "agi"):
        base[name] = len(names)
        names[name + "0"] = len(names)
        names[name + "1"] = len(names)

    @scoped
    def share_activation(ref, name):
        for j in range(2):
            r = rows(k * 512 + j * 256, 256)
            arrived(ref.at[r, :], f"{name}{j}")
            send(ref.at[r, :], ref.at[r, :], f"p{name}{j}", (pn, z))

    @scoped
    def shared_activation(ref, name):
        for j in range(2):
            arrived(ref.at[rows(other * 512 + j * 256, 256), :], f"p{name}{j}")

    @scoped
    def give_back(src_ref, out_ref, name, blocks=(0, 1)):
        m = lax.rem(z, 2)
        for j in blocks:
            src = src_ref.at[pl.ds(j * 256, 256), :]
            dst = out_ref.at[m]
            sem = rs_.at[base[name] + m]

            def away(j=j):
                return jnp.logical_or(2 * k + j != z, zh != k)

            send(src, dst, None, (2 * q + zh, 2 * k + j), when=away, sem=sem)
            pl.when(jnp.logical_not(away()))(pltpu.make_async_copy(src, dst, sem).start)

    @scoped
    def given_back(out_ref, name):
        for m in range(2):
            arrived(out_ref.at[m], f"{name}{m}")

    def seg_send():
        for m in range(2):
            src = seg_in.at[pl.ds(m, 1), :]
            dst = sg.at[:, lanes(z * 256, 256)]
            for c in range(2):

                def away(m=m, c=c):
                    return jnp.logical_or(2 * k + m != z, k != c)

                send(src, dst, "seg", (2 * q + c, 2 * k + m), when=away)
                pl.when(jnp.logical_not(away()))(pltpu.make_async_copy(src, dst, rsem("seg")).start)

    @scoped
    def s1(u):
        o, w = REDUCE[u]
        cols = pl.ds(o, w)
        for slot, quarter in enumerate((qx, qd)):
            send(grad.at[rows(quarter * 192, 96), cols], ra.at[slot, :, cols], f"ra{u}", (xn, z))
        for slot, quarter in enumerate((qy, qd)):
            send(grad.at[rows(quarter * 192 + 96, 96), cols], rb.at[slot, :, cols], f"rb{u}", (yn, z))

    @scoped
    def s2(u):
        o, w = REDUCE[u]
        cols = pl.ds(o, w)
        arrived(ra.at[:, :, cols], f"ra{u}")
        r = rows(qy * 192, 96)
        grad[r, cols] = (grad[r, cols].astype(f32) + ra[1, :, cols].astype(f32)).astype(bf16)
        send(grad.at[r, cols], ra2.at[:, cols], f"ra2{u}", (yn, z))
        arrived(rb.at[:, :, cols], f"rb{u}")
        r2 = rows(qx * 192 + 96, 96)
        grad[r2, cols] = (grad[r2, cols].astype(f32) + rb[1, :, cols].astype(f32)).astype(bf16)
        send(grad.at[r2, cols], rb2.at[:, cols], f"rb2{u}", (xn, z))

    @scoped
    def s3(u):
        o, w = REDUCE[u]
        cols = pl.ds(o, w)
        arrived(ra2.at[:, cols], f"ra2{u}")
        arrived(rb2.at[:, cols], f"rb2{u}")
        for j, (one, two) in enumerate(((ra, ra2), (rb, rb2))):
            total = (
                grad[rows(q * 192 + 96 * j, 96), cols].astype(f32)
                + one[0, :, cols].astype(f32)
                + two[:, cols].astype(f32)
            )
            for at in range(4):
                zs[j, at, :, cols] = total[24 * at : 24 * at + 24].astype(bf16)
        send(zs.at[:, zn, :, cols], zp.at[:, :, cols], f"zp{u}", (dp, zn))
        far = 2 * (1 - zh)
        send(zs.at[:, pl.ds(far, 2), :, cols], zm.at[:, :, :, cols], f"zm{u}", (dp, zn), when=lambda: outer)

    @scoped
    def s4(u):
        o, w = REDUCE[u]
        cols = pl.ds(o, w)
        far = 2 * (1 - zh)

        @pl.when(inner)
        def _():
            arrived(zm.at[:, :, :, cols], f"zm{u}")
            for j in range(2):
                for at in range(2):
                    zs[j, far + at, :, cols] = (
                        zs[j, far + at, :, cols].astype(f32) + zm[j, at, :, cols].astype(f32)
                    ).astype(bf16)

        for at in range(2):
            send(zs.at[:, far + at, :, cols], zx.at[:, :, cols], f"zx{u}", (dp, far + at), when=lambda: inner)

    @scoped
    def s5(u):
        o, w = REDUCE[u]
        cols = pl.ds(o, w)
        arrived(zp.at[:, :, cols], f"zp{u}")
        arrived(zx.at[:, :, cols], f"zx{u}")
        for j in range(2):
            fin[j, :, cols] = (
                zs[j, z, :, cols].astype(f32) + zp[j, :, cols].astype(f32) + zx[j, :, cols].astype(f32)
            )
        local(fin.at[k, :, cols], gp_out.at[k, :, cols], f"fl{u}")
        send(fin.at[other, :, cols], gp_out.at[k, :, cols], f"fr{u}", (pn, z))

    @scoped
    def s6(u):
        o, w = REDUCE[u]
        cols = pl.ds(o, w)
        arrived(gp_out.at[k, :, cols], f"fl{u}")
        arrived(gp_out.at[other, :, cols], f"fr{u}")

    pl.semaphore_wait(barrier, 9)

    for copy in packing:
        copy.wait()
    for u in range(6):
        zstage(u)
    seg_send()
    activation(x_in, xs, "ax", outer)
    xystage(0)
    xystage(1)
    xystage(2)
    activation(x_in, xs, "ax", inner)
    arrived(sg, "seg")
    positions = (lax.broadcasted_iota(jnp.int32, (1, 1024), 1) - sg[...]).astype(f32)
    angles = freq[:, 0:1] * positions
    cosr[...] = jnp.cos(angles)
    sinr[...] = jnp.sin(angles)
    starts = sg[...].astype(f32)
    column = jnp.broadcast_to(starts, (128, 1024)).T

    @pl.loop(0, 8)
    def _(i):
        r = lanes(i * 128, 128)
        here = jnp.broadcast_to(sg[:, r].astype(f32), (1024, 128))
        big[:, r] = jnp.where(column == here, 0.0, neg_large)

    diag(0)
    xystage(3)
    diag(1)
    xystage(4)
    share_activation(xs, "ax")
    done(0)
    local(land.at[:, pl.ds(0, 128)], gains, "cg")
    local(land.at[:, pl.ds(128, 384)], wq.at[0], "cq0")
    arrived(gains, "cg")
    gain_rows = gains[...].astype(f32).T
    grow[...] = gain_rows[0:8]
    shared_activation(xs, "ax")

    with scope("ln1"):
        @pl.loop(0, 4)
        def _(i):
            xb = xs[rows(i * 256, 256), :].astype(f32)
            c = xb - jnp.mean(xb, -1, keepdims=True)
            n = c * lax.rsqrt(jnp.mean(c * c, -1, keepdims=True) + norm_eps)
            h1t[:, lanes(i * 256, 256)] = (n * grow[0:1, :]).astype(bf16).T

    done(1)
    local(land.at[:, pl.ds(512, 384)], wq.at[1], "cq1")
    local(land.at[:, pl.ds(896, 384)], wq.at[2], "cq2")
    for p in range(3):
        arrived(wq.at[p], f"cq{p}")

    @pl.loop(0, 3)
    def _(p):
        t = times(wq[p].T, h1t[...])
        c = cosr[...]
        s = sinr[...]
        for hh in range(4):
            u1 = t[hh * 64 : hh * 64 + 32]
            u2 = t[hh * 64 + 32 : hh * 64 + 64]
            scale = HEAD_DIM**-0.5 if hh < 2 else 1.0
            qk[p, hh * 64 : hh * 64 + 32, :] = ((u1 * c - u2 * s) * scale).astype(bf16)
            qk[p, hh * 64 + 32 : hh * 64 + 64, :] = ((u2 * c + u1 * s) * scale).astype(bf16)
        qk[p, 256:384, :] = t[256:384].astype(bf16)

        @pl.when(p == 1)
        def _():
            xystage(5)
            activation(dy_in, dys, "ay")
            diag(2)
            diag(3)

    @scoped
    def weight_done(u):
        done(u)
        o, w = GATHER[u]
        if u == 2:
            pieces = [(land.at[:, pl.ds(o, w)], wa.at[k], None)]
        elif u == 3:
            pieces = [(land.at[:, pl.ds(o, w)], wi.at[k, :, pl.ds(0, 640)], None)]
        elif u == 4:
            pieces = [(land.at[:, pl.ds(o, w)], wi.at[k, :, pl.ds(640, 512)], None)]
        else:
            pieces = [
                (land.at[:, pl.ds(o, 640)], wm.at[:, pl.ds(0, 640)], lambda: k == 0),
                (land.at[:, pl.ds(o + 128, 512)], wm.at[:, pl.ds(640, 512)], lambda: k == 1),
            ]
        for src, dst, when in pieces:
            if when is None:
                local(src, dst, f"cw{u}")
            else:
                pl.when(when())(lambda src=src, dst=dst: local(src, dst, f"cw{u}") and None)
            send(src, dst, f"pw{u}", (pn, z), when=when)

    @scoped
    def weight_here(u):
        if u == 2:
            mine, theirs = [(wa.at[k], None)], [(wa.at[other], None)]
        elif u == 3:
            mine, theirs = [(wi.at[k, :, pl.ds(0, 640)], None)], [(wi.at[other, :, pl.ds(0, 640)], None)]
        elif u == 4:
            mine, theirs = [(wi.at[k, :, pl.ds(640, 512)], None)], [(wi.at[other, :, pl.ds(640, 512)], None)]
        else:
            low, high = wm.at[:, pl.ds(0, 640)], wm.at[:, pl.ds(640, 512)]
            mine, theirs = [(low, k == 0), (high, k == 1)], [(low, k == 1), (high, k == 0)]
        for group, name in ((mine, "cw"), (theirs, "pw")):
            for ref, when in group:
                if when is None:
                    arrived(ref, f"{name}{u}")
                else:
                    pl.when(when)(lambda ref=ref, name=name: arrived(ref, f"{name}{u}"))

    for h in range(6):
        rsem(f"e{h}")
        rsem(f"o{h}")
    first_send = count["send"]
    count["send"] += 6
    forward_steps = {
        0: lambda: diag(4),
        1: lambda: (weight_done(2), diag(5)),
        2: lambda: weight_done(3),
        3: lambda: weight_done(4),
        4: lambda: weight_done(5),
    }

    @pl.loop(0, 6)
    def _(h):
        p, hh = h // 2, lax.rem(h, 2)
        qrow, krow, vrow = (rows(at + hh * 64, 64) for at in (0, 128, 256))
        orow = rows(k * 384 + h * 64, 64)

        @pl.when(h >= 2)
        def _():
            pltpu.make_async_copy(probs.at[hh], keep.at[h - 2], rs_.at[names["e0"] + 2 * (h - 2)]).wait()

        s = dims(qk[p, krow, :], qk[p, qrow, :], 0, 0) + big[:, 0:1024]
        e = jnp.exp(s - jnp.max(s, 0, keepdims=True))
        r = 1.0 / jnp.sum(e, 0, keepdims=True)
        eb = e.astype(bf16)
        probs[hh] = eb
        otb[orow, :] = (times(qk[p, vrow, :], eb) * r).astype(bf16)
        rl[pl.ds(h, 1), :] = r
        pltpu.make_async_copy(probs.at[hh], keep.at[h], rs_.at[names["e0"] + 2 * h]).start()
        pltpu.make_async_remote_copy(
            src_ref=otb.at[orow, :], dst_ref=otb.at[orow, :], send_sem=sends.at[first_send + h],
            recv_sem=rs_.at[names["o0"] + 2 * h], device_id=(pn, z), device_id_type=MESH,
        ).start()
        for at, step in forward_steps.items():
            pl.when(h == at)(lambda step=step: step() and None)

    for h in range(6):
        drains.append((first_send + h, otb.at[pl.ds(0, 64), :], None))

    for u in range(2, 6):
        weight_here(u)
    for h in range(6):
        arrived(otb.at[rows(other * 384 + h * 64, 64), :], f"o{h}")
    arrived(probs.at[0], "e4")
    arrived(probs.at[1], "e5")

    mine = rows(k * 512, 512)
    theirs = rows(other * 512, 512)
    my_lanes = lanes(k * 512, 512)
    ot_mine = otb[:, my_lanes]
    x1[:, 0:384] = xs[mine, 0:384].astype(f32) + dims(ot_mine, wa[0], 0, 0)
    x1[:, 384:768] = xs[mine, 384:768].astype(f32) + dims(ot_mine, wa[1], 0, 0)
    xx = x1[...]
    c = xx - jnp.mean(xx, -1, keepdims=True)
    n = c * lax.rsqrt(jnp.mean(c * c, -1, keepdims=True) + norm_eps)
    h2[mine, :] = (n * grow[1:2, :]).astype(bf16)
    send(h2.at[mine, :], h2.at[mine, :], "h2", (pn, z))
    for o, w in ((0, 512), (512, 512), (1024, 128)):
        cols = pl.ds(o, w)
        a = times(h2[mine, :], wi[0, :, cols])
        b = times(h2[mine, :], wi[1, :, cols])
        phi = 0.5 * (1.0 + lax.erf(a * 0.7071067811865476))
        gelu = a * phi
        hid[:, cols] = (gelu * b).astype(bf16)
        big[0:512, cols] = b * (phi + a * (jnp.exp(-0.5 * a * a) * 0.3989422804014327))
        big[512:1024, cols] = gelu
    send(hid.at[:, lanes(other * 512, 640)], hidp, "hid", (pn, z))
    lo[...] = (x1[...] + dims(hid[...], wm[...], 1, 1)).astype(bf16)
    give_back(lo, lo_out, "alo")

    share_activation(dys, "ay")
    shared_activation(dys, "ay")
    arrived(hidp, "hid")
    grad[:, MLP : MLP + 640] = (
        dims(dys[mine, :], hid[:, lanes(k * 512, 640)], 0, 0) + dims(dys[theirs, :], hidp[...], 0, 0)
    ).astype(bf16)
    s1("m")
    for o, w in ((0, 512), (512, 512), (1024, 128)):
        cols = pl.ds(o, w)
        e = times(dys[mine, :], wm[:, cols])
        dgo[0, :, cols] = (e * big[0:512, cols]).astype(bf16)
        dgo[1, :, cols] = (e * big[512:1024, cols]).astype(bf16)
    send(dgo.at[other], dgp, "dg", (pn, z))
    f2 = dims(dgo[0], wi[0], 1, 1) + dims(dgo[1], wi[1], 1, 1)
    xx = x1[...]
    c = xx - jnp.mean(xx, -1, keepdims=True)
    r2 = lax.rsqrt(jnp.mean(c * c, -1, keepdims=True) + norm_eps)
    n = c * r2
    grow[3:4, :] = jnp.sum(f2 * n, 0, keepdims=True)
    cc = f2 * grow[1:2, :]
    dx = dys[mine, :].astype(f32) + r2 * (
        cc - jnp.mean(cc, -1, keepdims=True) - n * jnp.mean(cc * n, -1, keepdims=True)
    )
    x1[...] = dx
    dx1b[...] = dx.astype(bf16)
    send(dx1b.at[:, lanes(other * 384, 384)], dx1bp, "dx1b", (pn, z))
    for part in range(2):
        which = other if part == 0 else k
        col = lanes(which * 384, 384)
        feat = rows(which * 384, 384)
        left = jnp.concatenate([wa[0, feat, :], wa[1, feat, :]], axis=1)
        t = dims(left, dx1b[...], 1, 1).astype(bf16)
        if part == 0:
            dot_send[...] = t
            send(dot_send, dot_own.at[:, my_lanes], "do", (pn, z))
        else:
            dot_own[:, my_lanes] = t
    local(keep.at[5], probs.at[1], "e5")
    local(keep.at[4], probs.at[0], "e4")

    s2("m")
    arrived(h2.at[theirs, :], "h2")
    arrived(dgp, "dg")
    for name, o, w in (("i0", 0, 640), ("i1", 640, 512)):
        cols = pl.ds(o, w)
        grad[:, IN + o : IN + o + w] = (
            dims(h2[mine, :], dgo[k, :, cols], 0, 0) + dims(h2[theirs, :], dgp[:, cols], 0, 0)
        ).astype(bf16)
        s1(name)
    arrived(dx1bp, "dx1b")
    grad[:, ATTN : ATTN + 384] = (
        times(otb[:, my_lanes], dx1b[:, lanes(k * 384, 384)])
        + times(otb[:, lanes(other * 512, 512)], dx1bp[...])
    ).astype(bf16)
    s1("a")
    arrived(dot_own.at[:, lanes(other * 512, 512)], "do")

    for h in range(6):
        rsem(f"b{h}")
    backward_steps = {
        5: lambda: s3("m"),
        4: lambda: (s1("q2"), s2("i0")),
        3: lambda: (s2("i1"), s4("m")),
        2: lambda: (s1("q1"), s2("a"), s5("m"), s3("i0")),
        1: lambda: s2("q2"),
        0: lambda: (s1("q0"), s4("i0"), s3("i1"), s3("a")),
    }

    @pl.loop(0, 6)
    def _(turn):
        h = 5 - turn
        p, hh = h // 2, lax.rem(h, 2)
        qrow, krow, vrow = (rows(at + hh * 64, 64) for at in (0, 128, 256))
        arrived_at = rs_.at[names["e0"] + 2 * h]
        pltpu.make_async_copy(keep.at[h], probs.at[hh], arrived_at).wait()
        vt = qk[p, vrow, :]
        kt = qk[p, krow, :]
        for i in range(2):
            cols = slice(i * 512, i * 512 + 512)
            do = dot_own[rows(h * 64, 64), cols].astype(f32) * rl[pl.ds(h, 1), cols]
            delta = jnp.sum(do * otb[rows(k * 384 + h * 64, 64), cols].astype(f32), 0, keepdims=True)
            dob = do.astype(bf16)
            e = probs[hh, :, cols]
            ds = (e.astype(f32) * (dims(vt, dob, 0, 0) - delta)).astype(bf16)
            dk = dims(qk[p, qrow, cols], ds, 1, 1)
            dv = dims(dob, e, 1, 1)
            if i == 0:
                dkb[...] = dk
                dvb[...] = dv
            else:
                dkb[...] += dk
                dvb[...] += dv
            dq = times(kt, ds) * HEAD_DIM**-0.5
            c = cosr[:, cols]
            s = sinr[:, cols]
            qk[p, rows(hh * 64, 32), cols] = (dq[:32] * c + dq[32:] * s).astype(bf16)
            qk[p, rows(hh * 64 + 32, 32), cols] = (dq[32:] * c - dq[:32] * s).astype(bf16)

        @pl.when(h >= 2)
        def _():
            pltpu.make_async_copy(keep.at[h - 2], probs.at[hh], rs_.at[names["e0"] + 2 * (h - 2)]).start()

        d = dkb[...]
        c = cosr[...]
        s = sinr[...]
        qk[p, rows(128 + hh * 64, 32), :] = (d[:32] * c + d[32:] * s).astype(bf16)
        qk[p, rows(160 + hh * 64, 32), :] = (d[32:] * c - d[:32] * s).astype(bf16)
        qk[p, vrow, :] = dvb[...].astype(bf16)

        @pl.when(hh == 0)
        def _():
            grad[:, lanes(PAIR + 384 * p, 384)] = dims(h1t[...], qk[p], 1, 1).astype(bf16)

        for at, step in backward_steps.items():
            pl.when(h == at)(lambda step=step: step() and None)

    def f1_part(cols):
        return times(wq[0], qk[0, :, cols]) + times(wq[1], qk[1, :, cols]) + times(wq[2], qk[2, :, cols])

    big[0:768, 0:512] = f1_part(lanes(other * 512, 512))
    send(big.at[pl.ds(0, 768), pl.ds(0, 512)], f1r, "f1", (pn, z))
    s4("i1")
    big[0:768, 512:1024] = f1_part(my_lanes)
    s3("q2")
    s2("q1")
    s5("i0")
    s4("a")
    arrived(f1r, "f1")
    f1 = (big[0:768, 512:1024] + f1r[...]).T
    xx = xs[mine, :].astype(f32)
    c = xx - jnp.mean(xx, -1, keepdims=True)
    r1 = lax.rsqrt(jnp.mean(c * c, -1, keepdims=True) + norm_eps)
    n = c * r1
    grow[2:3, :] = jnp.sum(f1 * n, 0, keepdims=True)
    cc = f1 * grow[0:1, :]
    gi[...] = (
        x1[...] + r1 * (cc - jnp.mean(cc, -1, keepdims=True) - n * jnp.mean(cc * n, -1, keepdims=True))
    ).astype(bf16)
    two = jnp.concatenate([grow[2:4, :], jnp.zeros((126, 768), f32)], axis=0)
    grad[:, 0:128] = two.T.astype(bf16)
    s1("g")
    give_back(gi, gi_out, "agi", (0,))
    s4("q2")
    s2("q0")
    s3("q1")
    s5("i1")
    s5("a")
    give_back(gi, gi_out, "agi", (1,))
    s2("g")
    s3("q0")
    s4("q1")
    s3("g")
    s5("q2")
    s4("q0")
    s4("g")
    s5("q1")
    s5("q0")
    s5("g")
    for u in REDUCE:
        s6(u)
    given_back(lo_out, "alo")
    given_back(gi_out, "agi")
    drain_all()


frequency = np.broadcast_to(
    (np.float32(rope_base) ** (-(np.arange(32, dtype=np.float32) * 2) / HEAD_DIM))[:, None], (32, 128)
).astype(np.float32)


def finish_kernel(lo_raw, gi_raw, gp, lo, gi, g_qkv, g_attn, g_in, g_mlp, g_one, g_two, buf, sem):
    loads = [pltpu.make_async_copy(src, buf.at[i], sem.at[i]) for i, src in enumerate((lo_raw, gi_raw))]
    stores = [pltpu.make_async_copy(buf.at[i], dst, sem.at[2 + i]) for i, dst in enumerate((lo, gi))]
    for copy in loads:
        copy.start()
    for load, store in zip(loads, stores):
        load.wait()
        store.start()
    for c in range(2):
        for p in range(3):
            for t in range(3):
                o = 768 * t + 384 * c + 128 * p
                at = PAIR + 384 * p + 128 * t
                g_qkv[:, o : o + 128] = gp[c, :, at : at + 128]
        g_attn[:, 384 * c : 384 * c + 384] = gp[c, :, ATTN : ATTN + 384]
        g_in[:, 1152 * c : 1152 * c + 1152] = gp[c, :, IN : IN + 1152]
    g_mlp[:, 0:640] = gp[0, :, MLP : MLP + 640]
    g_mlp[:, 640:1152] = gp[1, :, MLP + 128 : MLP + 640]
    both = gp[0, :, 0:128] + gp[1, :, 0:128]
    flat = jnp.concatenate([both, jnp.zeros((104, 128), f32)], axis=0).T
    g_one[...] = flat[0:1, 0:24]
    g_two[...] = flat[1:2, 0:24]
    for store in stores:
        store.wait()


def fast(layer_in, seg_start, out_grad, w_qkv, w_attn_out, w_in, w_mlp_out, norm_attn, norm_mlp):
    hbm = pl.BlockSpec(memory_space=pltpu.HBM)
    vmem = pl.BlockSpec(memory_space=pltpu.VMEM)
    V = pltpu.VMEM
    outs = pl.pallas_call(
        step_kernel,
        name="layer",
        out_shape=[
            jax.ShapeDtypeStruct((2, 256, 768), bf16),
            jax.ShapeDtypeStruct((2, 256, 768), bf16),
            jax.ShapeDtypeStruct((2, 24, WIDTH), f32),
            jax.ShapeDtypeStruct((768, WIDTH), bf16),
            jax.ShapeDtypeStruct((6, 1024, 1024), bf16),
        ],
        in_specs=[hbm, hbm, vmem, hbm, hbm, hbm, hbm, vmem, vmem, vmem],
        out_specs=[hbm] * 5,
        scratch_shapes=[
            V((2, 24, WIDTH), bf16),
            V((8, 128), f32),
            V((1024, 768), bf16),
            V((1024, 768), bf16),
            V((1, 1024), jnp.int32),
            V((768, 1024), bf16),
            V((3, 768, 384), bf16),
            V((2, 768, 384), bf16),
            V((2, 768, 1152), bf16),
            V((768, 1152), bf16),
            V((768, 128), bf16),
            V((32, 1024), f32),
            V((32, 1024), f32),
            V((3, 384, 1024), bf16),
            V((1024, 1152), f32),
            V((2, 1024, 1024), bf16),
            V((768, 1024), bf16),
            V((8, 1024), f32),
            V((512, 768), f32),
            V((1024, 768), bf16),
            V((512, 1152), bf16),
            V((512, 640), bf16),
            V((2, 512, 1152), bf16),
            V((512, 1152), bf16),
            V((512, 768), bf16),
            V((512, 384), bf16),
            V((384, 512), bf16),
            V((384, 1024), bf16),
            V((768, 512), f32),
            V((512, 768), bf16),
            V((512, 768), bf16),
            V((768, WIDTH), bf16),
            V((8, 768), f32),
            V((64, 1024), f32),
            V((64, 1024), f32),
            V((2, 96, WIDTH), bf16),
            V((2, 96, WIDTH), bf16),
            V((96, WIDTH), bf16),
            V((96, WIDTH), bf16),
            V((2, 4, 24, WIDTH), bf16),
            V((2, 24, WIDTH), bf16),
            V((2, 2, 24, WIDTH), bf16),
            V((2, 24, WIDTH), bf16),
            V((2, 24, WIDTH), f32),
            pltpu.SemaphoreType.DMA((160,)),
            pltpu.SemaphoreType.DMA((24,)),
            pltpu.SemaphoreType.DMA((220,)),
        ],
        compiler_params=pltpu.CompilerParams(
            collective_id=0, has_side_effects=True, vmem_limit_bytes=67043328
        ),
    )(
        layer_in, out_grad, seg_start, w_qkv, w_attn_out, w_in, w_mlp_out,
        norm_attn[None], norm_mlp[None], frequency,
    )
    done = pl.pallas_call(
        finish_kernel,
        name="finish",
        out_shape=[
            jax.ShapeDtypeStruct((2, 256, 768), bf16),
            jax.ShapeDtypeStruct((2, 256, 768), bf16),
            jax.ShapeDtypeStruct((24, 2304), f32),
            jax.ShapeDtypeStruct((24, 768), f32),
            jax.ShapeDtypeStruct((24, 2304), f32),
            jax.ShapeDtypeStruct((24, 1152), f32),
            jax.ShapeDtypeStruct((1, 24), f32),
            jax.ShapeDtypeStruct((1, 24), f32),
        ],
        in_specs=[hbm, hbm, vmem],
        out_specs=[hbm, hbm] + [vmem] * 6,
        scratch_shapes=[V((2, 2, 256, 768), bf16), pltpu.SemaphoreType.DMA((4,))],
    )(*outs[:3])
    return (*done[:6], done[6][0], done[7][0])


def normalize(values):
    centered = values - jnp.mean(values, axis=-1, keepdims=True)
    spread = jnp.mean(centered * centered, axis=-1, keepdims=True)
    return centered * lax.rsqrt(spread + norm_eps)


def rope_tables(positions):
    half_dim = HEAD_DIM // 2
    frequency = rope_base ** (-(jnp.arange(half_dim).astype(jnp.float32) * 2.0) / HEAD_DIM)
    angles = positions.astype(jnp.float32)[:, None] * frequency[None, :]
    angles = jnp.concatenate([angles, angles], axis=-1)
    return (jnp.cos(angles), jnp.sin(angles))


def turn_half(values):
    half_dim = values.shape[-1] // 2
    return jnp.concatenate([-values[..., half_dim:], values[..., :half_dim]], axis=-1)


def rotate(values, cosine_table, sine_table):
    return values * cosine_table[:, None, :] + turn_half(values) * sine_table[:, None, :]


def unrotate(values, cosine_table, sine_table):
    return values * cosine_table[:, None, :] - turn_half(values) * sine_table[:, None, :]


def product(left, right):
    return jnp.dot(left, right, preferred_element_type=jnp.float32)


def left_transposed(left, right):
    return lax.dot_general(
        left, right, (((0,), (0,)), ((), ())), preferred_element_type=jnp.float32
    )


def right_transposed(left, right):
    return lax.dot_general(
        left, right, (((1,), (1,)), ((), ())), preferred_element_type=jnp.float32
    )


def to_groups(array):
    row_count, head_count, head_size = array.shape
    return array.reshape(row_count, head_count // 4, 4, head_size).transpose(1, 0, 2, 3)


def from_groups(array):
    group_count, row_count, group_heads, head_size = array.shape
    return array.transpose(1, 0, 2, 3).reshape(row_count, group_count * group_heads, head_size)


def attend_group(group_in, same_doc):
    query_part, key_part, value_part = group_in
    scores = jnp.einsum(
        "qhd,khd->hqk", query_part, key_part, preferred_element_type=jnp.float32
    ) * HEAD_DIM ** (-0.5)
    masked = jnp.where(same_doc[None], scores, neg_large)
    highest = jnp.max(masked, axis=-1, keepdims=True)
    shifted = jnp.exp(masked - highest)
    totals = jnp.sum(shifted, axis=-1, keepdims=True)
    attn_prob = shifted / totals
    log_total = highest + jnp.log(totals)
    mixed_out = jnp.einsum(
        "hqk,khd->qhd",
        attn_prob.astype(jnp.bfloat16),
        value_part,
        preferred_element_type=jnp.float32,
    )
    return (mixed_out, log_total[..., 0])


def attend_back(group_in, same_doc):
    query_part, key_part, value_part, grad_part, log_total = group_in
    scores = jnp.einsum(
        "qhd,khd->hqk", query_part, key_part, preferred_element_type=jnp.float32
    ) * HEAD_DIM ** (-0.5)
    attn_prob = jnp.where(same_doc[None], jnp.exp(scores - log_total[..., None]), 0.0)
    grad_prob = jnp.einsum(
        "qhd,khd->hqk", grad_part, value_part, preferred_element_type=jnp.float32
    )
    inner_sum = jnp.sum(attn_prob * grad_prob, axis=-1, keepdims=True)
    grad_score = (attn_prob * (grad_prob - inner_sum)).astype(jnp.bfloat16)
    grad_query = jnp.einsum(
        "hqk,khd->qhd", grad_score, key_part, preferred_element_type=jnp.float32
    ) * HEAD_DIM ** (-0.5)
    grad_key = jnp.einsum(
        "hqk,qhd->khd", grad_score, query_part, preferred_element_type=jnp.float32
    ) * HEAD_DIM ** (-0.5)
    grad_value = jnp.einsum(
        "hqk,qhd->khd",
        attn_prob.astype(jnp.bfloat16),
        grad_part,
        preferred_element_type=jnp.float32,
    )
    return (grad_query, grad_key, grad_value)


def scaled_norm(values_in, gain_row):
    return normalize(values_in) * gain_row


def geglu(first_half, second_half):
    return jax.nn.gelu(first_half, approximate=False) * second_half


def local(layer_in, seg_start, out_grad, w_qkv, w_attn_out, w_in, w_mlp_out, norm_attn, norm_mlp):
    micro_count = layer_in.shape[0]
    span_len = layer_in.shape[1]
    model_width = layer_in.shape[2]
    ctx_rank = lax.axis_index("ctx")
    grad_sums = (
        jnp.zeros((model_width, 3 * model_width), jnp.float32),
        jnp.zeros((model_width, model_width), jnp.float32),
        jnp.zeros((model_width, 2 * FF), jnp.float32),
        jnp.zeros((model_width, FF), jnp.float32),
        jnp.zeros((model_width,), jnp.float32),
        jnp.zeros((model_width,), jnp.float32),
    )
    offsets = ctx_rank * span_len + jnp.arange(span_len, dtype=jnp.int32)
    outputs = []
    grad_inputs = []
    for micro_step in range(micro_count):
        gathered = (
            lax.all_gather(w_qkv, ("dp", "ctx"), axis=0, tiled=True),
            lax.all_gather(w_attn_out, ("dp", "ctx"), axis=0, tiled=True),
            lax.all_gather(w_in, ("dp", "ctx"), axis=0, tiled=True),
            lax.all_gather(w_mlp_out, ("dp", "ctx"), axis=0, tiled=True),
            lax.all_gather(norm_attn, ("dp", "ctx"), axis=0, tiled=True),
            lax.all_gather(norm_mlp, ("dp", "ctx"), axis=0, tiled=True),
        )
        qkv_full, attn_full, in_full, mlp_full, gain_attn, gain_mlp = gathered
        starts_here = seg_start[micro_step]
        hidden = layer_in[micro_step].astype(jnp.float32)
        cosine_table, sine_table = rope_tables(offsets - starts_here)
        normed, norm_back = jax.vjp(scaled_norm, hidden, gain_attn.astype(jnp.float32))
        normed_low = normed.astype(jnp.bfloat16)
        qkv_local = product(normed_low, qkv_full).reshape(span_len, 3, HEADS, HEAD_DIM)
        queries = rotate(qkv_local[:, 0], cosine_table, sine_table).astype(jnp.bfloat16)
        keys_here = rotate(qkv_local[:, 1], cosine_table, sine_table).astype(jnp.bfloat16)
        values_here = qkv_local[:, 2].astype(jnp.bfloat16)
        keys_all, values_all, starts_all = (
            lax.all_gather(keys_here, "ctx", axis=0, tiled=True),
            lax.all_gather(values_here, "ctx", axis=0, tiled=True),
            lax.all_gather(starts_here, "ctx", axis=0, tiled=True),
        )
        same_doc = starts_here[:, None] == starts_all[None, :]
        query_groups = to_groups(queries)
        key_groups = to_groups(keys_all)
        value_groups = to_groups(values_all)
        mixed_out, log_total = lax.map(
            lambda group_in: attend_group(group_in, same_doc),
            (query_groups, key_groups, value_groups),
        )
        attended = from_groups(mixed_out).reshape(span_len, model_width).astype(jnp.bfloat16)
        middle = hidden + product(attended, attn_full)
        normed_mlp, norm_mlp_back = jax.vjp(scaled_norm, middle, gain_mlp.astype(jnp.float32))
        normed_mlp_low = normed_mlp.astype(jnp.bfloat16)
        projected = product(normed_mlp_low, in_full)
        gated_out, geglu_back = jax.vjp(geglu, projected[:, :FF], projected[:, FF:])
        gated_low = gated_out.astype(jnp.bfloat16)
        result = middle + right_transposed(gated_low, mlp_full)
        outputs.append(result.astype(jnp.bfloat16))
        qkv_full, attn_full, in_full, mlp_full = (
            lax.all_gather(w_qkv, ("dp", "ctx"), axis=0, tiled=True),
            lax.all_gather(w_attn_out, ("dp", "ctx"), axis=0, tiled=True),
            lax.all_gather(w_in, ("dp", "ctx"), axis=0, tiled=True),
            lax.all_gather(w_mlp_out, ("dp", "ctx"), axis=0, tiled=True),
        )
        grad_out = out_grad[micro_step].astype(jnp.float32)
        grad_out_low = out_grad[micro_step]
        grad_mlp_weight = left_transposed(grad_out_low, gated_low)
        grad_gated = product(grad_out_low, mlp_full)
        grad_first, grad_second = geglu_back(grad_gated)
        grad_projected = jnp.concatenate([grad_first, grad_second], axis=1).astype(jnp.bfloat16)
        grad_in_weight = left_transposed(normed_mlp_low, grad_projected)
        grad_normed_mlp = right_transposed(grad_projected, in_full)
        grad_middle_norm, grad_gain_mlp = norm_mlp_back(grad_normed_mlp)
        grad_middle = grad_out + grad_middle_norm
        grad_middle_low = grad_middle.astype(jnp.bfloat16)
        grad_attn_weight = left_transposed(attended, grad_middle_low)
        grad_attended = (
            right_transposed(grad_middle_low, attn_full)
            .astype(jnp.bfloat16)
            .reshape(span_len, HEADS, HEAD_DIM)
        )
        grad_groups = to_groups(grad_attended)
        grad_query_groups, grad_key_groups, grad_value_groups = lax.map(
            lambda group_in: attend_back(group_in, same_doc),
            (query_groups, key_groups, value_groups, grad_groups, log_total),
        )
        keys_total = keys_all.shape[0]
        grad_keys, grad_values = (
            lax.psum_scatter(
                from_groups(grad_key_groups).reshape(keys_total, model_width).astype(jnp.bfloat16),
                "ctx",
                scatter_dimension=0,
                tiled=True,
            ).astype(jnp.float32),
            lax.psum_scatter(
                from_groups(grad_value_groups)
                .reshape(keys_total, model_width)
                .astype(jnp.bfloat16),
                "ctx",
                scatter_dimension=0,
                tiled=True,
            ).astype(jnp.float32),
        )
        grad_qkv = jnp.stack(
            [
                unrotate(from_groups(grad_query_groups), cosine_table, sine_table),
                unrotate(grad_keys.reshape(span_len, HEADS, HEAD_DIM), cosine_table, sine_table),
                grad_values.reshape(span_len, HEADS, HEAD_DIM),
            ],
            axis=1,
        )
        grad_qkv = grad_qkv.reshape(span_len, 3 * model_width).astype(jnp.bfloat16)
        grad_qkv_weight = left_transposed(normed_low, grad_qkv)
        grad_normed = right_transposed(grad_qkv, qkv_full)
        grad_hidden_norm, grad_gain_attn = norm_back(grad_normed)
        grad_inputs.append((grad_middle + grad_hidden_norm).astype(jnp.bfloat16))
        grad_sums = (
            grad_sums[0] + grad_qkv_weight,
            grad_sums[1] + grad_attn_weight,
            grad_sums[2] + grad_in_weight,
            grad_sums[3] + grad_mlp_weight,
            grad_sums[4] + grad_gain_attn,
            grad_sums[5] + grad_gain_mlp,
        )
    shares = (
        lax.psum_scatter(grad_sums[0], ("dp", "ctx"), scatter_dimension=0, tiled=True),
        lax.psum_scatter(grad_sums[1], ("dp", "ctx"), scatter_dimension=0, tiled=True),
        lax.psum_scatter(grad_sums[2], ("dp", "ctx"), scatter_dimension=0, tiled=True),
        lax.psum_scatter(grad_sums[3], ("dp", "ctx"), scatter_dimension=0, tiled=True),
        lax.psum_scatter(grad_sums[4], ("dp", "ctx"), scatter_dimension=0, tiled=True),
        lax.psum_scatter(grad_sums[5], ("dp", "ctx"), scatter_dimension=0, tiled=True),
    )
    return (
        jnp.stack(outputs),
        jnp.stack(grad_inputs),
        shares[0],
        shares[1],
        shares[2],
        shares[3],
        shares[4],
        shares[5],
    )


def solution(mesh):
    A = P(None, ("dp", "ctx"), None)
    S = P(None, ("dp", "ctx"))
    W = P(("dp", "ctx"), None)
    G = P(("dp", "ctx"))
    return jax.shard_map(
        fast if dict(mesh.shape) == {"dp": 8, "ctx": 4} else local,
        mesh=mesh,
        in_specs=(A, S, A, W, W, W, W, G, G),
        out_specs=(A, A, W, W, W, W, G, G),
        check_vma=False,
    )
```

```python
import contextlib

import jax
import jax.numpy as jnp
import numpy as np
from jax import lax
from jax.experimental import pallas as pl
from jax.experimental.pallas import tpu as pltpu
from jax.sharding import PartitionSpec as P

MESH = pl.DeviceIdType.MESH
bf16 = jnp.bfloat16
f32 = jnp.float32

HEADS = 12
HEAD_DIM = 64
FF = 1152
rope_base = 160000.0
norm_eps = 1e-05
neg_large = -1e30

WIDTH = 3328
GATHER = [(0, 512), (512, 768), (1280, 384), (1664, 640), (2304, 512), (2816, 512)]
PAIR = 128
ATTN = 1280
IN = 1664
MLP = 2816
REDUCE = {
    "m": (2816, 512),
    "i0": (1664, 640),
    "i1": (2304, 512),
    "a": (1280, 384),
    "q2": (896, 384),
    "q1": (512, 384),
    "q0": (128, 384),
    "g": (0, 128),
}


TRACE = False


def scope(name):
    return jax.named_scope(name) if TRACE else contextlib.nullcontext()


def scoped(fn):
    def inner(*args):
        with scope(f"{fn.__name__}_{args[0] if args and isinstance(args[0], (int, str)) else ''}"):
            return fn(*args)

    return inner


def dims(left, right, left_at, right_at):
    return lax.dot_general(
        left, right, (((left_at,), (right_at,)), ((), ())), preferred_element_type=f32
    )


def times(left, right):
    return jnp.dot(left, right, preferred_element_type=f32)


def step_kernel(
    x_in, dy_in, seg_in, w_qkv, w_attn, w_in, w_mlp, g_attn, g_mlp, freq,
    lo_out, gi_out, gp_out, land, keep,
    wp, gcol,
    xs, dys, sg, h1t, wq, wa, wi, wm, gains, cosr, sinr, qk, big, probs, otb, rl, x1, h2, hid, hidp,
    dgo, dgp, dx1b, dx1bp, dot_send, dot_own, f1r, lo, gi, grad, grow, growp, dkb, dvb,
    ra, rb, ra2, rb2, zs, zp, zm, zx, fin,
    rs_, ls_, sends,
):
    dp = lax.axis_index("dp")
    z = lax.axis_index("ctx")
    q = dp // 2
    k = lax.rem(dp, 2)
    other = 1 - k
    pn = dp + 1 - 2 * k
    xn = dp + 2 - 4 * lax.rem(dp // 2, 2)
    yn = dp + 4 - 8 * (dp // 4)
    zn = z + 1 - 2 * lax.rem(z, 2)
    zb = jnp.where(z < 2, 2, 1)
    zh = z // 2
    qx = q + 1 - 2 * lax.rem(q, 2)
    qy = q + 2 - 4 * (q // 2)
    qd = qx + 2 - 4 * (qx // 2)
    inner = jnp.logical_or(z == 1, z == 2)
    outer = jnp.logical_or(z == 0, z == 3)
    near = k == zh
    away = k != zh
    names = {}
    count = {"send": 0, "local": 0}
    drains = []

    def rsem(name):
        return rs_.at[names.setdefault(name, len(names))]

    def still(view):
        index = view.transforms[0].indices
        return view.ref.at[tuple(pl.ds(0, at.size) if hasattr(at, "size") else 0 for at in index)]

    keyed = {}

    def send(src, dst, name, dev, when=None, sem=None, key=None):
        first = key is None or key not in keyed
        if first:
            i = count["send"]
            count["send"] += 1
            keyed[key] = i
        else:
            i = keyed[key]
        copy = pltpu.make_async_remote_copy(
            src_ref=src, dst_ref=dst, send_sem=sends.at[i], recv_sem=rsem(name) if sem is None else sem,
            device_id=dev, device_id_type=MESH,
        )
        if when is None:
            copy.start()
        else:
            pl.when(when())(copy.start)
        if first:
            drains.append((i, src, when))

    def drain_all():
        for i, src, when in drains:
            view = still(src) if hasattr(src, "transforms") else src

            def wait(view=view, i=i):
                pltpu.make_async_copy(view, view, sends.at[i]).wait()

            if when is None:
                wait()
            else:
                pl.when(when())(wait)

    def local(src, dst, name):
        copy = pltpu.make_async_copy(src, dst, rsem(name))
        copy.start()
        return copy

    def arrived(ref, name):
        pltpu.make_async_copy(ref, ref, rsem(name)).wait()

    def rows(start, size):
        return pl.ds(pl.multiple_of(start, 8), size)

    def lanes(start, size):
        return pl.ds(pl.multiple_of(start, 128), size)

    barrier = pltpu.get_barrier_semaphore()
    for dz in range(1, 4):
        for kk in range(2):
            pl.semaphore_signal(
                barrier, inc=1, device_id=(2 * q + kk, lax.rem(z + dz, 4)), device_id_type=MESH
            )
    for dev in (pn, xn, yn):
        pl.semaphore_signal(barrier, inc=1, device_id=(dev, z), device_id_type=MESH)

    packs = []
    for c in range(2):
        for p in range(3):
            for t in range(3):
                packs.append((w_qkv, 768 * t + 384 * c + 128 * p, c, PAIR + 384 * p + 128 * t, 128))
        packs.append((w_attn, 384 * c, c, ATTN, 384))
        packs.append((w_in, 1152 * c, c, IN, 1152))
        packs.append((w_mlp, 640 * c, c, MLP, 512))
    packs.append((w_mlp, 512, 0, 0, 128))
    packing = [
        pltpu.make_async_copy(w.at[:, pl.ds(o, n)], wp.at[c, :, pl.ds(at, n)], ls_.at[i])
        for i, (w, o, c, at, n) in enumerate(packs)
    ]
    for copy in packing:
        copy.start()
    gcol[...] = jnp.zeros_like(gcol)
    gcol[0:1, 0:24] = g_attn[...].astype(f32)
    gcol[1:2, 0:24] = g_mlp[...].astype(f32)
    columns = jnp.concatenate([gcol[...], jnp.zeros((120, 128), f32)], axis=0).T[0:24].astype(bf16)
    wp[1, :, 0:128] = columns

    @scoped
    def zstage(u, turn=None):
        o, w = GATHER[u]
        cols = pl.ds(o, w)

        def body():
            dst = land.at[rows(dp * 96 + z * 24, 24), cols]
            for c in range(2):
                src = wp.at[c, :, cols]
                send(src, dst, f"z{u}", (2 * q + c, zn), key=f"zn{u}{c}")
                send(src, dst, f"z{u}", (2 * q + c, zb), key=f"zb{u}{c}")
                send(src, dst, f"z{u}", (pn, z), when=lambda c=c: k != c, key=f"zp{u}{c}")
                pl.when(k == c)(lambda src=src: local(src, dst, f"z{u}") and None)

        in_turn(turn, body)

    def in_turn(turn, body):
        if turn is None:
            body()
        else:
            pl.when(turn)(body)

    @scoped
    def slab_in(u, turn=None):
        o, w = GATHER[u]
        cols = pl.ds(o, w)

        def body():
            arrived(land.at[rows(q * 192, 192), cols], f"z{u}")
            for j in range(2):
                part = land.at[rows((2 * q + j) * 96 + lax.rem(4 - 2 * z + 4, 4) * 24, 48), cols]
                send(part, part, f"z{u}", (dp, zn), when=lambda: inner, key=f"fs{u}{j}")

        in_turn(turn, body)

    @scoped
    def xysend(u):
        o, w = GATHER[u]
        slab = land.at[rows(q * 192, 192), pl.ds(o, w)]
        send(slab, slab, f"x{u}", (xn, z))
        send(slab, slab, f"y{u}", (yn, z))

    @scoped
    def diag(u):
        o, w = GATHER[u]
        cols = pl.ds(o, w)
        arrived(land.at[rows(qx * 192, 192), cols], f"x{u}")
        part = land.at[rows(qx * 192, 96), cols]
        send(part, part, f"dx{u}", (yn, z))
        arrived(land.at[rows(qy * 192, 192), cols], f"y{u}")
        part = land.at[rows(qy * 192 + 96, 96), cols]
        send(part, part, f"dy{u}", (xn, z))

    @scoped
    def done(u):
        o, w = GATHER[u]
        cols = pl.ds(o, w)
        arrived(land.at[rows(qd * 192, 96), cols], f"dx{u}")
        arrived(land.at[rows(qd * 192 + 96, 96), cols], f"dy{u}")

    def activation(src_ref, dst_ref, name, turn=None):
        for m in range(2):
            src = src_ref.at[m]
            dst = dst_ref.at[rows(z * 256, 256), :]
            sem = rs_.at[base[name] + lax.rem(z, 2)]

            def going(m=m):
                there = 2 * k + m != z
                return there if turn is None else jnp.logical_and(turn, there)

            here = 2 * k + m == z
            if turn is not None:
                here = jnp.logical_and(turn, here)
            send(src, dst, None, (2 * q + zh, 2 * k + m), when=going, sem=sem)
            pl.when(here)(pltpu.make_async_copy(src, dst, sem).start)

    base = {}
    for name in ("ax", "ay", "alo", "agi"):
        base[name] = len(names)
        names[name + "0"] = len(names)
        names[name + "1"] = len(names)

    @scoped
    def share_activation(ref, name, turn=None):
        def body():
            for j in range(2):
                r = rows(k * 512 + j * 256, 256)
                arrived(ref.at[r, :], f"{name}{j}")
                send(ref.at[r, :], ref.at[r, :], f"p{name}{j}", (pn, z), key=f"sh{name}{j}")

        in_turn(turn, body)

    @scoped
    def shared_activation(ref, name, turn=None):
        def body():
            for j in range(2):
                arrived(ref.at[rows(other * 512 + j * 256, 256), :], f"p{name}{j}")

        in_turn(turn, body)

    @scoped
    def give_back(src_ref, out_ref, name, blocks=(0, 1)):
        m = lax.rem(z, 2)
        for j in blocks:
            src = src_ref.at[pl.ds(j * 256, 256), :]
            dst = out_ref.at[m]
            sem = rs_.at[base[name] + m]

            def away(j=j):
                return jnp.logical_or(2 * k + j != z, zh != k)

            send(src, dst, None, (2 * q + zh, 2 * k + j), when=away, sem=sem)
            pl.when(jnp.logical_not(away()))(pltpu.make_async_copy(src, dst, sem).start)

    @scoped
    def given_back(out_ref, name):
        for m in range(2):
            arrived(out_ref.at[m], f"{name}{m}")

    def seg_send():
        for m in range(2):
            src = seg_in.at[pl.ds(m, 1), :]
            dst = sg.at[:, lanes(z * 256, 256)]
            for c in range(2):

                def away(m=m, c=c):
                    return jnp.logical_or(2 * k + m != z, k != c)

                send(src, dst, "seg", (2 * q + c, 2 * k + m), when=away)
                pl.when(jnp.logical_not(away()))(pltpu.make_async_copy(src, dst, rsem("seg")).start)

    @scoped
    def s1(u):
        o, w = REDUCE[u]
        cols = pl.ds(o, w)
        for slot, quarter in enumerate((qx, qd)):
            send(grad.at[rows(quarter * 192, 96), cols], ra.at[slot, :, cols], f"ra{u}", (xn, z))
        for slot, quarter in enumerate((qy, qd)):
            send(grad.at[rows(quarter * 192 + 96, 96), cols], rb.at[slot, :, cols], f"rb{u}", (yn, z))

    @scoped
    def s2(u):
        o, w = REDUCE[u]
        cols = pl.ds(o, w)
        arrived(ra.at[:, :, cols], f"ra{u}")
        r = rows(qy * 192, 96)
        grad[r, cols] = (grad[r, cols].astype(f32) + ra[1, :, cols].astype(f32)).astype(bf16)
        send(grad.at[r, cols], ra2.at[:, cols], f"ra2{u}", (yn, z))
        arrived(rb.at[:, :, cols], f"rb{u}")
        r2 = rows(qx * 192 + 96, 96)
        grad[r2, cols] = (grad[r2, cols].astype(f32) + rb[1, :, cols].astype(f32)).astype(bf16)
        send(grad.at[r2, cols], rb2.at[:, cols], f"rb2{u}", (xn, z))

    @scoped
    def s3(u):
        o, w = REDUCE[u]
        cols = pl.ds(o, w)
        arrived(ra2.at[:, cols], f"ra2{u}")
        arrived(rb2.at[:, cols], f"rb2{u}")
        for j, (one, two) in enumerate(((ra, ra2), (rb, rb2))):
            total = (
                grad[rows(q * 192 + 96 * j, 96), cols].astype(f32)
                + one[0, :, cols].astype(f32)
                + two[:, cols].astype(f32)
            )
            for at in range(4):
                zs[j, at, :, cols] = total[24 * at : 24 * at + 24].astype(bf16)
        send(zs.at[:, zn, :, cols], zp.at[:, :, cols], f"zp{u}", (dp, zn))
        far = 2 * (1 - zh)
        send(zs.at[:, pl.ds(far, 2), :, cols], zm.at[:, :, :, cols], f"zm{u}", (dp, zn), when=lambda: outer)

    @scoped
    def s4(u):
        o, w = REDUCE[u]
        cols = pl.ds(o, w)
        far = 2 * (1 - zh)

        @pl.when(inner)
        def _():
            arrived(zm.at[:, :, :, cols], f"zm{u}")
            for j in range(2):
                for at in range(2):
                    zs[j, far + at, :, cols] = (
                        zs[j, far + at, :, cols].astype(f32) + zm[j, at, :, cols].astype(f32)
                    ).astype(bf16)

        for at in range(2):
            send(zs.at[:, far + at, :, cols], zx.at[:, :, cols], f"zx{u}", (dp, far + at), when=lambda: inner)

    @scoped
    def s5(u):
        o, w = REDUCE[u]
        cols = pl.ds(o, w)
        arrived(zp.at[:, :, cols], f"zp{u}")
        arrived(zx.at[:, :, cols], f"zx{u}")
        for j in range(2):
            fin[j, :, cols] = (
                zs[j, z, :, cols].astype(f32) + zp[j, :, cols].astype(f32) + zx[j, :, cols].astype(f32)
            )
        local(fin.at[k, :, cols], gp_out.at[k, :, cols], f"fl{u}")
        send(fin.at[other, :, cols], gp_out.at[k, :, cols], f"fr{u}", (pn, z))

    @scoped
    def s6(u):
        o, w = REDUCE[u]
        cols = pl.ds(o, w)
        arrived(gp_out.at[k, :, cols], f"fl{u}")
        arrived(gp_out.at[other, :, cols], f"fr{u}")

    pl.semaphore_wait(barrier, 9)

    for copy in packing:
        copy.wait()
    seg_send()
    zstage(0)
    zstage(1)
    activation(x_in, xs, "ax", near)
    zstage(2, outer)
    zstage(3, outer)
    slab_in(0)
    xysend(0)
    slab_in(1)
    xysend(1)
    zstage(2, inner)
    zstage(3, inner)
    slab_in(2, inner)
    slab_in(3, inner)
    activation(x_in, xs, "ax", away)
    arrived(sg, "seg")
    positions = (lax.broadcasted_iota(jnp.int32, (1, 1024), 1) - sg[...]).astype(f32)
    angles = freq[:, 0:1] * positions
    cosr[...] = jnp.cos(angles)
    sinr[...] = jnp.sin(angles)
    starts = sg[...].astype(f32)
    column = jnp.broadcast_to(starts, (128, 1024)).T

    @pl.loop(0, 8)
    def _(i):
        r = lanes(i * 128, 128)
        here = jnp.broadcast_to(sg[:, r].astype(f32), (1024, 128))
        big[:, r] = jnp.where(column == here, 0.0, neg_large)

    diag(0)
    diag(1)
    slab_in(2, outer)
    xysend(2)
    zstage(4)
    zstage(5)
    done(0)
    first = land.at[:, pl.ds(0, 128)]
    spare = wm.at[:, pl.ds(512, 128)]

    @pl.when(k == 0)
    def _():
        local(first, spare, "cm")

    @pl.when(k == 1)
    def _():
        local(first, gains, "cg")

    send(first, spare, "cm", (pn, z), when=lambda: k == 0)
    send(first, gains, "cg", (pn, z), when=lambda: k == 1)
    local(land.at[:, pl.ds(128, 384)], wq.at[0], "cq0")
    arrived(gains, "cg")
    gain_rows = gains[...].astype(f32).T
    grow[...] = gain_rows[0:8]
    done(1)
    local(land.at[:, pl.ds(512, 384)], wq.at[1], "cq1")
    local(land.at[:, pl.ds(896, 384)], wq.at[2], "cq2")

    def queries(half):
        for i in range(2):
            at = half * 512 + i * 256
            xb = xs[rows(at, 256), :].astype(f32)
            c = xb - jnp.mean(xb, -1, keepdims=True)
            n = c * lax.rsqrt(jnp.mean(c * c, -1, keepdims=True) + norm_eps)
            h1t[:, lanes(at, 256)] = (n * grow[0:1, :]).astype(bf16).T

        cols = lanes(half * 512, 512)

        @pl.loop(0, 3)
        def _(p):
            t = times(wq[p].T, h1t[:, cols])
            c = cosr[:, cols]
            s = sinr[:, cols]
            for hh in range(4):
                u1 = t[hh * 64 : hh * 64 + 32]
                u2 = t[hh * 64 + 32 : hh * 64 + 64]
                scale = HEAD_DIM**-0.5 if hh < 2 else 1.0
                qk[p, hh * 64 : hh * 64 + 32, cols] = ((u1 * c - u2 * s) * scale).astype(bf16)
                qk[p, hh * 64 + 32 : hh * 64 + 64, cols] = ((u2 * c + u1 * s) * scale).astype(bf16)
            qk[p, 256:384, cols] = t[256:384].astype(bf16)

    share_activation(xs, "ax", k == zh)
    shared_activation(xs, "ax", k != zh)
    for p in range(3):
        arrived(wq.at[p], f"cq{p}")
    slab_in(3, outer)
    xysend(3)
    with scope("qkvnear"):
        queries(zh)
    diag(2)
    share_activation(xs, "ax", k != zh)
    slab_in(4, inner)
    shared_activation(xs, "ax", k == zh)
    with scope("qkvfar"):
        queries(1 - zh)
    slab_in(5, inner)
    slab_in(4, outer)
    xysend(4)

    @scoped
    def weight_done(u):
        done(u)
        o, w = GATHER[u]
        if u == 2:
            pieces = [(land.at[:, pl.ds(o, w)], wa.at[k], None)]
        elif u == 3:
            pieces = [(land.at[:, pl.ds(o, w)], wi.at[k, :, pl.ds(0, 640)], None)]
        elif u == 4:
            pieces = [(land.at[:, pl.ds(o, w)], wi.at[k, :, pl.ds(640, 512)], None)]
        else:
            pieces = [
                (land.at[:, pl.ds(o, w)], wm.at[:, pl.ds(0, 512)], lambda: k == 0),
                (land.at[:, pl.ds(o, w)], wm.at[:, pl.ds(640, 512)], lambda: k == 1),
            ]
        for src, dst, when in pieces:
            if when is None:
                local(src, dst, f"cw{u}")
            else:
                pl.when(when())(lambda src=src, dst=dst: local(src, dst, f"cw{u}") and None)
            send(src, dst, f"pw{u}", (pn, z), when=when)

    @scoped
    def weight_here(u):
        if u == 2:
            mine, theirs = [(wa.at[k], None)], [(wa.at[other], None)]
        elif u == 3:
            mine, theirs = [(wi.at[k, :, pl.ds(0, 640)], None)], [(wi.at[other, :, pl.ds(0, 640)], None)]
        elif u == 4:
            mine, theirs = [(wi.at[k, :, pl.ds(640, 512)], None)], [(wi.at[other, :, pl.ds(640, 512)], None)]
        else:
            low, high = wm.at[:, pl.ds(0, 512)], wm.at[:, pl.ds(640, 512)]
            mine, theirs = [(low, k == 0), (high, k == 1)], [(low, k == 1), (high, k == 0)]
        for group, name in ((mine, "cw"), (theirs, "pw")):
            for ref, when in group:
                if when is None:
                    arrived(ref, f"{name}{u}")
                else:
                    pl.when(when)(lambda ref=ref, name=name: arrived(ref, f"{name}{u}"))

    for h in range(6):
        rsem(f"e{h}")
        rsem(f"o{h}")
    first_send = count["send"]
    count["send"] += 6
    forward_steps = {
        0: lambda: (slab_in(5, outer), xysend(5), activation(dy_in, dys, "ay"), diag(3)),
        1: lambda: diag(4),
        2: lambda: (weight_done(2), diag(5)),
        3: lambda: weight_done(3),
        4: lambda: weight_done(4),
        5: lambda: weight_done(5),
    }

    @pl.loop(0, 6)
    def _(h):
        p, hh = h // 2, lax.rem(h, 2)
        qrow, krow, vrow = (rows(at + hh * 64, 64) for at in (0, 128, 256))
        orow = rows(k * 384 + h * 64, 64)

        @pl.when(h >= 2)
        def _():
            pltpu.make_async_copy(probs.at[hh], keep.at[h - 2], rs_.at[names["e0"] + 2 * (h - 2)]).wait()

        s = dims(qk[p, krow, :], qk[p, qrow, :], 0, 0) + big[:, 0:1024]
        e = jnp.exp(s - jnp.max(s, 0, keepdims=True))
        r = 1.0 / jnp.sum(e, 0, keepdims=True)
        eb = e.astype(bf16)
        probs[hh] = eb
        otb[orow, :] = (times(qk[p, vrow, :], eb) * r).astype(bf16)
        rl[pl.ds(h, 1), :] = r
        pltpu.make_async_copy(probs.at[hh], keep.at[h], rs_.at[names["e0"] + 2 * h]).start()
        pltpu.make_async_remote_copy(
            src_ref=otb.at[orow, :], dst_ref=otb.at[orow, :], send_sem=sends.at[first_send + h],
            recv_sem=rs_.at[names["o0"] + 2 * h], device_id=(pn, z), device_id_type=MESH,
        ).start()
        for at, step in forward_steps.items():
            pl.when(h == at)(lambda step=step: step() and None)

    for h in range(6):
        drains.append((first_send + h, otb.at[pl.ds(0, 64), :], None))

    for u in range(2, 6):
        weight_here(u)
    arrived(spare, "cm")
    for h in range(6):
        arrived(otb.at[rows(other * 384 + h * 64, 64), :], f"o{h}")
    arrived(probs.at[0], "e4")
    arrived(probs.at[1], "e5")

    mine = rows(k * 512, 512)
    theirs = rows(other * 512, 512)
    my_lanes = lanes(k * 512, 512)
    ot_mine = otb[:, my_lanes]
    x1[:, 0:384] = xs[mine, 0:384].astype(f32) + dims(ot_mine, wa[0], 0, 0)
    x1[:, 384:768] = xs[mine, 384:768].astype(f32) + dims(ot_mine, wa[1], 0, 0)
    xx = x1[...]
    c = xx - jnp.mean(xx, -1, keepdims=True)
    n = c * lax.rsqrt(jnp.mean(c * c, -1, keepdims=True) + norm_eps)
    h2[mine, :] = (n * grow[1:2, :]).astype(bf16)
    send(h2.at[mine, :], h2.at[mine, :], "h2", (pn, z))
    share_activation(dys, "ay")
    for o, w in ((0, 512), (512, 512), (1024, 128)):
        cols = pl.ds(o, w)
        a = times(h2[mine, :], wi[0, :, cols])
        b = times(h2[mine, :], wi[1, :, cols])
        phi = 0.5 * (1.0 + lax.erf(a * 0.7071067811865476))
        gelu = a * phi
        e = times(dys[mine, :], wm[:, cols])
        hid[:, cols] = (gelu * b).astype(bf16)
        dgo[0, :, cols] = (e * (b * (phi + a * (jnp.exp(-0.5 * a * a) * 0.3989422804014327)))).astype(bf16)
        dgo[1, :, cols] = (e * gelu).astype(bf16)
    send(hid.at[:, lanes(other * 512, 640)], hidp, "hid", (pn, z))
    send(dgo.at[other], dgp, "dg", (pn, z))

    shared_activation(dys, "ay")
    arrived(hidp, "hid")
    t = (
        dims(dys[mine, :], hid[:, lanes(k * 512, 640)], 0, 0) + dims(dys[theirs, :], hidp[...], 0, 0)
    ).astype(bf16)

    @pl.when(k == 0)
    def _():
        grad[:, MLP : MLP + 512] = t[:, 0:512]
        grad[:, 0:128] = t[:, 512:640]

    @pl.when(k == 1)
    def _():
        grad[:, MLP : MLP + 512] = t[:, 128:640]

    s1("m")
    lo[...] = (x1[...] + dims(hid[...], wm[...], 1, 1)).astype(bf16)
    give_back(lo, lo_out, "alo")
    arrived(h2.at[theirs, :], "h2")
    arrived(dgp, "dg")
    for name, o, w in (("i0", 0, 640), ("i1", 640, 512)):
        cols = pl.ds(o, w)
        grad[:, IN + o : IN + o + w] = (
            dims(h2[mine, :], dgo[k, :, cols], 0, 0) + dims(h2[theirs, :], dgp[:, cols], 0, 0)
        ).astype(bf16)
        if name == "i0":
            s1(name)
    f2 = dims(dgo[0], wi[0], 1, 1) + dims(dgo[1], wi[1], 1, 1)
    xx = x1[...]
    c = xx - jnp.mean(xx, -1, keepdims=True)
    r2 = lax.rsqrt(jnp.mean(c * c, -1, keepdims=True) + norm_eps)
    n = c * r2
    grow[3:4, :] = jnp.sum(f2 * n, 0, keepdims=True)
    cc = f2 * grow[1:2, :]
    dx = dys[mine, :].astype(f32) + r2 * (
        cc - jnp.mean(cc, -1, keepdims=True) - n * jnp.mean(cc * n, -1, keepdims=True)
    )
    x1[...] = dx
    dx1b[...] = dx.astype(bf16)
    send(dx1b.at[:, lanes(other * 384, 384)], dx1bp, "dx1b", (pn, z))
    for part in range(2):
        which = other if part == 0 else k
        col = lanes(which * 384, 384)
        feat = rows(which * 384, 384)
        left = jnp.concatenate([wa[0, feat, :], wa[1, feat, :]], axis=1)
        t = dims(left, dx1b[...], 1, 1).astype(bf16)
        if part == 0:
            dot_send[...] = t
            send(dot_send, dot_own.at[:, my_lanes], "do", (pn, z))
        else:
            dot_own[:, my_lanes] = t
    local(keep.at[5], probs.at[1], "e5")
    local(keep.at[4], probs.at[0], "e4")

    s2("m")
    s1("i1")
    arrived(dx1bp, "dx1b")
    grad[:, ATTN : ATTN + 384] = (
        times(otb[:, my_lanes], dx1b[:, lanes(k * 384, 384)])
        + times(otb[:, lanes(other * 512, 512)], dx1bp[...])
    ).astype(bf16)
    arrived(dot_own.at[:, lanes(other * 512, 512)], "do")

    for h in range(6):
        rsem(f"b{h}")
    backward_steps = {
        4: lambda: (s2("i0"), s3("m")),
        3: lambda: (s2("i1"), s1("a"), s1("q2")),
        2: lambda: (s1("q1"), s3("i0"), s4("m")),
        1: lambda: s3("i1"),
        0: lambda: (s2("a"), s1("q0"), s4("i0")),
    }

    @pl.loop(0, 6)
    def _(turn):
        h = 5 - turn
        p, hh = h // 2, lax.rem(h, 2)
        qrow, krow, vrow = (rows(at + hh * 64, 64) for at in (0, 128, 256))
        arrived_at = rs_.at[names["e0"] + 2 * h]
        pltpu.make_async_copy(keep.at[h], probs.at[hh], arrived_at).wait()
        vt = qk[p, vrow, :]
        kt = qk[p, krow, :]
        for i in range(2):
            cols = slice(i * 512, i * 512 + 512)
            do = dot_own[rows(h * 64, 64), cols].astype(f32) * rl[pl.ds(h, 1), cols]
            delta = jnp.sum(do * otb[rows(k * 384 + h * 64, 64), cols].astype(f32), 0, keepdims=True)
            dob = do.astype(bf16)
            e = probs[hh, :, cols]
            ds = (e.astype(f32) * (dims(vt, dob, 0, 0) - delta)).astype(bf16)
            dk = dims(qk[p, qrow, cols], ds, 1, 1)
            dv = dims(dob, e, 1, 1)
            if i == 0:
                dkb[...] = dk
                dvb[...] = dv
            else:
                dkb[...] += dk
                dvb[...] += dv
            dq = times(kt, ds) * HEAD_DIM**-0.5
            c = cosr[:, cols]
            s = sinr[:, cols]
            qk[p, rows(hh * 64, 32), cols] = (dq[:32] * c + dq[32:] * s).astype(bf16)
            qk[p, rows(hh * 64 + 32, 32), cols] = (dq[32:] * c - dq[:32] * s).astype(bf16)

        @pl.when(h >= 2)
        def _():
            pltpu.make_async_copy(keep.at[h - 2], probs.at[hh], rs_.at[names["e0"] + 2 * (h - 2)]).start()

        d = dkb[...]
        c = cosr[...]
        s = sinr[...]
        qk[p, rows(128 + hh * 64, 32), :] = (d[:32] * c + d[32:] * s).astype(bf16)
        qk[p, rows(160 + hh * 64, 32), :] = (d[32:] * c - d[:32] * s).astype(bf16)
        qk[p, vrow, :] = dvb[...].astype(bf16)

        @pl.when(hh == 0)
        def _():
            grad[:, lanes(PAIR + 384 * p, 384)] = dims(h1t[...], qk[p], 1, 1).astype(bf16)

        for at, step in backward_steps.items():
            pl.when(h == at)(lambda step=step: step() and None)

    def f1_part(cols):
        return times(wq[0], qk[0, :, cols]) + times(wq[1], qk[1, :, cols]) + times(wq[2], qk[2, :, cols])

    big[0:768, 0:512] = f1_part(lanes(other * 512, 512))
    send(big.at[pl.ds(0, 768), pl.ds(0, 512)], f1r, "f1", (pn, z))
    s2("q2")
    big[0:768, 512:1024] = f1_part(my_lanes)
    s4("i1")
    arrived(f1r, "f1")
    f1 = (big[0:768, 512:1024] + f1r[...]).T
    xx = xs[mine, :].astype(f32)
    c = xx - jnp.mean(xx, -1, keepdims=True)
    r1 = lax.rsqrt(jnp.mean(c * c, -1, keepdims=True) + norm_eps)
    n = c * r1
    grow[2:3, :] = jnp.sum(f1 * n, 0, keepdims=True)
    cc = f1 * grow[0:1, :]
    gi[...] = (
        x1[...] + r1 * (cc - jnp.mean(cc, -1, keepdims=True) - n * jnp.mean(cc * n, -1, keepdims=True))
    ).astype(bf16)
    send(grow, growp, "gr", (pn, z), when=lambda: k == 0)

    @pl.when(k == 1)
    def _():
        arrived(growp, "gr")
        two = jnp.concatenate([grow[2:4, :] + growp[2:4, :], jnp.zeros((126, 768), f32)], axis=0)
        grad[:, 0:128] = two.T.astype(bf16)

    s1("g")
    give_back(gi, gi_out, "agi", (0,))
    s2("q1")
    s3("a")
    s5("m")
    give_back(gi, gi_out, "agi", (1,))
    s2("q0")
    s4("a")
    s3("q2")
    s2("g")
    s3("q1")
    s5("i0")
    s3("q0")
    s4("q2")
    s3("g")
    s4("q1")
    s4("q0")
    s5("i1")
    s5("a")
    s4("g")
    s5("q2")
    s5("q1")
    s5("q0")
    s5("g")
    for u in REDUCE:
        s6(u)
    given_back(lo_out, "alo")
    given_back(gi_out, "agi")
    drain_all()
    assert len(names) <= 160 and count["send"] <= 220 and len(packing) <= 32


frequency = np.broadcast_to(
    (np.float32(rope_base) ** (-(np.arange(32, dtype=np.float32) * 2) / HEAD_DIM))[:, None], (32, 128)
).astype(np.float32)


def finish_kernel(
    lo_raw, gi_raw, gp_raw, lo, gi, o_qkv, o_attn, o_in, o_mlp, o_one, o_two,
    buf, gp, g_qkv, g_attn, g_in, g_mlp, g_one, g_two, sem,
):
    loads = [
        pltpu.make_async_copy(src, dst, sem.at[i])
        for i, (src, dst) in enumerate(((gp_raw, gp), (lo_raw, buf.at[0]), (gi_raw, buf.at[1])))
    ]
    for copy in loads:
        copy.start()
    pairs = ((buf.at[0], lo), (buf.at[1], gi), (g_qkv, o_qkv), (g_attn, o_attn), (g_in, o_in), (g_mlp, o_mlp), (g_one, o_one), (g_two, o_two))
    stores = [pltpu.make_async_copy(src, dst, sem.at[3 + i]) for i, (src, dst) in enumerate(pairs)]
    loads[0].wait()
    for c in range(2):
        for p in range(3):
            for t in range(3):
                o = 768 * t + 384 * c + 128 * p
                at = PAIR + 384 * p + 128 * t
                g_qkv[:, o : o + 128] = gp[c, :, at : at + 128]
        g_attn[:, 384 * c : 384 * c + 384] = gp[c, :, ATTN : ATTN + 384]
        g_in[:, 1152 * c : 1152 * c + 1152] = gp[c, :, IN : IN + 1152]
    g_mlp[:, 0:512] = gp[0, :, MLP : MLP + 512]
    g_mlp[:, 512:640] = gp[0, :, 0:128]
    g_mlp[:, 640:1152] = gp[1, :, MLP : MLP + 512]
    flat = jnp.concatenate([gp[1, :, 0:128], jnp.zeros((104, 128), f32)], axis=0).T
    g_one[...] = flat[0:1, 0:24]
    g_two[...] = flat[1:2, 0:24]
    for load, store in zip(loads[1:], stores[:2]):
        load.wait()
        store.start()
    for store in stores[2:]:
        store.start()
    for store in stores:
        store.wait()


def fast(layer_in, seg_start, out_grad, w_qkv, w_attn_out, w_in, w_mlp_out, norm_attn, norm_mlp):
    hbm = pl.BlockSpec(memory_space=pltpu.HBM)
    vmem = pl.BlockSpec(memory_space=pltpu.VMEM)
    V = pltpu.VMEM
    outs = pl.pallas_call(
        step_kernel,
        name="layer",
        out_shape=[
            jax.ShapeDtypeStruct((2, 256, 768), bf16),
            jax.ShapeDtypeStruct((2, 256, 768), bf16),
            jax.ShapeDtypeStruct((2, 24, WIDTH), f32),
            jax.ShapeDtypeStruct((768, WIDTH), bf16),
            jax.ShapeDtypeStruct((6, 1024, 1024), bf16),
        ],
        in_specs=[hbm, hbm, vmem, hbm, hbm, hbm, hbm, vmem, vmem, vmem],
        out_specs=[hbm] * 5,
        scratch_shapes=[
            V((2, 24, WIDTH), bf16),
            V((8, 128), f32),
            V((1024, 768), bf16),
            V((1024, 768), bf16),
            V((1, 1024), jnp.int32),
            V((768, 1024), bf16),
            V((3, 768, 384), bf16),
            V((2, 768, 384), bf16),
            V((2, 768, 1152), bf16),
            V((768, 1152), bf16),
            V((768, 128), bf16),
            V((32, 1024), f32),
            V((32, 1024), f32),
            V((3, 384, 1024), bf16),
            V((1024, 1152), f32),
            V((2, 1024, 1024), bf16),
            V((768, 1024), bf16),
            V((8, 1024), f32),
            V((512, 768), f32),
            V((1024, 768), bf16),
            V((512, 1152), bf16),
            V((512, 640), bf16),
            V((2, 512, 1152), bf16),
            V((512, 1152), bf16),
            V((512, 768), bf16),
            V((512, 384), bf16),
            V((384, 512), bf16),
            V((384, 1024), bf16),
            V((768, 512), f32),
            V((512, 768), bf16),
            V((512, 768), bf16),
            V((768, WIDTH), bf16),
            V((8, 768), f32),
            V((8, 768), f32),
            V((64, 1024), f32),
            V((64, 1024), f32),
            V((2, 96, WIDTH), bf16),
            V((2, 96, WIDTH), bf16),
            V((96, WIDTH), bf16),
            V((96, WIDTH), bf16),
            V((2, 4, 24, WIDTH), bf16),
            V((2, 24, WIDTH), bf16),
            V((2, 2, 24, WIDTH), bf16),
            V((2, 24, WIDTH), bf16),
            V((2, 24, WIDTH), f32),
            pltpu.SemaphoreType.DMA((160,)),
            pltpu.SemaphoreType.DMA((32,)),
            pltpu.SemaphoreType.DMA((220,)),
        ],
        compiler_params=pltpu.CompilerParams(
            collective_id=0, has_side_effects=True, vmem_limit_bytes=67043328
        ),
    )(
        layer_in, out_grad, seg_start, w_qkv, w_attn_out, w_in, w_mlp_out,
        norm_attn[None], norm_mlp[None], frequency,
    )
    done = pl.pallas_call(
        finish_kernel,
        name="finish",
        out_shape=[
            jax.ShapeDtypeStruct((2, 256, 768), bf16),
            jax.ShapeDtypeStruct((2, 256, 768), bf16),
            jax.ShapeDtypeStruct((24, 2304), f32),
            jax.ShapeDtypeStruct((24, 768), f32),
            jax.ShapeDtypeStruct((24, 2304), f32),
            jax.ShapeDtypeStruct((24, 1152), f32),
            jax.ShapeDtypeStruct((1, 24), f32),
            jax.ShapeDtypeStruct((1, 24), f32),
        ],
        in_specs=[hbm, hbm, hbm],
        out_specs=[hbm] * 8,
        scratch_shapes=[
            V((2, 2, 256, 768), bf16),
            V((2, 24, WIDTH), f32),
            V((24, 2304), f32),
            V((24, 768), f32),
            V((24, 2304), f32),
            V((24, 1152), f32),
            V((1, 24), f32),
            V((1, 24), f32),
            pltpu.SemaphoreType.DMA((11,)),
        ],
    )(*outs[:3])
    return (*done[:6], done[6][0], done[7][0])


def normalize(values):
    centered = values - jnp.mean(values, axis=-1, keepdims=True)
    spread = jnp.mean(centered * centered, axis=-1, keepdims=True)
    return centered * lax.rsqrt(spread + norm_eps)


def rope_tables(positions):
    half_dim = HEAD_DIM // 2
    frequency = rope_base ** (-(jnp.arange(half_dim).astype(jnp.float32) * 2.0) / HEAD_DIM)
    angles = positions.astype(jnp.float32)[:, None] * frequency[None, :]
    angles = jnp.concatenate([angles, angles], axis=-1)
    return (jnp.cos(angles), jnp.sin(angles))


def turn_half(values):
    half_dim = values.shape[-1] // 2
    return jnp.concatenate([-values[..., half_dim:], values[..., :half_dim]], axis=-1)


def rotate(values, cosine_table, sine_table):
    return values * cosine_table[:, None, :] + turn_half(values) * sine_table[:, None, :]


def unrotate(values, cosine_table, sine_table):
    return values * cosine_table[:, None, :] - turn_half(values) * sine_table[:, None, :]


def product(left, right):
    return jnp.dot(left, right, preferred_element_type=jnp.float32)


def left_transposed(left, right):
    return lax.dot_general(
        left, right, (((0,), (0,)), ((), ())), preferred_element_type=jnp.float32
    )


def right_transposed(left, right):
    return lax.dot_general(
        left, right, (((1,), (1,)), ((), ())), preferred_element_type=jnp.float32
    )


def to_groups(array):
    row_count, head_count, head_size = array.shape
    return array.reshape(row_count, head_count // 4, 4, head_size).transpose(1, 0, 2, 3)


def from_groups(array):
    group_count, row_count, group_heads, head_size = array.shape
    return array.transpose(1, 0, 2, 3).reshape(row_count, group_count * group_heads, head_size)


def attend_group(group_in, same_doc):
    query_part, key_part, value_part = group_in
    scores = jnp.einsum(
        "qhd,khd->hqk", query_part, key_part, preferred_element_type=jnp.float32
    ) * HEAD_DIM ** (-0.5)
    masked = jnp.where(same_doc[None], scores, neg_large)
    highest = jnp.max(masked, axis=-1, keepdims=True)
    shifted = jnp.exp(masked - highest)
    totals = jnp.sum(shifted, axis=-1, keepdims=True)
    attn_prob = shifted / totals
    log_total = highest + jnp.log(totals)
    mixed_out = jnp.einsum(
        "hqk,khd->qhd",
        attn_prob.astype(jnp.bfloat16),
        value_part,
        preferred_element_type=jnp.float32,
    )
    return (mixed_out, log_total[..., 0])


def attend_back(group_in, same_doc):
    query_part, key_part, value_part, grad_part, log_total = group_in
    scores = jnp.einsum(
        "qhd,khd->hqk", query_part, key_part, preferred_element_type=jnp.float32
    ) * HEAD_DIM ** (-0.5)
    attn_prob = jnp.where(same_doc[None], jnp.exp(scores - log_total[..., None]), 0.0)
    grad_prob = jnp.einsum(
        "qhd,khd->hqk", grad_part, value_part, preferred_element_type=jnp.float32
    )
    inner_sum = jnp.sum(attn_prob * grad_prob, axis=-1, keepdims=True)
    grad_score = (attn_prob * (grad_prob - inner_sum)).astype(jnp.bfloat16)
    grad_query = jnp.einsum(
        "hqk,khd->qhd", grad_score, key_part, preferred_element_type=jnp.float32
    ) * HEAD_DIM ** (-0.5)
    grad_key = jnp.einsum(
        "hqk,qhd->khd", grad_score, query_part, preferred_element_type=jnp.float32
    ) * HEAD_DIM ** (-0.5)
    grad_value = jnp.einsum(
        "hqk,qhd->khd",
        attn_prob.astype(jnp.bfloat16),
        grad_part,
        preferred_element_type=jnp.float32,
    )
    return (grad_query, grad_key, grad_value)


def scaled_norm(values_in, gain_row):
    return normalize(values_in) * gain_row


def geglu(first_half, second_half):
    return jax.nn.gelu(first_half, approximate=False) * second_half


def local(layer_in, seg_start, out_grad, w_qkv, w_attn_out, w_in, w_mlp_out, norm_attn, norm_mlp):
    micro_count = layer_in.shape[0]
    span_len = layer_in.shape[1]
    model_width = layer_in.shape[2]
    ctx_rank = lax.axis_index("ctx")
    grad_sums = (
        jnp.zeros((model_width, 3 * model_width), jnp.float32),
        jnp.zeros((model_width, model_width), jnp.float32),
        jnp.zeros((model_width, 2 * FF), jnp.float32),
        jnp.zeros((model_width, FF), jnp.float32),
        jnp.zeros((model_width,), jnp.float32),
        jnp.zeros((model_width,), jnp.float32),
    )
    offsets = ctx_rank * span_len + jnp.arange(span_len, dtype=jnp.int32)
    outputs = []
    grad_inputs = []
    for micro_step in range(micro_count):
        gathered = (
            lax.all_gather(w_qkv, ("dp", "ctx"), axis=0, tiled=True),
            lax.all_gather(w_attn_out, ("dp", "ctx"), axis=0, tiled=True),
            lax.all_gather(w_in, ("dp", "ctx"), axis=0, tiled=True),
            lax.all_gather(w_mlp_out, ("dp", "ctx"), axis=0, tiled=True),
            lax.all_gather(norm_attn, ("dp", "ctx"), axis=0, tiled=True),
            lax.all_gather(norm_mlp, ("dp", "ctx"), axis=0, tiled=True),
        )
        qkv_full, attn_full, in_full, mlp_full, gain_attn, gain_mlp = gathered
        starts_here = seg_start[micro_step]
        hidden = layer_in[micro_step].astype(jnp.float32)
        cosine_table, sine_table = rope_tables(offsets - starts_here)
        normed, norm_back = jax.vjp(scaled_norm, hidden, gain_attn.astype(jnp.float32))
        normed_low = normed.astype(jnp.bfloat16)
        qkv_local = product(normed_low, qkv_full).reshape(span_len, 3, HEADS, HEAD_DIM)
        queries = rotate(qkv_local[:, 0], cosine_table, sine_table).astype(jnp.bfloat16)
        keys_here = rotate(qkv_local[:, 1], cosine_table, sine_table).astype(jnp.bfloat16)
        values_here = qkv_local[:, 2].astype(jnp.bfloat16)
        keys_all, values_all, starts_all = (
            lax.all_gather(keys_here, "ctx", axis=0, tiled=True),
            lax.all_gather(values_here, "ctx", axis=0, tiled=True),
            lax.all_gather(starts_here, "ctx", axis=0, tiled=True),
        )
        same_doc = starts_here[:, None] == starts_all[None, :]
        query_groups = to_groups(queries)
        key_groups = to_groups(keys_all)
        value_groups = to_groups(values_all)
        mixed_out, log_total = lax.map(
            lambda group_in: attend_group(group_in, same_doc),
            (query_groups, key_groups, value_groups),
        )
        attended = from_groups(mixed_out).reshape(span_len, model_width).astype(jnp.bfloat16)
        middle = hidden + product(attended, attn_full)
        normed_mlp, norm_mlp_back = jax.vjp(scaled_norm, middle, gain_mlp.astype(jnp.float32))
        normed_mlp_low = normed_mlp.astype(jnp.bfloat16)
        projected = product(normed_mlp_low, in_full)
        gated_out, geglu_back = jax.vjp(geglu, projected[:, :FF], projected[:, FF:])
        gated_low = gated_out.astype(jnp.bfloat16)
        result = middle + right_transposed(gated_low, mlp_full)
        outputs.append(result.astype(jnp.bfloat16))
        qkv_full, attn_full, in_full, mlp_full = (
            lax.all_gather(w_qkv, ("dp", "ctx"), axis=0, tiled=True),
            lax.all_gather(w_attn_out, ("dp", "ctx"), axis=0, tiled=True),
            lax.all_gather(w_in, ("dp", "ctx"), axis=0, tiled=True),
            lax.all_gather(w_mlp_out, ("dp", "ctx"), axis=0, tiled=True),
        )
        grad_out = out_grad[micro_step].astype(jnp.float32)
        grad_out_low = out_grad[micro_step]
        grad_mlp_weight = left_transposed(grad_out_low, gated_low)
        grad_gated = product(grad_out_low, mlp_full)
        grad_first, grad_second = geglu_back(grad_gated)
        grad_projected = jnp.concatenate([grad_first, grad_second], axis=1).astype(jnp.bfloat16)
        grad_in_weight = left_transposed(normed_mlp_low, grad_projected)
        grad_normed_mlp = right_transposed(grad_projected, in_full)
        grad_middle_norm, grad_gain_mlp = norm_mlp_back(grad_normed_mlp)
        grad_middle = grad_out + grad_middle_norm
        grad_middle_low = grad_middle.astype(jnp.bfloat16)
        grad_attn_weight = left_transposed(attended, grad_middle_low)
        grad_attended = (
            right_transposed(grad_middle_low, attn_full)
            .astype(jnp.bfloat16)
            .reshape(span_len, HEADS, HEAD_DIM)
        )
        grad_groups = to_groups(grad_attended)
        grad_query_groups, grad_key_groups, grad_value_groups = lax.map(
            lambda group_in: attend_back(group_in, same_doc),
            (query_groups, key_groups, value_groups, grad_groups, log_total),
        )
        keys_total = keys_all.shape[0]
        grad_keys, grad_values = (
            lax.psum_scatter(
                from_groups(grad_key_groups).reshape(keys_total, model_width).astype(jnp.bfloat16),
                "ctx",
                scatter_dimension=0,
                tiled=True,
            ).astype(jnp.float32),
            lax.psum_scatter(
                from_groups(grad_value_groups)
                .reshape(keys_total, model_width)
                .astype(jnp.bfloat16),
                "ctx",
                scatter_dimension=0,
                tiled=True,
            ).astype(jnp.float32),
        )
        grad_qkv = jnp.stack(
            [
                unrotate(from_groups(grad_query_groups), cosine_table, sine_table),
                unrotate(grad_keys.reshape(span_len, HEADS, HEAD_DIM), cosine_table, sine_table),
                grad_values.reshape(span_len, HEADS, HEAD_DIM),
            ],
            axis=1,
        )
        grad_qkv = grad_qkv.reshape(span_len, 3 * model_width).astype(jnp.bfloat16)
        grad_qkv_weight = left_transposed(normed_low, grad_qkv)
        grad_normed = right_transposed(grad_qkv, qkv_full)
        grad_hidden_norm, grad_gain_attn = norm_back(grad_normed)
        grad_inputs.append((grad_middle + grad_hidden_norm).astype(jnp.bfloat16))
        grad_sums = (
            grad_sums[0] + grad_qkv_weight,
            grad_sums[1] + grad_attn_weight,
            grad_sums[2] + grad_in_weight,
            grad_sums[3] + grad_mlp_weight,
            grad_sums[4] + grad_gain_attn,
            grad_sums[5] + grad_gain_mlp,
        )
    shares = (
        lax.psum_scatter(grad_sums[0], ("dp", "ctx"), scatter_dimension=0, tiled=True),
        lax.psum_scatter(grad_sums[1], ("dp", "ctx"), scatter_dimension=0, tiled=True),
        lax.psum_scatter(grad_sums[2], ("dp", "ctx"), scatter_dimension=0, tiled=True),
        lax.psum_scatter(grad_sums[3], ("dp", "ctx"), scatter_dimension=0, tiled=True),
        lax.psum_scatter(grad_sums[4], ("dp", "ctx"), scatter_dimension=0, tiled=True),
        lax.psum_scatter(grad_sums[5], ("dp", "ctx"), scatter_dimension=0, tiled=True),
    )
    return (
        jnp.stack(outputs),
        jnp.stack(grad_inputs),
        shares[0],
        shares[1],
        shares[2],
        shares[3],
        shares[4],
        shares[5],
    )


def solution(mesh):
    A = P(None, ("dp", "ctx"), None)
    S = P(None, ("dp", "ctx"))
    W = P(("dp", "ctx"), None)
    G = P(("dp", "ctx"))
    return jax.shard_map(
        fast if dict(mesh.shape) == {"dp": 8, "ctx": 4} else local,
        mesh=mesh,
        in_specs=(A, S, A, W, W, W, W, G, G),
        out_specs=(A, A, W, W, W, W, G, G),
        check_vma=False,
    )
```

```python
import contextlib

import jax
import jax.numpy as jnp
import numpy as np
from jax import lax
from jax.experimental import pallas as pl
from jax.experimental.pallas import tpu as pltpu
from jax.sharding import PartitionSpec as P

MESH = pl.DeviceIdType.MESH
bf16 = jnp.bfloat16
f32 = jnp.float32

HEADS = 12
HEAD_DIM = 64
FF = 1152
rope_base = 160000.0
norm_eps = 1e-05
neg_large = -1e30

WIDTH = 3328
GATHER = [(0, 512), (512, 768), (1280, 384), (1664, 640), (2304, 512), (2816, 512)]
PAIR = 128
ATTN = 1280
IN = 1664
MLP = 2816
REDUCE = {
    "m": (2816, 512),
    "i0": (1664, 640),
    "i1": (2304, 512),
    "a": (1280, 384),
    "q2": (896, 384),
    "q1": (512, 384),
    "q0": (128, 384),
    "g": (0, 128),
}


TRACE = False


def scope(name):
    return jax.named_scope(name) if TRACE else contextlib.nullcontext()


def scoped(fn):
    def inner(*args):
        with scope(f"{fn.__name__}_{args[0] if args and isinstance(args[0], (int, str)) else ''}"):
            return fn(*args)

    return inner


def dims(left, right, left_at, right_at):
    return lax.dot_general(
        left, right, (((left_at,), (right_at,)), ((), ())), preferred_element_type=f32
    )


def times(left, right):
    return jnp.dot(left, right, preferred_element_type=f32)


def step_kernel(
    x_in, dy_in, seg_in, w_qkv, w_attn, w_in, w_mlp, g_attn, g_mlp, freq,
    lo_out, gi_out, gp_out, land, keep,
    wp, gcol,
    xs, dys, sg, h1t, wq, wa, wi, wm, gains, cosr, sinr, qk, big, probs, otb, rl, x1, h2, hid, hidp,
    dgo, dgp, dx1b, dx1bp, dot_send, dot_own, f1r, lo, gi, grad, grow, growp, dkb, dvb,
    ra, rb, ra2, rb2, zs, zp, zm, zx, fin,
    rs_, ls_, sends,
):
    dp = lax.axis_index("dp")
    z = lax.axis_index("ctx")
    q = dp // 2
    k = lax.rem(dp, 2)
    other = 1 - k
    pn = dp + 1 - 2 * k
    xn = dp + 2 - 4 * lax.rem(dp // 2, 2)
    yn = dp + 4 - 8 * (dp // 4)
    zn = z + 1 - 2 * lax.rem(z, 2)
    zb = jnp.where(z < 2, 2, 1)
    zh = z // 2
    qx = q + 1 - 2 * lax.rem(q, 2)
    qy = q + 2 - 4 * (q // 2)
    qd = qx + 2 - 4 * (qx // 2)
    inner = jnp.logical_or(z == 1, z == 2)
    outer = jnp.logical_or(z == 0, z == 3)
    near = k == zh
    away = k != zh
    names = {}
    count = {"send": 0, "local": 0}
    drains = []

    def rsem(name):
        return rs_.at[names.setdefault(name, len(names))]

    def still(view):
        index = view.transforms[0].indices
        return view.ref.at[tuple(pl.ds(0, at.size) if hasattr(at, "size") else 0 for at in index)]

    keyed = {}

    def send(src, dst, name, dev, when=None, sem=None, key=None):
        first = key is None or key not in keyed
        if first:
            i = count["send"]
            count["send"] += 1
            keyed[key] = i
        else:
            i = keyed[key]
        copy = pltpu.make_async_remote_copy(
            src_ref=src, dst_ref=dst, send_sem=sends.at[i], recv_sem=rsem(name) if sem is None else sem,
            device_id=dev, device_id_type=MESH,
        )
        if when is None:
            copy.start()
        else:
            pl.when(when())(copy.start)
        if first:
            drains.append((i, src, when))

    def drain_all():
        for i, src, when in drains:
            view = still(src) if hasattr(src, "transforms") else src

            def wait(view=view, i=i):
                pltpu.make_async_copy(view, view, sends.at[i]).wait()

            if when is None:
                wait()
            else:
                pl.when(when())(wait)

    def local(src, dst, name):
        copy = pltpu.make_async_copy(src, dst, rsem(name))
        copy.start()
        return copy

    def arrived(ref, name):
        pltpu.make_async_copy(ref, ref, rsem(name)).wait()

    def rows(start, size):
        return pl.ds(pl.multiple_of(start, 8), size)

    def lanes(start, size):
        return pl.ds(pl.multiple_of(start, 128), size)

    barrier = pltpu.get_barrier_semaphore()
    for dz in range(1, 4):
        for kk in range(2):
            pl.semaphore_signal(
                barrier, inc=1, device_id=(2 * q + kk, lax.rem(z + dz, 4)), device_id_type=MESH
            )
    for dev in (pn, xn, yn):
        pl.semaphore_signal(barrier, inc=1, device_id=(dev, z), device_id_type=MESH)

    packs = []
    for c in range(2):
        for p in range(3):
            for t in range(3):
                packs.append((w_qkv, 768 * t + 384 * c + 128 * p, c, PAIR + 384 * p + 128 * t, 128))
        packs.append((w_attn, 384 * c, c, ATTN, 384))
        packs.append((w_in, 1152 * c, c, IN, 1152))
        packs.append((w_mlp, 640 * c, c, MLP, 512))
    packs.append((w_mlp, 512, 0, 0, 128))
    packing = [
        pltpu.make_async_copy(w.at[:, pl.ds(o, n)], wp.at[c, :, pl.ds(at, n)], ls_.at[i])
        for i, (w, o, c, at, n) in enumerate(packs)
    ]
    for copy in packing:
        copy.start()
    gcol[...] = jnp.zeros_like(gcol)
    gcol[0:1, 0:24] = g_attn[...].astype(f32)
    gcol[1:2, 0:24] = g_mlp[...].astype(f32)
    columns = jnp.concatenate([gcol[...], jnp.zeros((120, 128), f32)], axis=0).T[0:24].astype(bf16)
    wp[1, :, 0:128] = columns

    @scoped
    def zstage(u, turn=None):
        o, w = GATHER[u]
        cols = pl.ds(o, w)

        def body():
            dst = land.at[rows(dp * 96 + z * 24, 24), cols]
            for c in range(2):
                src = wp.at[c, :, cols]
                send(src, dst, f"z{u}", (2 * q + c, zn), key=f"zn{u}{c}")
                send(src, dst, f"z{u}", (2 * q + c, zb), key=f"zb{u}{c}")
                send(src, dst, f"z{u}", (pn, z), when=lambda c=c: k != c, key=f"zp{u}{c}")
                pl.when(k == c)(lambda src=src: local(src, dst, f"z{u}") and None)

        in_turn(turn, body)

    def in_turn(turn, body):
        if turn is None:
            body()
        else:
            pl.when(turn)(body)

    @scoped
    def slab_in(u, turn=None):
        o, w = GATHER[u]
        cols = pl.ds(o, w)

        def body():
            arrived(land.at[rows(q * 192, 192), cols], f"z{u}")
            for j in range(2):
                part = land.at[rows((2 * q + j) * 96 + lax.rem(4 - 2 * z + 4, 4) * 24, 48), cols]
                send(part, part, f"z{u}", (dp, zn), when=lambda: inner, key=f"fs{u}{j}")

        in_turn(turn, body)

    @scoped
    def xysend(u):
        o, w = GATHER[u]
        slab = land.at[rows(q * 192, 192), pl.ds(o, w)]
        send(slab, slab, f"x{u}", (xn, z))
        send(slab, slab, f"y{u}", (yn, z))

    @scoped
    def diag(u):
        o, w = GATHER[u]
        cols = pl.ds(o, w)
        arrived(land.at[rows(qx * 192, 192), cols], f"x{u}")
        part = land.at[rows(qx * 192, 96), cols]
        send(part, part, f"dx{u}", (yn, z))
        arrived(land.at[rows(qy * 192, 192), cols], f"y{u}")
        part = land.at[rows(qy * 192 + 96, 96), cols]
        send(part, part, f"dy{u}", (xn, z))

    @scoped
    def done(u):
        o, w = GATHER[u]
        cols = pl.ds(o, w)
        arrived(land.at[rows(qd * 192, 96), cols], f"dx{u}")
        arrived(land.at[rows(qd * 192 + 96, 96), cols], f"dy{u}")

    def activation(src_ref, dst_ref, name, turn=None):
        for m in range(2):
            src = src_ref.at[m]
            dst = dst_ref.at[rows(z * 256, 256), :]
            sem = rs_.at[base[name] + lax.rem(z, 2)]

            def going(m=m):
                there = 2 * k + m != z
                return there if turn is None else jnp.logical_and(turn, there)

            here = 2 * k + m == z
            if turn is not None:
                here = jnp.logical_and(turn, here)
            send(src, dst, None, (2 * q + zh, 2 * k + m), when=going, sem=sem)
            pl.when(here)(pltpu.make_async_copy(src, dst, sem).start)

    base = {}
    for name in ("ax", "ay", "alo", "agi"):
        base[name] = len(names)
        names[name + "0"] = len(names)
        names[name + "1"] = len(names)

    @scoped
    def share_activation(ref, name, turn=None):
        def body():
            for j in range(2):
                r = rows(k * 512 + j * 256, 256)
                arrived(ref.at[r, :], f"{name}{j}")
                send(ref.at[r, :], ref.at[r, :], f"p{name}{j}", (pn, z), key=f"sh{name}{j}")

        in_turn(turn, body)

    @scoped
    def shared_activation(ref, name, turn=None):
        def body():
            for j in range(2):
                arrived(ref.at[rows(other * 512 + j * 256, 256), :], f"p{name}{j}")

        in_turn(turn, body)

    @scoped
    def give_back(src_ref, out_ref, name, blocks=(0, 1), turn=None):
        m = lax.rem(z, 2)
        for j in blocks:
            src = src_ref.at[pl.ds(j * 256, 256), :]
            dst = out_ref.at[m]
            sem = rs_.at[base[name] + m]

            def going(j=j):
                leaves = jnp.logical_or(2 * k + j != z, zh != k)
                return leaves if turn is None else jnp.logical_and(turn, leaves)

            stays = jnp.logical_and(2 * k + j == z, zh == k)
            if turn is not None:
                stays = jnp.logical_and(turn, stays)
            send(src, dst, None, (2 * q + zh, 2 * k + j), when=going, sem=sem)
            pl.when(stays)(pltpu.make_async_copy(src, dst, sem).start)

    @scoped
    def given_back(out_ref, name):
        for m in range(2):
            arrived(out_ref.at[m], f"{name}{m}")

    def seg_send():
        for m in range(2):
            src = seg_in.at[pl.ds(m, 1), :]
            dst = sg.at[:, lanes(z * 256, 256)]
            for c in range(2):

                def away(m=m, c=c):
                    return jnp.logical_or(2 * k + m != z, k != c)

                send(src, dst, "seg", (2 * q + c, 2 * k + m), when=away)
                pl.when(jnp.logical_not(away()))(pltpu.make_async_copy(src, dst, rsem("seg")).start)

    @scoped
    def s1(u):
        o, w = REDUCE[u]
        cols = pl.ds(o, w)
        for slot, quarter in enumerate((qx, qd)):
            send(grad.at[rows(quarter * 192, 96), cols], ra.at[slot, :, cols], f"ra{u}", (xn, z))
        for slot, quarter in enumerate((qy, qd)):
            send(grad.at[rows(quarter * 192 + 96, 96), cols], rb.at[slot, :, cols], f"rb{u}", (yn, z))

    @scoped
    def s2(u):
        o, w = REDUCE[u]
        cols = pl.ds(o, w)
        arrived(ra.at[:, :, cols], f"ra{u}")
        r = rows(qy * 192, 96)
        grad[r, cols] = (grad[r, cols].astype(f32) + ra[1, :, cols].astype(f32)).astype(bf16)
        send(grad.at[r, cols], ra2.at[:, cols], f"ra2{u}", (yn, z))
        arrived(rb.at[:, :, cols], f"rb{u}")
        r2 = rows(qx * 192 + 96, 96)
        grad[r2, cols] = (grad[r2, cols].astype(f32) + rb[1, :, cols].astype(f32)).astype(bf16)
        send(grad.at[r2, cols], rb2.at[:, cols], f"rb2{u}", (xn, z))

    @scoped
    def s3(u):
        o, w = REDUCE[u]
        cols = pl.ds(o, w)
        arrived(ra2.at[:, cols], f"ra2{u}")
        arrived(rb2.at[:, cols], f"rb2{u}")
        for j, (one, two) in enumerate(((ra, ra2), (rb, rb2))):
            total = (
                grad[rows(q * 192 + 96 * j, 96), cols].astype(f32)
                + one[0, :, cols].astype(f32)
                + two[:, cols].astype(f32)
            )
            for at in range(4):
                zs[j, at, :, cols] = total[24 * at : 24 * at + 24].astype(bf16)
        send(zs.at[:, zn, :, cols], zp.at[:, :, cols], f"zp{u}", (dp, zn))
        far = 2 * (1 - zh)
        send(zs.at[:, pl.ds(far, 2), :, cols], zm.at[:, :, :, cols], f"zm{u}", (dp, zn), when=lambda: outer)

    @scoped
    def s4(u):
        o, w = REDUCE[u]
        cols = pl.ds(o, w)
        far = 2 * (1 - zh)

        @pl.when(inner)
        def _():
            arrived(zm.at[:, :, :, cols], f"zm{u}")
            for j in range(2):
                for at in range(2):
                    zs[j, far + at, :, cols] = (
                        zs[j, far + at, :, cols].astype(f32) + zm[j, at, :, cols].astype(f32)
                    ).astype(bf16)

        for at in range(2):
            send(zs.at[:, far + at, :, cols], zx.at[:, :, cols], f"zx{u}", (dp, far + at), when=lambda: inner)

    @scoped
    def s5(u):
        o, w = REDUCE[u]
        cols = pl.ds(o, w)
        arrived(zp.at[:, :, cols], f"zp{u}")
        arrived(zx.at[:, :, cols], f"zx{u}")
        for j in range(2):
            fin[j, :, cols] = (
                zs[j, z, :, cols].astype(f32) + zp[j, :, cols].astype(f32) + zx[j, :, cols].astype(f32)
            )
        local(fin.at[k, :, cols], gp_out.at[k, :, cols], f"fl{u}")
        send(fin.at[other, :, cols], gp_out.at[k, :, cols], f"fr{u}", (pn, z))

    @scoped
    def s6(u):
        o, w = REDUCE[u]
        cols = pl.ds(o, w)
        arrived(gp_out.at[k, :, cols], f"fl{u}")
        arrived(gp_out.at[other, :, cols], f"fr{u}")

    pl.semaphore_wait(barrier, 9)

    for copy in packing:
        copy.wait()
    seg_send()
    zstage(0)
    zstage(1)
    activation(x_in, xs, "ax", near)
    zstage(2, outer)
    zstage(3, outer)
    slab_in(0)
    xysend(0)
    slab_in(1)
    xysend(1)
    zstage(2, inner)
    zstage(3, inner)
    zstage(4)
    zstage(5)
    activation(x_in, xs, "ax", away)
    slab_in(2, inner)
    slab_in(3, inner)
    arrived(sg, "seg")
    positions = (lax.broadcasted_iota(jnp.int32, (1, 1024), 1) - sg[...]).astype(f32)
    angles = freq[:, 0:1] * positions
    cosr[...] = jnp.cos(angles)
    sinr[...] = jnp.sin(angles)
    starts = sg[...].astype(f32)
    column = jnp.broadcast_to(starts, (128, 1024)).T

    @pl.loop(0, 8)
    def _(i):
        r = lanes(i * 128, 128)
        here = jnp.broadcast_to(sg[:, r].astype(f32), (1024, 128))
        big[:, r] = jnp.where(column == here, 0.0, neg_large)

    diag(0)
    diag(1)
    slab_in(2, outer)
    xysend(2)
    done(0)
    first = land.at[:, pl.ds(0, 128)]
    spare = wm.at[:, pl.ds(512, 128)]

    @pl.when(k == 0)
    def _():
        local(first, spare, "cm")

    @pl.when(k == 1)
    def _():
        local(first, gains, "cg")

    send(first, spare, "cm", (pn, z), when=lambda: k == 0)
    send(first, gains, "cg", (pn, z), when=lambda: k == 1)
    local(land.at[:, pl.ds(128, 384)], wq.at[0], "cq0")
    arrived(gains, "cg")
    gain_rows = gains[...].astype(f32).T
    grow[...] = gain_rows[0:8]
    done(1)
    local(land.at[:, pl.ds(512, 384)], wq.at[1], "cq1")
    local(land.at[:, pl.ds(896, 384)], wq.at[2], "cq2")

    def queries(half):
        for i in range(2):
            at = half * 512 + i * 256
            xb = xs[rows(at, 256), :].astype(f32)
            c = xb - jnp.mean(xb, -1, keepdims=True)
            n = c * lax.rsqrt(jnp.mean(c * c, -1, keepdims=True) + norm_eps)
            h1t[:, lanes(at, 256)] = (n * grow[0:1, :]).astype(bf16).T

        cols = lanes(half * 512, 512)

        @pl.loop(0, 3)
        def _(p):
            t = times(wq[p].T, h1t[:, cols])
            c = cosr[:, cols]
            s = sinr[:, cols]
            for hh in range(4):
                u1 = t[hh * 64 : hh * 64 + 32]
                u2 = t[hh * 64 + 32 : hh * 64 + 64]
                scale = HEAD_DIM**-0.5 if hh < 2 else 1.0
                qk[p, hh * 64 : hh * 64 + 32, cols] = ((u1 * c - u2 * s) * scale).astype(bf16)
                qk[p, hh * 64 + 32 : hh * 64 + 64, cols] = ((u2 * c + u1 * s) * scale).astype(bf16)
            qk[p, 256:384, cols] = t[256:384].astype(bf16)

    share_activation(xs, "ax", k == zh)
    shared_activation(xs, "ax", k != zh)
    for p in range(3):
        arrived(wq.at[p], f"cq{p}")
    slab_in(4, inner)
    slab_in(5, inner)
    slab_in(3, outer)
    xysend(3)
    with scope("qkvnear"):
        queries(zh)
    diag(2)
    slab_in(4, outer)
    xysend(4)
    share_activation(xs, "ax", k != zh)
    shared_activation(xs, "ax", k == zh)
    with scope("qkvfar"):
        queries(1 - zh)
    slab_in(5, outer)
    xysend(5)
    diag(3)

    @scoped
    def weight_done(u):
        done(u)
        o, w = GATHER[u]
        if u == 2:
            pieces = [(land.at[:, pl.ds(o, w)], wa.at[k], None)]
        elif u == 3:
            pieces = [(land.at[:, pl.ds(o, w)], wi.at[k, :, pl.ds(0, 640)], None)]
        elif u == 4:
            pieces = [(land.at[:, pl.ds(o, w)], wi.at[k, :, pl.ds(640, 512)], None)]
        else:
            pieces = [
                (land.at[:, pl.ds(o, w)], wm.at[:, pl.ds(0, 512)], lambda: k == 0),
                (land.at[:, pl.ds(o, w)], wm.at[:, pl.ds(640, 512)], lambda: k == 1),
            ]
        for src, dst, when in pieces:
            if when is None:
                local(src, dst, f"cw{u}")
            else:
                pl.when(when())(lambda src=src, dst=dst: local(src, dst, f"cw{u}") and None)
            send(src, dst, f"pw{u}", (pn, z), when=when)

    @scoped
    def weight_here(u):
        if u == 2:
            mine, theirs = [(wa.at[k], None)], [(wa.at[other], None)]
        elif u == 3:
            mine, theirs = [(wi.at[k, :, pl.ds(0, 640)], None)], [(wi.at[other, :, pl.ds(0, 640)], None)]
        elif u == 4:
            mine, theirs = [(wi.at[k, :, pl.ds(640, 512)], None)], [(wi.at[other, :, pl.ds(640, 512)], None)]
        else:
            low, high = wm.at[:, pl.ds(0, 512)], wm.at[:, pl.ds(640, 512)]
            mine, theirs = [(low, k == 0), (high, k == 1)], [(low, k == 1), (high, k == 0)]
        for group, name in ((mine, "cw"), (theirs, "pw")):
            for ref, when in group:
                if when is None:
                    arrived(ref, f"{name}{u}")
                else:
                    pl.when(when)(lambda ref=ref, name=name: arrived(ref, f"{name}{u}"))

    for h in range(6):
        rsem(f"e{h}")
        rsem(f"o{h}")
    first_send = count["send"]
    count["send"] += 6
    forward_steps = {
        0: lambda: (activation(dy_in, dys, "ay"), diag(4)),
        2: lambda: (weight_done(2), diag(5)),
        3: lambda: weight_done(3),
        4: lambda: weight_done(4),
        5: lambda: weight_done(5),
    }

    @pl.loop(0, 6)
    def _(h):
        p, hh = h // 2, lax.rem(h, 2)
        qrow, krow, vrow = (rows(at + hh * 64, 64) for at in (0, 128, 256))
        orow = rows(k * 384 + h * 64, 64)

        @pl.when(h >= 2)
        def _():
            pltpu.make_async_copy(probs.at[hh], keep.at[h - 2], rs_.at[names["e0"] + 2 * (h - 2)]).wait()

        s = dims(qk[p, krow, :], qk[p, qrow, :], 0, 0) + big[:, 0:1024]
        e = jnp.exp(s - jnp.max(s, 0, keepdims=True))
        r = 1.0 / jnp.sum(e, 0, keepdims=True)
        eb = e.astype(bf16)
        probs[hh] = eb
        otb[orow, :] = (times(qk[p, vrow, :], eb) * r).astype(bf16)
        rl[pl.ds(h, 1), :] = r
        pltpu.make_async_copy(probs.at[hh], keep.at[h], rs_.at[names["e0"] + 2 * h]).start()
        pltpu.make_async_remote_copy(
            src_ref=otb.at[orow, :], dst_ref=otb.at[orow, :], send_sem=sends.at[first_send + h],
            recv_sem=rs_.at[names["o0"] + 2 * h], device_id=(pn, z), device_id_type=MESH,
        ).start()
        for at, step in forward_steps.items():
            pl.when(h == at)(lambda step=step: step() and None)

    for h in range(6):
        drains.append((first_send + h, otb.at[pl.ds(0, 64), :], None))

    for u in range(2, 6):
        weight_here(u)
    arrived(spare, "cm")
    for h in range(6):
        arrived(otb.at[rows(other * 384 + h * 64, 64), :], f"o{h}")
    arrived(probs.at[0], "e4")
    arrived(probs.at[1], "e5")

    mine = rows(k * 512, 512)
    theirs = rows(other * 512, 512)
    my_lanes = lanes(k * 512, 512)
    ot_mine = otb[:, my_lanes]
    x1[:, 0:384] = xs[mine, 0:384].astype(f32) + dims(ot_mine, wa[0], 0, 0)
    x1[:, 384:768] = xs[mine, 384:768].astype(f32) + dims(ot_mine, wa[1], 0, 0)
    xx = x1[...]
    c = xx - jnp.mean(xx, -1, keepdims=True)
    n = c * lax.rsqrt(jnp.mean(c * c, -1, keepdims=True) + norm_eps)
    h2[mine, :] = (n * grow[1:2, :]).astype(bf16)
    send(h2.at[mine, :], h2.at[mine, :], "h2", (pn, z))
    share_activation(dys, "ay")
    for o, w in ((0, 512), (512, 512), (1024, 128)):
        cols = pl.ds(o, w)
        a = times(h2[mine, :], wi[0, :, cols])
        b = times(h2[mine, :], wi[1, :, cols])
        phi = 0.5 * (1.0 + lax.erf(a * 0.7071067811865476))
        gelu = a * phi
        e = times(dys[mine, :], wm[:, cols])
        hid[:, cols] = (gelu * b).astype(bf16)
        dgo[0, :, cols] = (e * (b * (phi + a * (jnp.exp(-0.5 * a * a) * 0.3989422804014327)))).astype(bf16)
        dgo[1, :, cols] = (e * gelu).astype(bf16)
    send(hid.at[:, lanes(other * 512, 640)], hidp, "hid", (pn, z))
    send(dgo.at[other], dgp, "dg", (pn, z))

    shared_activation(dys, "ay")
    arrived(hidp, "hid")
    t = (
        dims(dys[mine, :], hid[:, lanes(k * 512, 640)], 0, 0) + dims(dys[theirs, :], hidp[...], 0, 0)
    ).astype(bf16)

    @pl.when(k == 0)
    def _():
        grad[:, MLP : MLP + 512] = t[:, 0:512]
        grad[:, 0:128] = t[:, 512:640]

    @pl.when(k == 1)
    def _():
        grad[:, MLP : MLP + 512] = t[:, 128:640]

    s1("m")
    lo[...] = (x1[...] + dims(hid[...], wm[...], 1, 1)).astype(bf16)
    give_back(lo, lo_out, "alo")
    arrived(h2.at[theirs, :], "h2")
    arrived(dgp, "dg")
    for name, o, w in (("i0", 0, 640), ("i1", 640, 512)):
        cols = pl.ds(o, w)
        grad[:, IN + o : IN + o + w] = (
            dims(h2[mine, :], dgo[k, :, cols], 0, 0) + dims(h2[theirs, :], dgp[:, cols], 0, 0)
        ).astype(bf16)
        if name == "i0":
            s1(name)
    f2 = dims(dgo[0], wi[0], 1, 1) + dims(dgo[1], wi[1], 1, 1)
    xx = x1[...]
    c = xx - jnp.mean(xx, -1, keepdims=True)
    r2 = lax.rsqrt(jnp.mean(c * c, -1, keepdims=True) + norm_eps)
    n = c * r2
    grow[3:4, :] = jnp.sum(f2 * n, 0, keepdims=True)
    cc = f2 * grow[1:2, :]
    dx = dys[mine, :].astype(f32) + r2 * (
        cc - jnp.mean(cc, -1, keepdims=True) - n * jnp.mean(cc * n, -1, keepdims=True)
    )
    x1[...] = dx
    dx1b[...] = dx.astype(bf16)
    send(dx1b.at[:, lanes(other * 384, 384)], dx1bp, "dx1b", (pn, z))
    for part in range(2):
        which = other if part == 0 else k
        col = lanes(which * 384, 384)
        feat = rows(which * 384, 384)
        left = jnp.concatenate([wa[0, feat, :], wa[1, feat, :]], axis=1)
        t = dims(left, dx1b[...], 1, 1).astype(bf16)
        if part == 0:
            dot_send[...] = t
            send(dot_send, dot_own.at[:, my_lanes], "do", (pn, z))
        else:
            dot_own[:, my_lanes] = t
    local(keep.at[5], probs.at[1], "e5")
    local(keep.at[4], probs.at[0], "e4")

    s2("m")
    s1("i1")
    arrived(dx1bp, "dx1b")
    grad[:, ATTN : ATTN + 384] = (
        times(otb[:, my_lanes], dx1b[:, lanes(k * 384, 384)])
        + times(otb[:, lanes(other * 512, 512)], dx1bp[...])
    ).astype(bf16)
    arrived(dot_own.at[:, lanes(other * 512, 512)], "do")

    for h in range(6):
        rsem(f"b{h}")
    backward_steps = {
        4: lambda: (s2("i0"), s3("m")),
        3: lambda: (s2("i1"), s1("a"), s1("q2")),
        2: lambda: (s3("i0"), s4("m")),
        1: lambda: s3("i1"),
        0: lambda: (s2("a"), s4("i0")),
    }

    @pl.loop(0, 6)
    def _(turn):
        h = 5 - turn
        p, hh = h // 2, lax.rem(h, 2)
        qrow, krow, vrow = (rows(at + hh * 64, 64) for at in (0, 128, 256))
        arrived_at = rs_.at[names["e0"] + 2 * h]
        pltpu.make_async_copy(keep.at[h], probs.at[hh], arrived_at).wait()
        vt = qk[p, vrow, :]
        kt = qk[p, krow, :]
        for i in range(2):
            cols = slice(i * 512, i * 512 + 512)
            do = dot_own[rows(h * 64, 64), cols].astype(f32) * rl[pl.ds(h, 1), cols]
            delta = jnp.sum(do * otb[rows(k * 384 + h * 64, 64), cols].astype(f32), 0, keepdims=True)
            dob = do.astype(bf16)
            e = probs[hh, :, cols]
            ds = (e.astype(f32) * (dims(vt, dob, 0, 0) - delta)).astype(bf16)
            dk = dims(qk[p, qrow, cols], ds, 1, 1)
            dv = dims(dob, e, 1, 1)
            if i == 0:
                dkb[...] = dk
                dvb[...] = dv
            else:
                dkb[...] += dk
                dvb[...] += dv
            dq = times(kt, ds) * HEAD_DIM**-0.5
            c = cosr[:, cols]
            s = sinr[:, cols]
            qk[p, rows(hh * 64, 32), cols] = (dq[:32] * c + dq[32:] * s).astype(bf16)
            qk[p, rows(hh * 64 + 32, 32), cols] = (dq[32:] * c - dq[:32] * s).astype(bf16)

        @pl.when(h >= 2)
        def _():
            pltpu.make_async_copy(keep.at[h - 2], probs.at[hh], rs_.at[names["e0"] + 2 * (h - 2)]).start()

        d = dkb[...]
        c = cosr[...]
        s = sinr[...]
        qk[p, rows(128 + hh * 64, 32), :] = (d[:32] * c + d[32:] * s).astype(bf16)
        qk[p, rows(160 + hh * 64, 32), :] = (d[32:] * c - d[:32] * s).astype(bf16)
        qk[p, vrow, :] = dvb[...].astype(bf16)

        @pl.when(h == 4)
        def _():
            grad[:, lanes(PAIR + 384 * p, 384)] = dims(h1t[...], qk[p], 1, 1).astype(bf16)

        for at, step in backward_steps.items():
            pl.when(h == at)(lambda step=step: step() and None)

    def f1_part(cols):
        return times(wq[0], qk[0, :, cols]) + times(wq[1], qk[1, :, cols]) + times(wq[2], qk[2, :, cols])

    big[0:768, 0:512] = f1_part(lanes(other * 512, 512))
    send(big.at[pl.ds(0, 768), pl.ds(0, 512)], f1r, "f1", (pn, z))
    s2("q2")
    big[0:768, 512:1024] = f1_part(my_lanes)
    s4("i1")
    arrived(f1r, "f1")
    f1 = (big[0:768, 512:1024] + f1r[...]).T
    xx = xs[mine, :].astype(f32)
    c = xx - jnp.mean(xx, -1, keepdims=True)
    r1 = lax.rsqrt(jnp.mean(c * c, -1, keepdims=True) + norm_eps)
    n = c * r1
    grow[2:3, :] = jnp.sum(f1 * n, 0, keepdims=True)
    cc = f1 * grow[0:1, :]
    gi[...] = (
        x1[...] + r1 * (cc - jnp.mean(cc, -1, keepdims=True) - n * jnp.mean(cc * n, -1, keepdims=True))
    ).astype(bf16)
    send(grow, growp, "gr", (pn, z), when=lambda: k == 0)

    @pl.when(k == 1)
    def _():
        arrived(growp, "gr")
        two = jnp.concatenate([grow[2:4, :] + growp[2:4, :], jnp.zeros((126, 768), f32)], axis=0)
        grad[:, 0:128] = two.T.astype(bf16)

    s1("g")
    give_back(gi, gi_out, "agi", (0,))
    give_back(gi, gi_out, "agi", (1,), inner)
    for p in (1, 0):
        grad[:, PAIR + 384 * p : PAIR + 384 * p + 384] = dims(h1t[...], qk[p], 1, 1).astype(bf16)
        s1(f"q{p}")
        if p == 1:
            s3("a")
    s3("q2")
    s5("m")
    s4("a")
    s2("q1")
    s2("g")
    s4("q2")
    s5("i0")
    s2("q0")
    s5("i1")
    s3("q1")
    s3("g")
    s3("q0")
    give_back(gi, gi_out, "agi", (1,), outer)
    s5("a")
    s4("q1")
    s4("g")
    s4("q0")
    s5("q2")
    s5("q1")
    s5("g")
    s5("q0")
    for u in REDUCE:
        s6(u)
    given_back(lo_out, "alo")
    given_back(gi_out, "agi")
    drain_all()
    assert len(names) <= 160 and count["send"] <= 220 and len(packing) <= 32


frequency = np.broadcast_to(
    (np.float32(rope_base) ** (-(np.arange(32, dtype=np.float32) * 2) / HEAD_DIM))[:, None], (32, 128)
).astype(np.float32)


def finish_kernel(
    lo_raw, gi_raw, gp_raw, lo, gi, o_qkv, o_attn, o_in, o_mlp, o_one, o_two,
    buf, gp, g_qkv, g_attn, g_in, g_mlp, g_one, g_two, sem,
):
    loads = [
        pltpu.make_async_copy(src, dst, sem.at[i])
        for i, (src, dst) in enumerate(((gp_raw, gp), (lo_raw, buf.at[0]), (gi_raw, buf.at[1])))
    ]
    for copy in loads:
        copy.start()
    pairs = ((buf.at[0], lo), (buf.at[1], gi), (g_qkv, o_qkv), (g_attn, o_attn), (g_in, o_in), (g_mlp, o_mlp), (g_one, o_one), (g_two, o_two))
    stores = [pltpu.make_async_copy(src, dst, sem.at[3 + i]) for i, (src, dst) in enumerate(pairs)]
    loads[0].wait()
    for c in range(2):
        for p in range(3):
            for t in range(3):
                o = 768 * t + 384 * c + 128 * p
                at = PAIR + 384 * p + 128 * t
                g_qkv[:, o : o + 128] = gp[c, :, at : at + 128]
        g_attn[:, 384 * c : 384 * c + 384] = gp[c, :, ATTN : ATTN + 384]
        g_in[:, 1152 * c : 1152 * c + 1152] = gp[c, :, IN : IN + 1152]
    g_mlp[:, 0:512] = gp[0, :, MLP : MLP + 512]
    g_mlp[:, 512:640] = gp[0, :, 0:128]
    g_mlp[:, 640:1152] = gp[1, :, MLP : MLP + 512]
    flat = jnp.concatenate([gp[1, :, 0:128], jnp.zeros((104, 128), f32)], axis=0).T
    g_one[...] = flat[0:1, 0:24]
    g_two[...] = flat[1:2, 0:24]
    for load, store in zip(loads[1:], stores[:2]):
        load.wait()
        store.start()
    for store in stores[2:]:
        store.start()
    for store in stores:
        store.wait()


def fast(layer_in, seg_start, out_grad, w_qkv, w_attn_out, w_in, w_mlp_out, norm_attn, norm_mlp):
    hbm = pl.BlockSpec(memory_space=pltpu.HBM)
    vmem = pl.BlockSpec(memory_space=pltpu.VMEM)
    V = pltpu.VMEM
    outs = pl.pallas_call(
        step_kernel,
        name="layer",
        out_shape=[
            jax.ShapeDtypeStruct((2, 256, 768), bf16),
            jax.ShapeDtypeStruct((2, 256, 768), bf16),
            jax.ShapeDtypeStruct((2, 24, WIDTH), f32),
            jax.ShapeDtypeStruct((768, WIDTH), bf16),
            jax.ShapeDtypeStruct((6, 1024, 1024), bf16),
        ],
        in_specs=[hbm, hbm, vmem, hbm, hbm, hbm, hbm, vmem, vmem, vmem],
        out_specs=[hbm] * 5,
        scratch_shapes=[
            V((2, 24, WIDTH), bf16),
            V((8, 128), f32),
            V((1024, 768), bf16),
            V((1024, 768), bf16),
            V((1, 1024), jnp.int32),
            V((768, 1024), bf16),
            V((3, 768, 384), bf16),
            V((2, 768, 384), bf16),
            V((2, 768, 1152), bf16),
            V((768, 1152), bf16),
            V((768, 128), bf16),
            V((32, 1024), f32),
            V((32, 1024), f32),
            V((3, 384, 1024), bf16),
            V((1024, 1152), f32),
            V((2, 1024, 1024), bf16),
            V((768, 1024), bf16),
            V((8, 1024), f32),
            V((512, 768), f32),
            V((1024, 768), bf16),
            V((512, 1152), bf16),
            V((512, 640), bf16),
            V((2, 512, 1152), bf16),
            V((512, 1152), bf16),
            V((512, 768), bf16),
            V((512, 384), bf16),
            V((384, 512), bf16),
            V((384, 1024), bf16),
            V((768, 512), f32),
            V((512, 768), bf16),
            V((512, 768), bf16),
            V((768, WIDTH), bf16),
            V((8, 768), f32),
            V((8, 768), f32),
            V((64, 1024), f32),
            V((64, 1024), f32),
            V((2, 96, WIDTH), bf16),
            V((2, 96, WIDTH), bf16),
            V((96, WIDTH), bf16),
            V((96, WIDTH), bf16),
            V((2, 4, 24, WIDTH), bf16),
            V((2, 24, WIDTH), bf16),
            V((2, 2, 24, WIDTH), bf16),
            V((2, 24, WIDTH), bf16),
            V((2, 24, WIDTH), f32),
            pltpu.SemaphoreType.DMA((160,)),
            pltpu.SemaphoreType.DMA((32,)),
            pltpu.SemaphoreType.DMA((220,)),
        ],
        compiler_params=pltpu.CompilerParams(
            collective_id=0, has_side_effects=True, vmem_limit_bytes=67043328
        ),
    )(
        layer_in, out_grad, seg_start, w_qkv, w_attn_out, w_in, w_mlp_out,
        norm_attn[None], norm_mlp[None], frequency,
    )
    done = pl.pallas_call(
        finish_kernel,
        name="finish",
        out_shape=[
            jax.ShapeDtypeStruct((2, 256, 768), bf16),
            jax.ShapeDtypeStruct((2, 256, 768), bf16),
            jax.ShapeDtypeStruct((24, 2304), f32),
            jax.ShapeDtypeStruct((24, 768), f32),
            jax.ShapeDtypeStruct((24, 2304), f32),
            jax.ShapeDtypeStruct((24, 1152), f32),
            jax.ShapeDtypeStruct((1, 24), f32),
            jax.ShapeDtypeStruct((1, 24), f32),
        ],
        in_specs=[hbm, hbm, hbm],
        out_specs=[hbm] * 8,
        scratch_shapes=[
            V((2, 2, 256, 768), bf16),
            V((2, 24, WIDTH), f32),
            V((24, 2304), f32),
            V((24, 768), f32),
            V((24, 2304), f32),
            V((24, 1152), f32),
            V((1, 24), f32),
            V((1, 24), f32),
            pltpu.SemaphoreType.DMA((11,)),
        ],
    )(*outs[:3])
    return (*done[:6], done[6][0], done[7][0])


def normalize(values):
    centered = values - jnp.mean(values, axis=-1, keepdims=True)
    spread = jnp.mean(centered * centered, axis=-1, keepdims=True)
    return centered * lax.rsqrt(spread + norm_eps)


def rope_tables(positions):
    half_dim = HEAD_DIM // 2
    frequency = rope_base ** (-(jnp.arange(half_dim).astype(jnp.float32) * 2.0) / HEAD_DIM)
    angles = positions.astype(jnp.float32)[:, None] * frequency[None, :]
    angles = jnp.concatenate([angles, angles], axis=-1)
    return (jnp.cos(angles), jnp.sin(angles))


def turn_half(values):
    half_dim = values.shape[-1] // 2
    return jnp.concatenate([-values[..., half_dim:], values[..., :half_dim]], axis=-1)


def rotate(values, cosine_table, sine_table):
    return values * cosine_table[:, None, :] + turn_half(values) * sine_table[:, None, :]


def unrotate(values, cosine_table, sine_table):
    return values * cosine_table[:, None, :] - turn_half(values) * sine_table[:, None, :]


def product(left, right):
    return jnp.dot(left, right, preferred_element_type=jnp.float32)


def left_transposed(left, right):
    return lax.dot_general(
        left, right, (((0,), (0,)), ((), ())), preferred_element_type=jnp.float32
    )


def right_transposed(left, right):
    return lax.dot_general(
        left, right, (((1,), (1,)), ((), ())), preferred_element_type=jnp.float32
    )


def to_groups(array):
    row_count, head_count, head_size = array.shape
    return array.reshape(row_count, head_count // 4, 4, head_size).transpose(1, 0, 2, 3)


def from_groups(array):
    group_count, row_count, group_heads, head_size = array.shape
    return array.transpose(1, 0, 2, 3).reshape(row_count, group_count * group_heads, head_size)


def attend_group(group_in, same_doc):
    query_part, key_part, value_part = group_in
    scores = jnp.einsum(
        "qhd,khd->hqk", query_part, key_part, preferred_element_type=jnp.float32
    ) * HEAD_DIM ** (-0.5)
    masked = jnp.where(same_doc[None], scores, neg_large)
    highest = jnp.max(masked, axis=-1, keepdims=True)
    shifted = jnp.exp(masked - highest)
    totals = jnp.sum(shifted, axis=-1, keepdims=True)
    attn_prob = shifted / totals
    log_total = highest + jnp.log(totals)
    mixed_out = jnp.einsum(
        "hqk,khd->qhd",
        attn_prob.astype(jnp.bfloat16),
        value_part,
        preferred_element_type=jnp.float32,
    )
    return (mixed_out, log_total[..., 0])


def attend_back(group_in, same_doc):
    query_part, key_part, value_part, grad_part, log_total = group_in
    scores = jnp.einsum(
        "qhd,khd->hqk", query_part, key_part, preferred_element_type=jnp.float32
    ) * HEAD_DIM ** (-0.5)
    attn_prob = jnp.where(same_doc[None], jnp.exp(scores - log_total[..., None]), 0.0)
    grad_prob = jnp.einsum(
        "qhd,khd->hqk", grad_part, value_part, preferred_element_type=jnp.float32
    )
    inner_sum = jnp.sum(attn_prob * grad_prob, axis=-1, keepdims=True)
    grad_score = (attn_prob * (grad_prob - inner_sum)).astype(jnp.bfloat16)
    grad_query = jnp.einsum(
        "hqk,khd->qhd", grad_score, key_part, preferred_element_type=jnp.float32
    ) * HEAD_DIM ** (-0.5)
    grad_key = jnp.einsum(
        "hqk,qhd->khd", grad_score, query_part, preferred_element_type=jnp.float32
    ) * HEAD_DIM ** (-0.5)
    grad_value = jnp.einsum(
        "hqk,qhd->khd",
        attn_prob.astype(jnp.bfloat16),
        grad_part,
        preferred_element_type=jnp.float32,
    )
    return (grad_query, grad_key, grad_value)


def scaled_norm(values_in, gain_row):
    return normalize(values_in) * gain_row


def geglu(first_half, second_half):
    return jax.nn.gelu(first_half, approximate=False) * second_half


def local(layer_in, seg_start, out_grad, w_qkv, w_attn_out, w_in, w_mlp_out, norm_attn, norm_mlp):
    micro_count = layer_in.shape[0]
    span_len = layer_in.shape[1]
    model_width = layer_in.shape[2]
    ctx_rank = lax.axis_index("ctx")
    grad_sums = (
        jnp.zeros((model_width, 3 * model_width), jnp.float32),
        jnp.zeros((model_width, model_width), jnp.float32),
        jnp.zeros((model_width, 2 * FF), jnp.float32),
        jnp.zeros((model_width, FF), jnp.float32),
        jnp.zeros((model_width,), jnp.float32),
        jnp.zeros((model_width,), jnp.float32),
    )
    offsets = ctx_rank * span_len + jnp.arange(span_len, dtype=jnp.int32)
    outputs = []
    grad_inputs = []
    for micro_step in range(micro_count):
        gathered = (
            lax.all_gather(w_qkv, ("dp", "ctx"), axis=0, tiled=True),
            lax.all_gather(w_attn_out, ("dp", "ctx"), axis=0, tiled=True),
            lax.all_gather(w_in, ("dp", "ctx"), axis=0, tiled=True),
            lax.all_gather(w_mlp_out, ("dp", "ctx"), axis=0, tiled=True),
            lax.all_gather(norm_attn, ("dp", "ctx"), axis=0, tiled=True),
            lax.all_gather(norm_mlp, ("dp", "ctx"), axis=0, tiled=True),
        )
        qkv_full, attn_full, in_full, mlp_full, gain_attn, gain_mlp = gathered
        starts_here = seg_start[micro_step]
        hidden = layer_in[micro_step].astype(jnp.float32)
        cosine_table, sine_table = rope_tables(offsets - starts_here)
        normed, norm_back = jax.vjp(scaled_norm, hidden, gain_attn.astype(jnp.float32))
        normed_low = normed.astype(jnp.bfloat16)
        qkv_local = product(normed_low, qkv_full).reshape(span_len, 3, HEADS, HEAD_DIM)
        queries = rotate(qkv_local[:, 0], cosine_table, sine_table).astype(jnp.bfloat16)
        keys_here = rotate(qkv_local[:, 1], cosine_table, sine_table).astype(jnp.bfloat16)
        values_here = qkv_local[:, 2].astype(jnp.bfloat16)
        keys_all, values_all, starts_all = (
            lax.all_gather(keys_here, "ctx", axis=0, tiled=True),
            lax.all_gather(values_here, "ctx", axis=0, tiled=True),
            lax.all_gather(starts_here, "ctx", axis=0, tiled=True),
        )
        same_doc = starts_here[:, None] == starts_all[None, :]
        query_groups = to_groups(queries)
        key_groups = to_groups(keys_all)
        value_groups = to_groups(values_all)
        mixed_out, log_total = lax.map(
            lambda group_in: attend_group(group_in, same_doc),
            (query_groups, key_groups, value_groups),
        )
        attended = from_groups(mixed_out).reshape(span_len, model_width).astype(jnp.bfloat16)
        middle = hidden + product(attended, attn_full)
        normed_mlp, norm_mlp_back = jax.vjp(scaled_norm, middle, gain_mlp.astype(jnp.float32))
        normed_mlp_low = normed_mlp.astype(jnp.bfloat16)
        projected = product(normed_mlp_low, in_full)
        gated_out, geglu_back = jax.vjp(geglu, projected[:, :FF], projected[:, FF:])
        gated_low = gated_out.astype(jnp.bfloat16)
        result = middle + right_transposed(gated_low, mlp_full)
        outputs.append(result.astype(jnp.bfloat16))
        qkv_full, attn_full, in_full, mlp_full = (
            lax.all_gather(w_qkv, ("dp", "ctx"), axis=0, tiled=True),
            lax.all_gather(w_attn_out, ("dp", "ctx"), axis=0, tiled=True),
            lax.all_gather(w_in, ("dp", "ctx"), axis=0, tiled=True),
            lax.all_gather(w_mlp_out, ("dp", "ctx"), axis=0, tiled=True),
        )
        grad_out = out_grad[micro_step].astype(jnp.float32)
        grad_out_low = out_grad[micro_step]
        grad_mlp_weight = left_transposed(grad_out_low, gated_low)
        grad_gated = product(grad_out_low, mlp_full)
        grad_first, grad_second = geglu_back(grad_gated)
        grad_projected = jnp.concatenate([grad_first, grad_second], axis=1).astype(jnp.bfloat16)
        grad_in_weight = left_transposed(normed_mlp_low, grad_projected)
        grad_normed_mlp = right_transposed(grad_projected, in_full)
        grad_middle_norm, grad_gain_mlp = norm_mlp_back(grad_normed_mlp)
        grad_middle = grad_out + grad_middle_norm
        grad_middle_low = grad_middle.astype(jnp.bfloat16)
        grad_attn_weight = left_transposed(attended, grad_middle_low)
        grad_attended = (
            right_transposed(grad_middle_low, attn_full)
            .astype(jnp.bfloat16)
            .reshape(span_len, HEADS, HEAD_DIM)
        )
        grad_groups = to_groups(grad_attended)
        grad_query_groups, grad_key_groups, grad_value_groups = lax.map(
            lambda group_in: attend_back(group_in, same_doc),
            (query_groups, key_groups, value_groups, grad_groups, log_total),
        )
        keys_total = keys_all.shape[0]
        grad_keys, grad_values = (
            lax.psum_scatter(
                from_groups(grad_key_groups).reshape(keys_total, model_width).astype(jnp.bfloat16),
                "ctx",
                scatter_dimension=0,
                tiled=True,
            ).astype(jnp.float32),
            lax.psum_scatter(
                from_groups(grad_value_groups)
                .reshape(keys_total, model_width)
                .astype(jnp.bfloat16),
                "ctx",
                scatter_dimension=0,
                tiled=True,
            ).astype(jnp.float32),
        )
        grad_qkv = jnp.stack(
            [
                unrotate(from_groups(grad_query_groups), cosine_table, sine_table),
                unrotate(grad_keys.reshape(span_len, HEADS, HEAD_DIM), cosine_table, sine_table),
                grad_values.reshape(span_len, HEADS, HEAD_DIM),
            ],
            axis=1,
        )
        grad_qkv = grad_qkv.reshape(span_len, 3 * model_width).astype(jnp.bfloat16)
        grad_qkv_weight = left_transposed(normed_low, grad_qkv)
        grad_normed = right_transposed(grad_qkv, qkv_full)
        grad_hidden_norm, grad_gain_attn = norm_back(grad_normed)
        grad_inputs.append((grad_middle + grad_hidden_norm).astype(jnp.bfloat16))
        grad_sums = (
            grad_sums[0] + grad_qkv_weight,
            grad_sums[1] + grad_attn_weight,
            grad_sums[2] + grad_in_weight,
            grad_sums[3] + grad_mlp_weight,
            grad_sums[4] + grad_gain_attn,
            grad_sums[5] + grad_gain_mlp,
        )
    shares = (
        lax.psum_scatter(grad_sums[0], ("dp", "ctx"), scatter_dimension=0, tiled=True),
        lax.psum_scatter(grad_sums[1], ("dp", "ctx"), scatter_dimension=0, tiled=True),
        lax.psum_scatter(grad_sums[2], ("dp", "ctx"), scatter_dimension=0, tiled=True),
        lax.psum_scatter(grad_sums[3], ("dp", "ctx"), scatter_dimension=0, tiled=True),
        lax.psum_scatter(grad_sums[4], ("dp", "ctx"), scatter_dimension=0, tiled=True),
        lax.psum_scatter(grad_sums[5], ("dp", "ctx"), scatter_dimension=0, tiled=True),
    )
    return (
        jnp.stack(outputs),
        jnp.stack(grad_inputs),
        shares[0],
        shares[1],
        shares[2],
        shares[3],
        shares[4],
        shares[5],
    )


def solution(mesh):
    A = P(None, ("dp", "ctx"), None)
    S = P(None, ("dp", "ctx"))
    W = P(("dp", "ctx"), None)
    G = P(("dp", "ctx"))
    return jax.shard_map(
        fast if dict(mesh.shape) == {"dp": 8, "ctx": 4} else local,
        mesh=mesh,
        in_specs=(A, S, A, W, W, W, W, G, G),
        out_specs=(A, A, W, W, W, W, G, G),
        check_vma=False,
    )
```

```python
import contextlib

import jax
import jax.numpy as jnp
import numpy as np
from jax import lax
from jax.experimental import pallas as pl
from jax.experimental.pallas import tpu as pltpu
from jax.sharding import PartitionSpec as P

MESH = pl.DeviceIdType.MESH
bf16 = jnp.bfloat16
f32 = jnp.float32

HEADS = 12
HEAD_DIM = 64
FF = 1152
rope_base = 160000.0
norm_eps = 1e-05
neg_large = -1e30

WIDTH = 3328
GATHER = [(0, 512), (512, 768), (1280, 384), (1664, 640), (2304, 512), (2816, 512)]
PAIR = 128
ATTN = 1280
IN = 1664
MLP = 2816
REDUCE = {
    "m": (2816, 512),
    "i0": (1664, 640),
    "i1": (2304, 512),
    "a": (1280, 384),
    "q2": (896, 384),
    "q1": (512, 384),
    "q0": (128, 384),
    "g": (0, 128),
}


TRACE = False


def scope(name):
    return jax.named_scope(name) if TRACE else contextlib.nullcontext()


def scoped(fn):
    def inner(*args):
        with scope(f"{fn.__name__}_{args[0] if args and isinstance(args[0], (int, str)) else ''}"):
            return fn(*args)

    return inner


def dims(left, right, left_at, right_at):
    return lax.dot_general(
        left, right, (((left_at,), (right_at,)), ((), ())), preferred_element_type=f32
    )


def times(left, right):
    return jnp.dot(left, right, preferred_element_type=f32)


def step_kernel(
    x_in, dy_in, seg_raw, w_qkv, w_attn, w_in, w_mlp, g_attn_raw, g_mlp_raw, freq_raw,
    lo_out, gi_out, gp_out, land, keep,
    wp, gcol, seg_in, g_attn, g_mlp, freq,
    xs, dys, sg, h1t, wq, wa, wi, wm, gains, cosr, sinr, qk, big, probs, otb, rl, x1, h2, hid, hidp,
    dgo, dgp, dx1b, dx1bp, dot_send, dot_own, f1r, lo, gi, grad, grow, growp, dkb, dvb,
    ra, rb, ra2, rb2, zs, zp, zm, zx, fin,
    rs_, ls_, sends,
):
    dp = lax.axis_index("dp")
    z = lax.axis_index("ctx")
    q = dp // 2
    k = lax.rem(dp, 2)
    other = 1 - k
    pn = dp + 1 - 2 * k
    xn = dp + 2 - 4 * lax.rem(dp // 2, 2)
    yn = dp + 4 - 8 * (dp // 4)
    zn = z + 1 - 2 * lax.rem(z, 2)
    zb = jnp.where(z < 2, 2, 1)
    zh = z // 2
    qx = q + 1 - 2 * lax.rem(q, 2)
    qy = q + 2 - 4 * (q // 2)
    qd = qx + 2 - 4 * (qx // 2)
    inner = jnp.logical_or(z == 1, z == 2)
    outer = jnp.logical_or(z == 0, z == 3)
    near = k == zh
    away = k != zh
    names = {}
    count = {"send": 0, "local": 0}
    drains = []

    def rsem(name):
        return rs_.at[names.setdefault(name, len(names))]

    def still(view):
        index = view.transforms[0].indices
        return view.ref.at[tuple(pl.ds(0, at.size) if hasattr(at, "size") else 0 for at in index)]

    keyed = {}

    def send(src, dst, name, dev, when=None, sem=None, key=None):
        first = key is None or key not in keyed
        if first:
            i = count["send"]
            count["send"] += 1
            keyed[key] = i
        else:
            i = keyed[key]
        copy = pltpu.make_async_remote_copy(
            src_ref=src, dst_ref=dst, send_sem=sends.at[i], recv_sem=rsem(name) if sem is None else sem,
            device_id=dev, device_id_type=MESH,
        )
        if when is None:
            copy.start()
        else:
            pl.when(when())(copy.start)
        if first:
            drains.append((i, src, when))

    def drain_all():
        for i, src, when in drains:
            view = still(src) if hasattr(src, "transforms") else src

            def wait(view=view, i=i):
                pltpu.make_async_copy(view, view, sends.at[i]).wait()

            if when is None:
                wait()
            else:
                pl.when(when())(wait)

    def local(src, dst, name):
        copy = pltpu.make_async_copy(src, dst, rsem(name))
        copy.start()
        return copy

    def arrived(ref, name):
        pltpu.make_async_copy(ref, ref, rsem(name)).wait()

    def rows(start, size):
        return pl.ds(pl.multiple_of(start, 8), size)

    def lanes(start, size):
        return pl.ds(pl.multiple_of(start, 128), size)

    barrier = pltpu.get_barrier_semaphore()
    for dz in range(1, 4):
        for kk in range(2):
            pl.semaphore_signal(
                barrier, inc=1, device_id=(2 * q + kk, lax.rem(z + dz, 4)), device_id_type=MESH
            )
    for dev in (pn, xn, yn):
        pl.semaphore_signal(barrier, inc=1, device_id=(dev, z), device_id_type=MESH)

    packs = []
    for c in range(2):
        for p in range(3):
            for t in range(3):
                packs.append((w_qkv, 768 * t + 384 * c + 128 * p, c, PAIR + 384 * p + 128 * t, 128))
        packs.append((w_attn, 384 * c, c, ATTN, 384))
        packs.append((w_in, 1152 * c, c, IN, 1152))
        packs.append((w_mlp, 640 * c, c, MLP, 512))
    packs.append((w_mlp, 512, 0, 0, 128))
    packing = [
        pltpu.make_async_copy(w.at[:, pl.ds(o, n)], wp.at[c, :, pl.ds(at, n)], ls_.at[i])
        for i, (w, o, c, at, n) in enumerate(packs)
    ]
    small = [
        pltpu.make_async_copy(src, dst, ls_.at[len(packs) + i])
        for i, (src, dst) in enumerate(
            ((g_attn_raw, g_attn), (g_mlp_raw, g_mlp), (seg_raw, seg_in), (freq_raw, freq))
        )
    ]
    for copy in small + packing:
        copy.start()
    gcol[...] = jnp.zeros_like(gcol)
    for copy in small:
        copy.wait()
    gcol[0:1, 0:24] = g_attn[...].astype(f32)
    gcol[1:2, 0:24] = g_mlp[...].astype(f32)
    columns = jnp.concatenate([gcol[...], jnp.zeros((120, 128), f32)], axis=0).T[0:24].astype(bf16)
    wp[1, :, 0:128] = columns

    @scoped
    def zstage(u, turn=None):
        o, w = GATHER[u]
        cols = pl.ds(o, w)

        def body():
            dst = land.at[rows(dp * 96 + z * 24, 24), cols]
            for c in range(2):
                src = wp.at[c, :, cols]
                send(src, dst, f"z{u}", (2 * q + c, zn), key=f"zn{u}{c}")
                send(src, dst, f"z{u}", (2 * q + c, zb), key=f"zb{u}{c}")
                send(src, dst, f"z{u}", (pn, z), when=lambda c=c: k != c, key=f"zp{u}{c}")
                pl.when(k == c)(lambda src=src: local(src, dst, f"z{u}") and None)

        in_turn(turn, body)

    def in_turn(turn, body):
        if turn is None:
            body()
        else:
            pl.when(turn)(body)

    @scoped
    def slab_in(u, turn=None):
        o, w = GATHER[u]
        cols = pl.ds(o, w)

        def body():
            arrived(land.at[rows(q * 192, 192), cols], f"z{u}")
            for j in range(2):
                part = land.at[rows((2 * q + j) * 96 + lax.rem(4 - 2 * z + 4, 4) * 24, 48), cols]
                send(part, part, f"z{u}", (dp, zn), when=lambda: inner, key=f"fs{u}{j}")

        in_turn(turn, body)

    @scoped
    def xysend(u):
        o, w = GATHER[u]
        slab = land.at[rows(q * 192, 192), pl.ds(o, w)]
        send(slab, slab, f"x{u}", (xn, z))
        send(slab, slab, f"y{u}", (yn, z))

    @scoped
    def diag(u):
        o, w = GATHER[u]
        cols = pl.ds(o, w)
        arrived(land.at[rows(qx * 192, 192), cols], f"x{u}")
        part = land.at[rows(qx * 192, 96), cols]
        send(part, part, f"dx{u}", (yn, z))
        arrived(land.at[rows(qy * 192, 192), cols], f"y{u}")
        part = land.at[rows(qy * 192 + 96, 96), cols]
        send(part, part, f"dy{u}", (xn, z))

    @scoped
    def done(u):
        o, w = GATHER[u]
        cols = pl.ds(o, w)
        arrived(land.at[rows(qd * 192, 96), cols], f"dx{u}")
        arrived(land.at[rows(qd * 192 + 96, 96), cols], f"dy{u}")

    def activation(src_ref, dst_ref, name, turn=None):
        for m in range(2):
            src = src_ref.at[m]
            dst = dst_ref.at[rows(z * 256, 256), :]
            sem = rs_.at[base[name] + lax.rem(z, 2)]

            def going(m=m):
                there = 2 * k + m != z
                return there if turn is None else jnp.logical_and(turn, there)

            here = 2 * k + m == z
            if turn is not None:
                here = jnp.logical_and(turn, here)
            send(src, dst, None, (2 * q + zh, 2 * k + m), when=going, sem=sem)
            pl.when(here)(pltpu.make_async_copy(src, dst, sem).start)

    base = {}
    for name in ("ax", "ay", "alo", "agi"):
        base[name] = len(names)
        names[name + "0"] = len(names)
        names[name + "1"] = len(names)

    @scoped
    def share_activation(ref, name, turn=None):
        def body():
            for j in range(2):
                r = rows(k * 512 + j * 256, 256)
                arrived(ref.at[r, :], f"{name}{j}")
                send(ref.at[r, :], ref.at[r, :], f"p{name}{j}", (pn, z), key=f"sh{name}{j}")

        in_turn(turn, body)

    @scoped
    def shared_activation(ref, name, turn=None):
        def body():
            for j in range(2):
                arrived(ref.at[rows(other * 512 + j * 256, 256), :], f"p{name}{j}")

        in_turn(turn, body)

    @scoped
    def give_back(src_ref, out_ref, name, blocks=(0, 1), turn=None):
        m = lax.rem(z, 2)
        for j in blocks:
            src = src_ref.at[pl.ds(j * 256, 256), :]
            dst = out_ref.at[m]
            sem = rs_.at[base[name] + m]

            def going(j=j):
                leaves = jnp.logical_or(2 * k + j != z, zh != k)
                return leaves if turn is None else jnp.logical_and(turn, leaves)

            stays = jnp.logical_and(2 * k + j == z, zh == k)
            if turn is not None:
                stays = jnp.logical_and(turn, stays)
            send(src, dst, None, (2 * q + zh, 2 * k + j), when=going, sem=sem)
            pl.when(stays)(pltpu.make_async_copy(src, dst, sem).start)

    @scoped
    def given_back(out_ref, name):
        for m in range(2):
            arrived(out_ref.at[m], f"{name}{m}")

    def seg_send():
        for m in range(2):
            src = seg_in.at[pl.ds(m, 1), :]
            dst = sg.at[:, lanes(z * 256, 256)]
            for c in range(2):

                def away(m=m, c=c):
                    return jnp.logical_or(2 * k + m != z, k != c)

                send(src, dst, "seg", (2 * q + c, 2 * k + m), when=away)
                pl.when(jnp.logical_not(away()))(pltpu.make_async_copy(src, dst, rsem("seg")).start)

    @scoped
    def s1(u):
        o, w = REDUCE[u]
        cols = pl.ds(o, w)
        for slot, quarter in enumerate((qx, qd)):
            send(grad.at[rows(quarter * 192, 96), cols], ra.at[slot, :, cols], f"ra{u}", (xn, z))
        for slot, quarter in enumerate((qy, qd)):
            send(grad.at[rows(quarter * 192 + 96, 96), cols], rb.at[slot, :, cols], f"rb{u}", (yn, z))

    @scoped
    def s2(u):
        o, w = REDUCE[u]
        cols = pl.ds(o, w)
        arrived(ra.at[:, :, cols], f"ra{u}")
        r = rows(qy * 192, 96)
        grad[r, cols] = (grad[r, cols].astype(f32) + ra[1, :, cols].astype(f32)).astype(bf16)
        send(grad.at[r, cols], ra2.at[:, cols], f"ra2{u}", (yn, z))
        arrived(rb.at[:, :, cols], f"rb{u}")
        r2 = rows(qx * 192 + 96, 96)
        grad[r2, cols] = (grad[r2, cols].astype(f32) + rb[1, :, cols].astype(f32)).astype(bf16)
        send(grad.at[r2, cols], rb2.at[:, cols], f"rb2{u}", (xn, z))

    @scoped
    def s3(u):
        o, w = REDUCE[u]
        cols = pl.ds(o, w)
        arrived(ra2.at[:, cols], f"ra2{u}")
        arrived(rb2.at[:, cols], f"rb2{u}")
        for j, (one, two) in enumerate(((ra, ra2), (rb, rb2))):
            total = (
                grad[rows(q * 192 + 96 * j, 96), cols].astype(f32)
                + one[0, :, cols].astype(f32)
                + two[:, cols].astype(f32)
            )
            for at in range(4):
                zs[j, at, :, cols] = total[24 * at : 24 * at + 24].astype(bf16)
        send(zs.at[:, zn, :, cols], zp.at[:, :, cols], f"zp{u}", (dp, zn))
        far = 2 * (1 - zh)
        send(zs.at[:, pl.ds(far, 2), :, cols], zm.at[:, :, :, cols], f"zm{u}", (dp, zn), when=lambda: outer)

    @scoped
    def s4(u):
        o, w = REDUCE[u]
        cols = pl.ds(o, w)
        far = 2 * (1 - zh)

        @pl.when(inner)
        def _():
            arrived(zm.at[:, :, :, cols], f"zm{u}")
            for j in range(2):
                for at in range(2):
                    zs[j, far + at, :, cols] = (
                        zs[j, far + at, :, cols].astype(f32) + zm[j, at, :, cols].astype(f32)
                    ).astype(bf16)

        for at in range(2):
            send(zs.at[:, far + at, :, cols], zx.at[:, :, cols], f"zx{u}", (dp, far + at), when=lambda: inner)

    @scoped
    def s5(u):
        o, w = REDUCE[u]
        cols = pl.ds(o, w)
        arrived(zp.at[:, :, cols], f"zp{u}")
        arrived(zx.at[:, :, cols], f"zx{u}")
        for j in range(2):
            fin[j, :, cols] = (
                zs[j, z, :, cols].astype(f32) + zp[j, :, cols].astype(f32) + zx[j, :, cols].astype(f32)
            )
        local(fin.at[k, :, cols], gp_out.at[k, :, cols], f"fl{u}")
        send(fin.at[other, :, cols], gp_out.at[k, :, cols], f"fr{u}", (pn, z))

    @scoped
    def s6(u):
        o, w = REDUCE[u]
        cols = pl.ds(o, w)
        arrived(gp_out.at[k, :, cols], f"fl{u}")
        arrived(gp_out.at[other, :, cols], f"fr{u}")

    pl.semaphore_wait(barrier, 9)

    for copy in packing:
        copy.wait()
    seg_send()
    zstage(0)
    zstage(1)
    activation(x_in, xs, "ax", near)
    zstage(2, outer)
    zstage(3, outer)
    slab_in(0)
    xysend(0)
    slab_in(1)
    xysend(1)
    zstage(2, inner)
    zstage(3, inner)
    zstage(4)
    zstage(5)
    activation(x_in, xs, "ax", away)
    slab_in(2, inner)
    slab_in(3, inner)
    arrived(sg, "seg")
    positions = (lax.broadcasted_iota(jnp.int32, (1, 1024), 1) - sg[...]).astype(f32)
    angles = freq[:, 0:1] * positions
    cosr[...] = jnp.cos(angles)
    sinr[...] = jnp.sin(angles)
    starts = sg[...].astype(f32)
    column = jnp.broadcast_to(starts, (128, 1024)).T

    @pl.loop(0, 8)
    def _(i):
        r = lanes(i * 128, 128)
        here = jnp.broadcast_to(sg[:, r].astype(f32), (1024, 128))
        big[:, r] = jnp.where(column == here, 0.0, neg_large)

    diag(0)
    diag(1)
    slab_in(2, outer)
    xysend(2)
    done(0)
    first = land.at[:, pl.ds(0, 128)]
    spare = wm.at[:, pl.ds(512, 128)]

    @pl.when(k == 0)
    def _():
        local(first, spare, "cm")

    @pl.when(k == 1)
    def _():
        local(first, gains, "cg")

    send(first, spare, "cm", (pn, z), when=lambda: k == 0)
    send(first, gains, "cg", (pn, z), when=lambda: k == 1)
    local(land.at[:, pl.ds(128, 384)], wq.at[0], "cq0")
    arrived(gains, "cg")
    gain_rows = gains[...].astype(f32).T
    grow[...] = gain_rows[0:8]
    done(1)
    local(land.at[:, pl.ds(512, 384)], wq.at[1], "cq1")
    local(land.at[:, pl.ds(896, 384)], wq.at[2], "cq2")

    def queries(half):
        for i in range(2):
            at = half * 512 + i * 256
            xb = xs[rows(at, 256), :].astype(f32)
            c = xb - jnp.mean(xb, -1, keepdims=True)
            n = c * lax.rsqrt(jnp.mean(c * c, -1, keepdims=True) + norm_eps)
            h1t[:, lanes(at, 256)] = (n * grow[0:1, :]).astype(bf16).T

        cols = lanes(half * 512, 512)

        @pl.loop(0, 3)
        def _(p):
            t = times(wq[p].T, h1t[:, cols])
            c = cosr[:, cols]
            s = sinr[:, cols]
            for hh in range(4):
                u1 = t[hh * 64 : hh * 64 + 32]
                u2 = t[hh * 64 + 32 : hh * 64 + 64]
                scale = HEAD_DIM**-0.5 if hh < 2 else 1.0
                qk[p, hh * 64 : hh * 64 + 32, cols] = ((u1 * c - u2 * s) * scale).astype(bf16)
                qk[p, hh * 64 + 32 : hh * 64 + 64, cols] = ((u2 * c + u1 * s) * scale).astype(bf16)
            qk[p, 256:384, cols] = t[256:384].astype(bf16)

    share_activation(xs, "ax", k == zh)
    shared_activation(xs, "ax", k != zh)
    for p in range(3):
        arrived(wq.at[p], f"cq{p}")
    slab_in(4, inner)
    slab_in(5, inner)
    slab_in(3, outer)
    xysend(3)
    with scope("qkvnear"):
        queries(zh)
    diag(2)
    slab_in(4, outer)
    xysend(4)
    share_activation(xs, "ax", k != zh)
    shared_activation(xs, "ax", k == zh)
    with scope("qkvfar"):
        queries(1 - zh)
    slab_in(5, outer)
    xysend(5)
    diag(3)

    @scoped
    def weight_done(u):
        done(u)
        o, w = GATHER[u]
        if u == 2:
            pieces = [(land.at[:, pl.ds(o, w)], wa.at[k], None)]
        elif u == 3:
            pieces = [(land.at[:, pl.ds(o, w)], wi.at[k, :, pl.ds(0, 640)], None)]
        elif u == 4:
            pieces = [(land.at[:, pl.ds(o, w)], wi.at[k, :, pl.ds(640, 512)], None)]
        else:
            pieces = [
                (land.at[:, pl.ds(o, w)], wm.at[:, pl.ds(0, 512)], lambda: k == 0),
                (land.at[:, pl.ds(o, w)], wm.at[:, pl.ds(640, 512)], lambda: k == 1),
            ]
        for src, dst, when in pieces:
            if when is None:
                local(src, dst, f"cw{u}")
            else:
                pl.when(when())(lambda src=src, dst=dst: local(src, dst, f"cw{u}") and None)
            send(src, dst, f"pw{u}", (pn, z), when=when)

    @scoped
    def weight_here(u):
        if u == 2:
            mine, theirs = [(wa.at[k], None)], [(wa.at[other], None)]
        elif u == 3:
            mine, theirs = [(wi.at[k, :, pl.ds(0, 640)], None)], [(wi.at[other, :, pl.ds(0, 640)], None)]
        elif u == 4:
            mine, theirs = [(wi.at[k, :, pl.ds(640, 512)], None)], [(wi.at[other, :, pl.ds(640, 512)], None)]
        else:
            low, high = wm.at[:, pl.ds(0, 512)], wm.at[:, pl.ds(640, 512)]
            mine, theirs = [(low, k == 0), (high, k == 1)], [(low, k == 1), (high, k == 0)]
        for group, name in ((mine, "cw"), (theirs, "pw")):
            for ref, when in group:
                if when is None:
                    arrived(ref, f"{name}{u}")
                else:
                    pl.when(when)(lambda ref=ref, name=name: arrived(ref, f"{name}{u}"))

    for h in range(6):
        rsem(f"e{h}")
        rsem(f"o{h}")
    first_send = count["send"]
    count["send"] += 6
    forward_steps = {
        0: lambda: (activation(dy_in, dys, "ay"), diag(4)),
        2: lambda: (weight_done(2), diag(5)),
        3: lambda: weight_done(3),
        4: lambda: (weight_done(4), weight_done(5)),
    }

    @pl.loop(0, 6)
    def _(h):
        p, hh = h // 2, lax.rem(h, 2)
        qrow, krow, vrow = (rows(at + hh * 64, 64) for at in (0, 128, 256))
        orow = rows(k * 384 + h * 64, 64)

        @pl.when(h >= 2)
        def _():
            pltpu.make_async_copy(probs.at[hh], keep.at[h - 2], rs_.at[names["e0"] + 2 * (h - 2)]).wait()

        s = dims(qk[p, krow, :], qk[p, qrow, :], 0, 0) + big[:, 0:1024]
        e = jnp.exp(s - jnp.max(s, 0, keepdims=True))
        r = 1.0 / jnp.sum(e, 0, keepdims=True)
        eb = e.astype(bf16)
        probs[hh] = eb
        otb[orow, :] = (times(qk[p, vrow, :], eb) * r).astype(bf16)
        rl[pl.ds(h, 1), :] = r
        pltpu.make_async_copy(probs.at[hh], keep.at[h], rs_.at[names["e0"] + 2 * h]).start()
        pltpu.make_async_remote_copy(
            src_ref=otb.at[orow, :], dst_ref=otb.at[orow, :], send_sem=sends.at[first_send + h],
            recv_sem=rs_.at[names["o0"] + 2 * h], device_id=(pn, z), device_id_type=MESH,
        ).start()
        for at, step in forward_steps.items():
            pl.when(h == at)(lambda step=step: step() and None)

    for h in range(6):
        drains.append((first_send + h, otb.at[pl.ds(0, 64), :], None))

    for u in range(2, 6):
        weight_here(u)
    arrived(spare, "cm")
    for h in range(6):
        arrived(otb.at[rows(other * 384 + h * 64, 64), :], f"o{h}")
    arrived(probs.at[0], "e4")
    arrived(probs.at[1], "e5")

    mine = rows(k * 512, 512)
    theirs = rows(other * 512, 512)
    my_lanes = lanes(k * 512, 512)
    ot_mine = otb[:, my_lanes]
    x1[:, 0:384] = xs[mine, 0:384].astype(f32) + dims(ot_mine, wa[0], 0, 0)
    x1[:, 384:768] = xs[mine, 384:768].astype(f32) + dims(ot_mine, wa[1], 0, 0)
    xx = x1[...]
    c = xx - jnp.mean(xx, -1, keepdims=True)
    n = c * lax.rsqrt(jnp.mean(c * c, -1, keepdims=True) + norm_eps)
    h2[mine, :] = (n * grow[1:2, :]).astype(bf16)
    send(h2.at[mine, :], h2.at[mine, :], "h2", (pn, z))
    share_activation(dys, "ay")
    for o, w in ((0, 512), (512, 512), (1024, 128)):
        cols = pl.ds(o, w)
        a = times(h2[mine, :], wi[0, :, cols])
        b = times(h2[mine, :], wi[1, :, cols])
        phi = 0.5 * (1.0 + lax.erf(a * 0.7071067811865476))
        gelu = a * phi
        e = times(dys[mine, :], wm[:, cols])
        hid[:, cols] = (gelu * b).astype(bf16)
        dgo[0, :, cols] = (e * (b * (phi + a * (jnp.exp(-0.5 * a * a) * 0.3989422804014327)))).astype(bf16)
        dgo[1, :, cols] = (e * gelu).astype(bf16)
    send(hid.at[:, lanes(other * 512, 640)], hidp, "hid", (pn, z))
    send(dgo.at[other], dgp, "dg", (pn, z))

    lo[...] = (x1[...] + dims(hid[...], wm[...], 1, 1)).astype(bf16)
    give_back(lo, lo_out, "alo")
    shared_activation(dys, "ay")
    arrived(hidp, "hid")
    t = (
        dims(dys[mine, :], hid[:, lanes(k * 512, 640)], 0, 0) + dims(dys[theirs, :], hidp[...], 0, 0)
    ).astype(bf16)

    @pl.when(k == 0)
    def _():
        grad[:, MLP : MLP + 512] = t[:, 0:512]
        grad[:, 0:128] = t[:, 512:640]

    @pl.when(k == 1)
    def _():
        grad[:, MLP : MLP + 512] = t[:, 128:640]

    s1("m")
    arrived(h2.at[theirs, :], "h2")
    arrived(dgp, "dg")
    for name, o, w in (("i0", 0, 640), ("i1", 640, 512)):
        cols = pl.ds(o, w)
        grad[:, IN + o : IN + o + w] = (
            dims(h2[mine, :], dgo[k, :, cols], 0, 0) + dims(h2[theirs, :], dgp[:, cols], 0, 0)
        ).astype(bf16)
        if name == "i0":
            s1(name)
    f2 = dims(dgo[0], wi[0], 1, 1) + dims(dgo[1], wi[1], 1, 1)
    xx = x1[...]
    c = xx - jnp.mean(xx, -1, keepdims=True)
    r2 = lax.rsqrt(jnp.mean(c * c, -1, keepdims=True) + norm_eps)
    n = c * r2
    grow[3:4, :] = jnp.sum(f2 * n, 0, keepdims=True)
    cc = f2 * grow[1:2, :]
    dx = dys[mine, :].astype(f32) + r2 * (
        cc - jnp.mean(cc, -1, keepdims=True) - n * jnp.mean(cc * n, -1, keepdims=True)
    )
    x1[...] = dx
    dx1b[...] = dx.astype(bf16)
    send(dx1b.at[:, lanes(other * 384, 384)], dx1bp, "dx1b", (pn, z))
    for part in range(2):
        which = other if part == 0 else k
        col = lanes(which * 384, 384)
        feat = rows(which * 384, 384)
        left = jnp.concatenate([wa[0, feat, :], wa[1, feat, :]], axis=1)
        t = dims(left, dx1b[...], 1, 1).astype(bf16)
        if part == 0:
            dot_send[...] = t
            send(dot_send, dot_own.at[:, my_lanes], "do", (pn, z))
        else:
            dot_own[:, my_lanes] = t
    local(keep.at[5], probs.at[1], "e5")
    local(keep.at[4], probs.at[0], "e4")

    s2("m")
    s1("i1")
    arrived(dx1bp, "dx1b")
    grad[:, ATTN : ATTN + 384] = (
        times(otb[:, my_lanes], dx1b[:, lanes(k * 384, 384)])
        + times(otb[:, lanes(other * 512, 512)], dx1bp[...])
    ).astype(bf16)
    arrived(dot_own.at[:, lanes(other * 512, 512)], "do")

    for h in range(6):
        rsem(f"b{h}")
    backward_steps = {
        4: lambda: (s2("i0"), s3("m")),
        3: lambda: (s2("i1"), s1("a"), s1("q2")),
        2: lambda: (s3("i0"), s4("m")),
        1: lambda: s3("i1"),
        0: lambda: (s2("a"), s4("i0")),
    }

    @pl.loop(0, 6)
    def _(turn):
        h = 5 - turn
        p, hh = h // 2, lax.rem(h, 2)
        qrow, krow, vrow = (rows(at + hh * 64, 64) for at in (0, 128, 256))
        arrived_at = rs_.at[names["e0"] + 2 * h]
        pltpu.make_async_copy(keep.at[h], probs.at[hh], arrived_at).wait()
        vt = qk[p, vrow, :]
        kt = qk[p, krow, :]
        for i in range(2):
            cols = slice(i * 512, i * 512 + 512)
            do = dot_own[rows(h * 64, 64), cols].astype(f32) * rl[pl.ds(h, 1), cols]
            delta = jnp.sum(do * otb[rows(k * 384 + h * 64, 64), cols].astype(f32), 0, keepdims=True)
            dob = do.astype(bf16)
            e = probs[hh, :, cols]
            ds = (e.astype(f32) * (dims(vt, dob, 0, 0) - delta)).astype(bf16)
            dk = dims(qk[p, qrow, cols], ds, 1, 1)
            dv = dims(dob, e, 1, 1)
            if i == 0:
                dkb[...] = dk
                dvb[...] = dv
            else:
                dkb[...] += dk
                dvb[...] += dv
            dq = times(kt, ds) * HEAD_DIM**-0.5
            c = cosr[:, cols]
            s = sinr[:, cols]
            qk[p, rows(hh * 64, 32), cols] = (dq[:32] * c + dq[32:] * s).astype(bf16)
            qk[p, rows(hh * 64 + 32, 32), cols] = (dq[32:] * c - dq[:32] * s).astype(bf16)

        @pl.when(h >= 2)
        def _():
            pltpu.make_async_copy(keep.at[h - 2], probs.at[hh], rs_.at[names["e0"] + 2 * (h - 2)]).start()

        d = dkb[...]
        c = cosr[...]
        s = sinr[...]
        qk[p, rows(128 + hh * 64, 32), :] = (d[:32] * c + d[32:] * s).astype(bf16)
        qk[p, rows(160 + hh * 64, 32), :] = (d[32:] * c - d[:32] * s).astype(bf16)
        qk[p, vrow, :] = dvb[...].astype(bf16)

        @pl.when(h == 4)
        def _():
            grad[:, lanes(PAIR + 384 * p, 384)] = dims(h1t[...], qk[p], 1, 1).astype(bf16)

        for at, step in backward_steps.items():
            pl.when(h == at)(lambda step=step: step() and None)

    def f1_part(cols):
        return times(wq[0], qk[0, :, cols]) + times(wq[1], qk[1, :, cols]) + times(wq[2], qk[2, :, cols])

    big[0:768, 0:512] = f1_part(lanes(other * 512, 512))
    send(big.at[pl.ds(0, 768), pl.ds(0, 512)], f1r, "f1", (pn, z))
    big[0:768, 512:1024] = f1_part(my_lanes)
    s2("q2")
    s4("i1")
    arrived(f1r, "f1")
    f1 = (big[0:768, 512:1024] + f1r[...]).T
    xx = xs[mine, :].astype(f32)
    c = xx - jnp.mean(xx, -1, keepdims=True)
    r1 = lax.rsqrt(jnp.mean(c * c, -1, keepdims=True) + norm_eps)
    n = c * r1
    grow[2:3, :] = jnp.sum(f1 * n, 0, keepdims=True)
    cc = f1 * grow[0:1, :]
    gi[...] = (
        x1[...] + r1 * (cc - jnp.mean(cc, -1, keepdims=True) - n * jnp.mean(cc * n, -1, keepdims=True))
    ).astype(bf16)
    send(grow, growp, "gr", (pn, z), when=lambda: k == 0)

    @pl.when(k == 1)
    def _():
        arrived(growp, "gr")
        two = jnp.concatenate([grow[2:4, :] + growp[2:4, :], jnp.zeros((126, 768), f32)], axis=0)
        grad[:, 0:128] = two.T.astype(bf16)

    s1("g")
    give_back(gi, gi_out, "agi", (0,))
    give_back(gi, gi_out, "agi", (1,), inner)
    for p in (1, 0):
        grad[:, PAIR + 384 * p : PAIR + 384 * p + 384] = dims(h1t[...], qk[p], 1, 1).astype(bf16)
        s1(f"q{p}")
        if p == 1:
            s3("a")
    s3("q2")
    s5("m")
    s4("a")
    s2("q1")
    s2("g")
    s4("q2")
    s5("i0")
    s2("q0")
    s5("i1")
    s3("q1")
    s3("g")
    s3("q0")
    give_back(gi, gi_out, "agi", (1,), outer)
    s5("a")
    s4("q1")
    s4("g")
    s4("q0")
    s5("q2")
    s5("q1")
    s5("g")
    s5("q0")
    for u in REDUCE:
        s6(u)
    given_back(lo_out, "alo")
    given_back(gi_out, "agi")
    drain_all()
    assert len(names) <= 160 and count["send"] <= 220 and len(packing) + len(small) <= 32


frequency = np.broadcast_to(
    (np.float32(rope_base) ** (-(np.arange(32, dtype=np.float32) * 2) / HEAD_DIM))[:, None], (32, 128)
).astype(np.float32)


def finish_kernel(
    lo_raw, gi_raw, gp_raw, lo, gi, o_qkv, o_attn, o_in, o_mlp, o_one, o_two,
    buf, gp, g_qkv, g_attn, g_in, g_mlp, g_one, g_two, sem,
):
    loads = [
        pltpu.make_async_copy(src, dst, sem.at[i])
        for i, (src, dst) in enumerate(((gp_raw, gp), (lo_raw, buf.at[0]), (gi_raw, buf.at[1])))
    ]
    for copy in loads:
        copy.start()
    pairs = ((buf.at[0], lo), (buf.at[1], gi), (g_qkv, o_qkv), (g_attn, o_attn), (g_in, o_in), (g_mlp, o_mlp), (g_one, o_one), (g_two, o_two))
    stores = [pltpu.make_async_copy(src, dst, sem.at[3 + i]) for i, (src, dst) in enumerate(pairs)]
    loads[0].wait()
    for c in range(2):
        for p in range(3):
            for t in range(3):
                o = 768 * t + 384 * c + 128 * p
                at = PAIR + 384 * p + 128 * t
                g_qkv[:, o : o + 128] = gp[c, :, at : at + 128]
        g_attn[:, 384 * c : 384 * c + 384] = gp[c, :, ATTN : ATTN + 384]
        g_in[:, 1152 * c : 1152 * c + 1152] = gp[c, :, IN : IN + 1152]
    g_mlp[:, 0:512] = gp[0, :, MLP : MLP + 512]
    g_mlp[:, 512:640] = gp[0, :, 0:128]
    g_mlp[:, 640:1152] = gp[1, :, MLP : MLP + 512]
    flat = jnp.concatenate([gp[1, :, 0:128], jnp.zeros((104, 128), f32)], axis=0).T
    g_one[...] = flat[0:1, 0:24]
    g_two[...] = flat[1:2, 0:24]
    for load, store in zip(loads[1:], stores[:2]):
        load.wait()
        store.start()
    for store in stores[2:]:
        store.start()
    for store in stores:
        store.wait()


def fast(layer_in, seg_start, out_grad, w_qkv, w_attn_out, w_in, w_mlp_out, norm_attn, norm_mlp):
    hbm = pl.BlockSpec(memory_space=pltpu.HBM)
    V = pltpu.VMEM
    outs = pl.pallas_call(
        step_kernel,
        name="layer",
        out_shape=[
            jax.ShapeDtypeStruct((2, 256, 768), bf16),
            jax.ShapeDtypeStruct((2, 256, 768), bf16),
            jax.ShapeDtypeStruct((2, 24, WIDTH), f32),
            jax.ShapeDtypeStruct((768, WIDTH), bf16),
            jax.ShapeDtypeStruct((6, 1024, 1024), bf16),
        ],
        in_specs=[hbm] * 10,
        out_specs=[hbm] * 5,
        scratch_shapes=[
            V((2, 24, WIDTH), bf16),
            V((8, 128), f32),
            V((2, 256), jnp.int32),
            V((1, 24), bf16),
            V((1, 24), bf16),
            V((32, 128), f32),
            V((1024, 768), bf16),
            V((1024, 768), bf16),
            V((1, 1024), jnp.int32),
            V((768, 1024), bf16),
            V((3, 768, 384), bf16),
            V((2, 768, 384), bf16),
            V((2, 768, 1152), bf16),
            V((768, 1152), bf16),
            V((768, 128), bf16),
            V((32, 1024), f32),
            V((32, 1024), f32),
            V((3, 384, 1024), bf16),
            V((1024, 1152), f32),
            V((2, 1024, 1024), bf16),
            V((768, 1024), bf16),
            V((8, 1024), f32),
            V((512, 768), f32),
            V((1024, 768), bf16),
            V((512, 1152), bf16),
            V((512, 640), bf16),
            V((2, 512, 1152), bf16),
            V((512, 1152), bf16),
            V((512, 768), bf16),
            V((512, 384), bf16),
            V((384, 512), bf16),
            V((384, 1024), bf16),
            V((768, 512), f32),
            V((512, 768), bf16),
            V((512, 768), bf16),
            V((768, WIDTH), bf16),
            V((8, 768), f32),
            V((8, 768), f32),
            V((64, 1024), f32),
            V((64, 1024), f32),
            V((2, 96, WIDTH), bf16),
            V((2, 96, WIDTH), bf16),
            V((96, WIDTH), bf16),
            V((96, WIDTH), bf16),
            V((2, 4, 24, WIDTH), bf16),
            V((2, 24, WIDTH), bf16),
            V((2, 2, 24, WIDTH), bf16),
            V((2, 24, WIDTH), bf16),
            V((2, 24, WIDTH), f32),
            pltpu.SemaphoreType.DMA((160,)),
            pltpu.SemaphoreType.DMA((32,)),
            pltpu.SemaphoreType.DMA((220,)),
        ],
        compiler_params=pltpu.CompilerParams(
            collective_id=0, has_side_effects=True, vmem_limit_bytes=67043328
        ),
    )(
        layer_in, out_grad, seg_start, w_qkv, w_attn_out, w_in, w_mlp_out,
        norm_attn[None], norm_mlp[None], frequency,
    )
    done = pl.pallas_call(
        finish_kernel,
        name="finish",
        out_shape=[
            jax.ShapeDtypeStruct((2, 256, 768), bf16),
            jax.ShapeDtypeStruct((2, 256, 768), bf16),
            jax.ShapeDtypeStruct((24, 2304), f32),
            jax.ShapeDtypeStruct((24, 768), f32),
            jax.ShapeDtypeStruct((24, 2304), f32),
            jax.ShapeDtypeStruct((24, 1152), f32),
            jax.ShapeDtypeStruct((1, 24), f32),
            jax.ShapeDtypeStruct((1, 24), f32),
        ],
        in_specs=[hbm, hbm, hbm],
        out_specs=[hbm] * 8,
        scratch_shapes=[
            V((2, 2, 256, 768), bf16),
            V((2, 24, WIDTH), f32),
            V((24, 2304), f32),
            V((24, 768), f32),
            V((24, 2304), f32),
            V((24, 1152), f32),
            V((1, 24), f32),
            V((1, 24), f32),
            pltpu.SemaphoreType.DMA((11,)),
        ],
    )(*outs[:3])
    return (*done[:6], done[6][0], done[7][0])


def normalize(values):
    centered = values - jnp.mean(values, axis=-1, keepdims=True)
    spread = jnp.mean(centered * centered, axis=-1, keepdims=True)
    return centered * lax.rsqrt(spread + norm_eps)


def rope_tables(positions):
    half_dim = HEAD_DIM // 2
    frequency = rope_base ** (-(jnp.arange(half_dim).astype(jnp.float32) * 2.0) / HEAD_DIM)
    angles = positions.astype(jnp.float32)[:, None] * frequency[None, :]
    angles = jnp.concatenate([angles, angles], axis=-1)
    return (jnp.cos(angles), jnp.sin(angles))


def turn_half(values):
    half_dim = values.shape[-1] // 2
    return jnp.concatenate([-values[..., half_dim:], values[..., :half_dim]], axis=-1)


def rotate(values, cosine_table, sine_table):
    return values * cosine_table[:, None, :] + turn_half(values) * sine_table[:, None, :]


def unrotate(values, cosine_table, sine_table):
    return values * cosine_table[:, None, :] - turn_half(values) * sine_table[:, None, :]


def product(left, right):
    return jnp.dot(left, right, preferred_element_type=jnp.float32)


def left_transposed(left, right):
    return lax.dot_general(
        left, right, (((0,), (0,)), ((), ())), preferred_element_type=jnp.float32
    )


def right_transposed(left, right):
    return lax.dot_general(
        left, right, (((1,), (1,)), ((), ())), preferred_element_type=jnp.float32
    )


def to_groups(array):
    row_count, head_count, head_size = array.shape
    return array.reshape(row_count, head_count // 4, 4, head_size).transpose(1, 0, 2, 3)


def from_groups(array):
    group_count, row_count, group_heads, head_size = array.shape
    return array.transpose(1, 0, 2, 3).reshape(row_count, group_count * group_heads, head_size)


def attend_group(group_in, same_doc):
    query_part, key_part, value_part = group_in
    scores = jnp.einsum(
        "qhd,khd->hqk", query_part, key_part, preferred_element_type=jnp.float32
    ) * HEAD_DIM ** (-0.5)
    masked = jnp.where(same_doc[None], scores, neg_large)
    highest = jnp.max(masked, axis=-1, keepdims=True)
    shifted = jnp.exp(masked - highest)
    totals = jnp.sum(shifted, axis=-1, keepdims=True)
    attn_prob = shifted / totals
    log_total = highest + jnp.log(totals)
    mixed_out = jnp.einsum(
        "hqk,khd->qhd",
        attn_prob.astype(jnp.bfloat16),
        value_part,
        preferred_element_type=jnp.float32,
    )
    return (mixed_out, log_total[..., 0])


def attend_back(group_in, same_doc):
    query_part, key_part, value_part, grad_part, log_total = group_in
    scores = jnp.einsum(
        "qhd,khd->hqk", query_part, key_part, preferred_element_type=jnp.float32
    ) * HEAD_DIM ** (-0.5)
    attn_prob = jnp.where(same_doc[None], jnp.exp(scores - log_total[..., None]), 0.0)
    grad_prob = jnp.einsum(
        "qhd,khd->hqk", grad_part, value_part, preferred_element_type=jnp.float32
    )
    inner_sum = jnp.sum(attn_prob * grad_prob, axis=-1, keepdims=True)
    grad_score = (attn_prob * (grad_prob - inner_sum)).astype(jnp.bfloat16)
    grad_query = jnp.einsum(
        "hqk,khd->qhd", grad_score, key_part, preferred_element_type=jnp.float32
    ) * HEAD_DIM ** (-0.5)
    grad_key = jnp.einsum(
        "hqk,qhd->khd", grad_score, query_part, preferred_element_type=jnp.float32
    ) * HEAD_DIM ** (-0.5)
    grad_value = jnp.einsum(
        "hqk,qhd->khd",
        attn_prob.astype(jnp.bfloat16),
        grad_part,
        preferred_element_type=jnp.float32,
    )
    return (grad_query, grad_key, grad_value)


def scaled_norm(values_in, gain_row):
    return normalize(values_in) * gain_row


def geglu(first_half, second_half):
    return jax.nn.gelu(first_half, approximate=False) * second_half


def local(layer_in, seg_start, out_grad, w_qkv, w_attn_out, w_in, w_mlp_out, norm_attn, norm_mlp):
    micro_count = layer_in.shape[0]
    span_len = layer_in.shape[1]
    model_width = layer_in.shape[2]
    ctx_rank = lax.axis_index("ctx")
    grad_sums = (
        jnp.zeros((model_width, 3 * model_width), jnp.float32),
        jnp.zeros((model_width, model_width), jnp.float32),
        jnp.zeros((model_width, 2 * FF), jnp.float32),
        jnp.zeros((model_width, FF), jnp.float32),
        jnp.zeros((model_width,), jnp.float32),
        jnp.zeros((model_width,), jnp.float32),
    )
    offsets = ctx_rank * span_len + jnp.arange(span_len, dtype=jnp.int32)
    outputs = []
    grad_inputs = []
    for micro_step in range(micro_count):
        gathered = (
            lax.all_gather(w_qkv, ("dp", "ctx"), axis=0, tiled=True),
            lax.all_gather(w_attn_out, ("dp", "ctx"), axis=0, tiled=True),
            lax.all_gather(w_in, ("dp", "ctx"), axis=0, tiled=True),
            lax.all_gather(w_mlp_out, ("dp", "ctx"), axis=0, tiled=True),
            lax.all_gather(norm_attn, ("dp", "ctx"), axis=0, tiled=True),
            lax.all_gather(norm_mlp, ("dp", "ctx"), axis=0, tiled=True),
        )
        qkv_full, attn_full, in_full, mlp_full, gain_attn, gain_mlp = gathered
        starts_here = seg_start[micro_step]
        hidden = layer_in[micro_step].astype(jnp.float32)
        cosine_table, sine_table = rope_tables(offsets - starts_here)
        normed, norm_back = jax.vjp(scaled_norm, hidden, gain_attn.astype(jnp.float32))
        normed_low = normed.astype(jnp.bfloat16)
        qkv_local = product(normed_low, qkv_full).reshape(span_len, 3, HEADS, HEAD_DIM)
        queries = rotate(qkv_local[:, 0], cosine_table, sine_table).astype(jnp.bfloat16)
        keys_here = rotate(qkv_local[:, 1], cosine_table, sine_table).astype(jnp.bfloat16)
        values_here = qkv_local[:, 2].astype(jnp.bfloat16)
        keys_all, values_all, starts_all = (
            lax.all_gather(keys_here, "ctx", axis=0, tiled=True),
            lax.all_gather(values_here, "ctx", axis=0, tiled=True),
            lax.all_gather(starts_here, "ctx", axis=0, tiled=True),
        )
        same_doc = starts_here[:, None] == starts_all[None, :]
        query_groups = to_groups(queries)
        key_groups = to_groups(keys_all)
        value_groups = to_groups(values_all)
        mixed_out, log_total = lax.map(
            lambda group_in: attend_group(group_in, same_doc),
            (query_groups, key_groups, value_groups),
        )
        attended = from_groups(mixed_out).reshape(span_len, model_width).astype(jnp.bfloat16)
        middle = hidden + product(attended, attn_full)
        normed_mlp, norm_mlp_back = jax.vjp(scaled_norm, middle, gain_mlp.astype(jnp.float32))
        normed_mlp_low = normed_mlp.astype(jnp.bfloat16)
        projected = product(normed_mlp_low, in_full)
        gated_out, geglu_back = jax.vjp(geglu, projected[:, :FF], projected[:, FF:])
        gated_low = gated_out.astype(jnp.bfloat16)
        result = middle + right_transposed(gated_low, mlp_full)
        outputs.append(result.astype(jnp.bfloat16))
        qkv_full, attn_full, in_full, mlp_full = (
            lax.all_gather(w_qkv, ("dp", "ctx"), axis=0, tiled=True),
            lax.all_gather(w_attn_out, ("dp", "ctx"), axis=0, tiled=True),
            lax.all_gather(w_in, ("dp", "ctx"), axis=0, tiled=True),
            lax.all_gather(w_mlp_out, ("dp", "ctx"), axis=0, tiled=True),
        )
        grad_out = out_grad[micro_step].astype(jnp.float32)
        grad_out_low = out_grad[micro_step]
        grad_mlp_weight = left_transposed(grad_out_low, gated_low)
        grad_gated = product(grad_out_low, mlp_full)
        grad_first, grad_second = geglu_back(grad_gated)
        grad_projected = jnp.concatenate([grad_first, grad_second], axis=1).astype(jnp.bfloat16)
        grad_in_weight = left_transposed(normed_mlp_low, grad_projected)
        grad_normed_mlp = right_transposed(grad_projected, in_full)
        grad_middle_norm, grad_gain_mlp = norm_mlp_back(grad_normed_mlp)
        grad_middle = grad_out + grad_middle_norm
        grad_middle_low = grad_middle.astype(jnp.bfloat16)
        grad_attn_weight = left_transposed(attended, grad_middle_low)
        grad_attended = (
            right_transposed(grad_middle_low, attn_full)
            .astype(jnp.bfloat16)
            .reshape(span_len, HEADS, HEAD_DIM)
        )
        grad_groups = to_groups(grad_attended)
        grad_query_groups, grad_key_groups, grad_value_groups = lax.map(
            lambda group_in: attend_back(group_in, same_doc),
            (query_groups, key_groups, value_groups, grad_groups, log_total),
        )
        keys_total = keys_all.shape[0]
        grad_keys, grad_values = (
            lax.psum_scatter(
                from_groups(grad_key_groups).reshape(keys_total, model_width).astype(jnp.bfloat16),
                "ctx",
                scatter_dimension=0,
                tiled=True,
            ).astype(jnp.float32),
            lax.psum_scatter(
                from_groups(grad_value_groups)
                .reshape(keys_total, model_width)
                .astype(jnp.bfloat16),
                "ctx",
                scatter_dimension=0,
                tiled=True,
            ).astype(jnp.float32),
        )
        grad_qkv = jnp.stack(
            [
                unrotate(from_groups(grad_query_groups), cosine_table, sine_table),
                unrotate(grad_keys.reshape(span_len, HEADS, HEAD_DIM), cosine_table, sine_table),
                grad_values.reshape(span_len, HEADS, HEAD_DIM),
            ],
            axis=1,
        )
        grad_qkv = grad_qkv.reshape(span_len, 3 * model_width).astype(jnp.bfloat16)
        grad_qkv_weight = left_transposed(normed_low, grad_qkv)
        grad_normed = right_transposed(grad_qkv, qkv_full)
        grad_hidden_norm, grad_gain_attn = norm_back(grad_normed)
        grad_inputs.append((grad_middle + grad_hidden_norm).astype(jnp.bfloat16))
        grad_sums = (
            grad_sums[0] + grad_qkv_weight,
            grad_sums[1] + grad_attn_weight,
            grad_sums[2] + grad_in_weight,
            grad_sums[3] + grad_mlp_weight,
            grad_sums[4] + grad_gain_attn,
            grad_sums[5] + grad_gain_mlp,
        )
    shares = (
        lax.psum_scatter(grad_sums[0], ("dp", "ctx"), scatter_dimension=0, tiled=True),
        lax.psum_scatter(grad_sums[1], ("dp", "ctx"), scatter_dimension=0, tiled=True),
        lax.psum_scatter(grad_sums[2], ("dp", "ctx"), scatter_dimension=0, tiled=True),
        lax.psum_scatter(grad_sums[3], ("dp", "ctx"), scatter_dimension=0, tiled=True),
        lax.psum_scatter(grad_sums[4], ("dp", "ctx"), scatter_dimension=0, tiled=True),
        lax.psum_scatter(grad_sums[5], ("dp", "ctx"), scatter_dimension=0, tiled=True),
    )
    return (
        jnp.stack(outputs),
        jnp.stack(grad_inputs),
        shares[0],
        shares[1],
        shares[2],
        shares[3],
        shares[4],
        shares[5],
    )


def solution(mesh):
    A = P(None, ("dp", "ctx"), None)
    S = P(None, ("dp", "ctx"))
    W = P(("dp", "ctx"), None)
    G = P(("dp", "ctx"))
    return jax.shard_map(
        fast if dict(mesh.shape) == {"dp": 8, "ctx": 4} else local,
        mesh=mesh,
        in_specs=(A, S, A, W, W, W, W, G, G),
        out_specs=(A, A, W, W, W, W, G, G),
        check_vma=False,
    )
```

```python
import contextlib

import jax
import jax.numpy as jnp
import numpy as np
from jax import lax
from jax.experimental import pallas as pl
from jax.experimental.pallas import tpu as pltpu
from jax.sharding import PartitionSpec as P

MESH = pl.DeviceIdType.MESH
bf16 = jnp.bfloat16
f32 = jnp.float32

HEADS = 12
HEAD_DIM = 64
FF = 1152
rope_base = 160000.0
norm_eps = 1e-05
neg_large = -1e30

WIDTH = 3328
GATHER = [(0, 512), (512, 768), (1280, 384), (1664, 640), (2304, 512), (2816, 512)]
PAIR = 128
ATTN = 1280
IN = 1664
MLP = 2816
REDUCE = {
    "m": (2816, 512),
    "i0": (1664, 640),
    "i1": (2304, 512),
    "a": (1280, 384),
    "q2": (896, 384),
    "q1": (512, 384),
    "q0": (128, 384),
    "g": (0, 128),
}


TRACE = False


def scope(name):
    return jax.named_scope(name) if TRACE else contextlib.nullcontext()


def scoped(fn):
    def inner(*args):
        with scope(f"{fn.__name__}_{args[0] if args and isinstance(args[0], (int, str)) else ''}"):
            return fn(*args)

    return inner


def dims(left, right, left_at, right_at):
    return lax.dot_general(
        left, right, (((left_at,), (right_at,)), ((), ())), preferred_element_type=f32
    )


def times(left, right):
    return jnp.dot(left, right, preferred_element_type=f32)


def step_kernel(
    x_in, dy_in, seg_raw, w_qkv, w_attn, w_in, w_mlp, g_attn_raw, g_mlp_raw, freq_raw,
    lo_out, gi_out, gp_out, land, keep,
    wp, gcol, seg_in, g_attn, g_mlp, freq,
    xs, dys, sg, h1t, wq, wa, wi, wm, gains, cosr, sinr, qk, big, probs, otb, rl, x1, h2, hid, hidp,
    dgo, dgp, dx1b, dx1bp, dot_send, dot_own, f1r, lo, gi, grad, grow, growp, dkb, dvb,
    ra, rb, ra2, rb2, zs, zp, zm, zx, fin,
    rs_, ls_, sends,
):
    dp = lax.axis_index("dp")
    z = lax.axis_index("ctx")
    q = dp // 2
    k = lax.rem(dp, 2)
    other = 1 - k
    pn = dp + 1 - 2 * k
    xn = dp + 2 - 4 * lax.rem(dp // 2, 2)
    yn = dp + 4 - 8 * (dp // 4)
    zn = z + 1 - 2 * lax.rem(z, 2)
    zb = jnp.where(z < 2, 2, 1)
    zh = z // 2
    qx = q + 1 - 2 * lax.rem(q, 2)
    qy = q + 2 - 4 * (q // 2)
    qd = qx + 2 - 4 * (qx // 2)
    inner = jnp.logical_or(z == 1, z == 2)
    outer = jnp.logical_or(z == 0, z == 3)
    near = k == zh
    away = k != zh
    names = {}
    count = {"send": 0, "local": 0}
    drains = []

    def rsem(name):
        return rs_.at[names.setdefault(name, len(names))]

    def still(view):
        index = view.transforms[0].indices
        return view.ref.at[tuple(pl.ds(0, at.size) if hasattr(at, "size") else 0 for at in index)]

    keyed = {}

    def send(src, dst, name, dev, when=None, sem=None, key=None):
        first = key is None or key not in keyed
        if first:
            i = count["send"]
            count["send"] += 1
            keyed[key] = i
        else:
            i = keyed[key]
        copy = pltpu.make_async_remote_copy(
            src_ref=src, dst_ref=dst, send_sem=sends.at[i], recv_sem=rsem(name) if sem is None else sem,
            device_id=dev, device_id_type=MESH,
        )
        if when is None:
            copy.start()
        else:
            pl.when(when())(copy.start)
        if first:
            drains.append((i, src, when))

    def drain_all():
        for i, src, when in drains:
            view = still(src) if hasattr(src, "transforms") else src

            def wait(view=view, i=i):
                pltpu.make_async_copy(view, view, sends.at[i]).wait()

            if when is None:
                wait()
            else:
                pl.when(when())(wait)

    def local(src, dst, name):
        copy = pltpu.make_async_copy(src, dst, rsem(name))
        copy.start()
        return copy

    def arrived(ref, name):
        pltpu.make_async_copy(ref, ref, rsem(name)).wait()

    def rows(start, size):
        return pl.ds(pl.multiple_of(start, 8), size)

    def lanes(start, size):
        return pl.ds(pl.multiple_of(start, 128), size)

    barrier = pltpu.get_barrier_semaphore()
    for dz in range(1, 4):
        for kk in range(2):
            pl.semaphore_signal(
                barrier, inc=1, device_id=(2 * q + kk, lax.rem(z + dz, 4)), device_id_type=MESH
            )
    for dev in (pn, xn, yn):
        pl.semaphore_signal(barrier, inc=1, device_id=(dev, z), device_id_type=MESH)

    packs = []
    for c in range(2):
        for p in range(3):
            for t in range(3):
                packs.append((w_qkv, 768 * t + 384 * c + 128 * p, c, PAIR + 384 * p + 128 * t, 128))
        packs.append((w_attn, 384 * c, c, ATTN, 384))
        packs.append((w_in, 1152 * c, c, IN, 1152))
        packs.append((w_mlp, 640 * c, c, MLP, 512))
    packs.append((w_mlp, 512, 0, 0, 128))
    packing = [
        pltpu.make_async_copy(w.at[:, pl.ds(o, n)], wp.at[c, :, pl.ds(at, n)], ls_.at[i])
        for i, (w, o, c, at, n) in enumerate(packs)
    ]
    small = [
        pltpu.make_async_copy(src, dst, ls_.at[len(packs) + i])
        for i, (src, dst) in enumerate(
            ((g_attn_raw, g_attn), (g_mlp_raw, g_mlp), (seg_raw, seg_in), (freq_raw, freq))
        )
    ]
    for copy in small + packing:
        copy.start()
    gcol[...] = jnp.zeros_like(gcol)
    for copy in small:
        copy.wait()
    gcol[0:1, 0:24] = g_attn[...].astype(f32)
    gcol[1:2, 0:24] = g_mlp[...].astype(f32)
    columns = jnp.concatenate([gcol[...], jnp.zeros((120, 128), f32)], axis=0).T[0:24].astype(bf16)
    wp[1, :, 0:128] = columns

    @scoped
    def zstage(u, turn=None):
        o, w = GATHER[u]
        cols = pl.ds(o, w)

        def body():
            dst = land.at[rows(dp * 96 + z * 24, 24), cols]
            for c in range(2):
                src = wp.at[c, :, cols]
                send(src, dst, f"z{u}", (2 * q + c, zn), key=f"zn{u}{c}")
                send(src, dst, f"z{u}", (2 * q + c, zb), key=f"zb{u}{c}")
                send(src, dst, f"z{u}", (pn, z), when=lambda c=c: k != c, key=f"zp{u}{c}")
                pl.when(k == c)(lambda src=src: local(src, dst, f"z{u}") and None)

        in_turn(turn, body)

    def in_turn(turn, body):
        if turn is None:
            body()
        else:
            pl.when(turn)(body)

    @scoped
    def slab_in(u, turn=None):
        o, w = GATHER[u]
        cols = pl.ds(o, w)

        def body():
            arrived(land.at[rows(q * 192, 192), cols], f"z{u}")
            for j in range(2):
                part = land.at[rows((2 * q + j) * 96 + lax.rem(4 - 2 * z + 4, 4) * 24, 48), cols]
                send(part, part, f"z{u}", (dp, zn), when=lambda: inner, key=f"fs{u}{j}")

        in_turn(turn, body)

    @scoped
    def xysend(u):
        o, w = GATHER[u]
        slab = land.at[rows(q * 192, 192), pl.ds(o, w)]
        send(slab, slab, f"x{u}", (xn, z))
        send(slab, slab, f"y{u}", (yn, z))

    @scoped
    def diag(u):
        o, w = GATHER[u]
        cols = pl.ds(o, w)
        arrived(land.at[rows(qx * 192, 192), cols], f"x{u}")
        part = land.at[rows(qx * 192, 96), cols]
        send(part, part, f"dx{u}", (yn, z))
        arrived(land.at[rows(qy * 192, 192), cols], f"y{u}")
        part = land.at[rows(qy * 192 + 96, 96), cols]
        send(part, part, f"dy{u}", (xn, z))

    @scoped
    def done(u):
        o, w = GATHER[u]
        cols = pl.ds(o, w)
        arrived(land.at[rows(qd * 192, 96), cols], f"dx{u}")
        arrived(land.at[rows(qd * 192 + 96, 96), cols], f"dy{u}")

    def activation(src_ref, dst_ref, name, turn=None):
        for j in range(2):
            m = j + k - 2 * j * k
            src = src_ref.at[m]
            dst = dst_ref.at[rows(z * 256, 256), :]
            sem = rs_.at[base[name] + lax.rem(z, 2)]

            def going(j=j):
                there = 2 * k + j + k - 2 * j * k != z
                return there if turn is None else jnp.logical_and(turn, there)

            here = 2 * k + m == z
            if turn is not None:
                here = jnp.logical_and(turn, here)
            send(src, dst, None, (2 * q + zh, 2 * k + m), when=going, sem=sem)
            pl.when(here)(pltpu.make_async_copy(src, dst, sem).start)

    base = {}
    for name in ("ax", "ay", "alo", "agi"):
        base[name] = len(names)
        names[name + "0"] = len(names)
        names[name + "1"] = len(names)

    @scoped
    def share_activation(ref, name, turn=None):
        def body():
            for j in range(2):
                r = rows(k * 512 + j * 256, 256)
                arrived(ref.at[r, :], f"{name}{j}")
                send(ref.at[r, :], ref.at[r, :], f"p{name}{j}", (pn, z), key=f"sh{name}{j}")

        in_turn(turn, body)

    @scoped
    def shared_activation(ref, name, turn=None):
        def body():
            for j in range(2):
                arrived(ref.at[rows(other * 512 + j * 256, 256), :], f"p{name}{j}")

        in_turn(turn, body)

    @scoped
    def give_back(src_ref, out_ref, name, blocks=(0, 1), turn=None):
        m = lax.rem(z, 2)
        for j in blocks:
            src = src_ref.at[pl.ds(j * 256, 256), :]
            dst = out_ref.at[m]
            sem = rs_.at[base[name] + m]

            def going(j=j):
                leaves = jnp.logical_or(2 * k + j != z, zh != k)
                return leaves if turn is None else jnp.logical_and(turn, leaves)

            stays = jnp.logical_and(2 * k + j == z, zh == k)
            if turn is not None:
                stays = jnp.logical_and(turn, stays)
            send(src, dst, None, (2 * q + zh, 2 * k + j), when=going, sem=sem)
            pl.when(stays)(pltpu.make_async_copy(src, dst, sem).start)

    @scoped
    def given_back(out_ref, name):
        for m in range(2):
            arrived(out_ref.at[m], f"{name}{m}")

    def seg_send():
        for m in range(2):
            src = seg_in.at[pl.ds(m, 1), :]
            dst = sg.at[:, lanes(z * 256, 256)]
            for c in range(2):

                def away(m=m, c=c):
                    return jnp.logical_or(2 * k + m != z, k != c)

                send(src, dst, "seg", (2 * q + c, 2 * k + m), when=away)
                pl.when(jnp.logical_not(away()))(pltpu.make_async_copy(src, dst, rsem("seg")).start)

    @scoped
    def s1(u):
        o, w = REDUCE[u]
        cols = pl.ds(o, w)
        for slot, quarter in enumerate((qx, qd)):
            send(grad.at[rows(quarter * 192, 96), cols], ra.at[slot, :, cols], f"ra{u}", (xn, z))
        for slot, quarter in enumerate((qy, qd)):
            send(grad.at[rows(quarter * 192 + 96, 96), cols], rb.at[slot, :, cols], f"rb{u}", (yn, z))

    @scoped
    def s2(u):
        o, w = REDUCE[u]
        cols = pl.ds(o, w)
        arrived(ra.at[:, :, cols], f"ra{u}")
        r = rows(qy * 192, 96)
        grad[r, cols] = (grad[r, cols].astype(f32) + ra[1, :, cols].astype(f32)).astype(bf16)
        send(grad.at[r, cols], ra2.at[:, cols], f"ra2{u}", (yn, z))
        arrived(rb.at[:, :, cols], f"rb{u}")
        r2 = rows(qx * 192 + 96, 96)
        grad[r2, cols] = (grad[r2, cols].astype(f32) + rb[1, :, cols].astype(f32)).astype(bf16)
        send(grad.at[r2, cols], rb2.at[:, cols], f"rb2{u}", (xn, z))

    @scoped
    def s3(u):
        o, w = REDUCE[u]
        cols = pl.ds(o, w)
        arrived(ra2.at[:, cols], f"ra2{u}")
        arrived(rb2.at[:, cols], f"rb2{u}")
        for j, (one, two) in enumerate(((ra, ra2), (rb, rb2))):
            total = (
                grad[rows(q * 192 + 96 * j, 96), cols].astype(f32)
                + one[0, :, cols].astype(f32)
                + two[:, cols].astype(f32)
            )
            for at in range(4):
                zs[j, at, :, cols] = total[24 * at : 24 * at + 24].astype(bf16)
        send(zs.at[:, zn, :, cols], zp.at[:, :, cols], f"zp{u}", (dp, zn))
        far = 2 * (1 - zh)
        send(zs.at[:, pl.ds(far, 2), :, cols], zm.at[:, :, :, cols], f"zm{u}", (dp, zn), when=lambda: outer)

    @scoped
    def s4(u):
        o, w = REDUCE[u]
        cols = pl.ds(o, w)
        far = 2 * (1 - zh)

        @pl.when(inner)
        def _():
            arrived(zm.at[:, :, :, cols], f"zm{u}")
            for j in range(2):
                for at in range(2):
                    zs[j, far + at, :, cols] = (
                        zs[j, far + at, :, cols].astype(f32) + zm[j, at, :, cols].astype(f32)
                    ).astype(bf16)

        for at in range(2):
            send(zs.at[:, far + at, :, cols], zx.at[:, :, cols], f"zx{u}", (dp, far + at), when=lambda: inner)

    @scoped
    def s5(u):
        o, w = REDUCE[u]
        cols = pl.ds(o, w)
        arrived(zp.at[:, :, cols], f"zp{u}")
        arrived(zx.at[:, :, cols], f"zx{u}")
        for j in range(2):
            fin[j, :, cols] = (
                zs[j, z, :, cols].astype(f32) + zp[j, :, cols].astype(f32) + zx[j, :, cols].astype(f32)
            )
        local(fin.at[k, :, cols], gp_out.at[k, :, cols], f"fl{u}")
        send(fin.at[other, :, cols], gp_out.at[k, :, cols], f"fr{u}", (pn, z))

    @scoped
    def s6(u):
        o, w = REDUCE[u]
        cols = pl.ds(o, w)
        arrived(gp_out.at[k, :, cols], f"fl{u}")
        arrived(gp_out.at[other, :, cols], f"fr{u}")

    pl.semaphore_wait(barrier, 9)

    for copy in packing:
        copy.wait()
    seg_send()
    zstage(0)
    zstage(1)
    activation(x_in, xs, "ax", near)
    zstage(2, outer)
    zstage(3, outer)
    slab_in(0)
    xysend(0)
    slab_in(1)
    xysend(1)
    zstage(2, inner)
    zstage(3, inner)
    zstage(4)
    zstage(5)
    activation(x_in, xs, "ax", away)
    slab_in(2, inner)
    slab_in(3, inner)
    arrived(sg, "seg")
    positions = (lax.broadcasted_iota(jnp.int32, (1, 1024), 1) - sg[...]).astype(f32)
    angles = freq[:, 0:1] * positions
    cosr[...] = jnp.cos(angles)
    sinr[...] = jnp.sin(angles)
    starts = sg[...].astype(f32)
    column = jnp.broadcast_to(starts, (128, 1024)).T

    @pl.loop(0, 8)
    def _(i):
        r = lanes(i * 128, 128)
        here = jnp.broadcast_to(sg[:, r].astype(f32), (1024, 128))
        big[:, r] = jnp.where(column == here, 0.0, neg_large)

    diag(0)
    diag(1)
    slab_in(2, outer)
    xysend(2)
    done(0)
    first = land.at[:, pl.ds(0, 128)]
    spare = wm.at[:, pl.ds(512, 128)]

    @pl.when(k == 0)
    def _():
        local(first, spare, "cm")

    @pl.when(k == 1)
    def _():
        local(first, gains, "cg")

    send(first, spare, "cm", (pn, z), when=lambda: k == 0)
    send(first, gains, "cg", (pn, z), when=lambda: k == 1)
    local(land.at[:, pl.ds(128, 384)], wq.at[0], "cq0")
    arrived(gains, "cg")
    gain_rows = gains[...].astype(f32).T
    grow[...] = gain_rows[0:8]
    done(1)
    local(land.at[:, pl.ds(512, 384)], wq.at[1], "cq1")
    local(land.at[:, pl.ds(896, 384)], wq.at[2], "cq2")

    def queries(half):
        for i in range(2):
            at = half * 512 + i * 256
            xb = xs[rows(at, 256), :].astype(f32)
            c = xb - jnp.mean(xb, -1, keepdims=True)
            n = c * lax.rsqrt(jnp.mean(c * c, -1, keepdims=True) + norm_eps)
            h1t[:, lanes(at, 256)] = (n * grow[0:1, :]).astype(bf16).T

        cols = lanes(half * 512, 512)

        @pl.loop(0, 3)
        def _(p):
            t = times(wq[p].T, h1t[:, cols])
            c = cosr[:, cols]
            s = sinr[:, cols]
            for hh in range(4):
                u1 = t[hh * 64 : hh * 64 + 32]
                u2 = t[hh * 64 + 32 : hh * 64 + 64]
                scale = HEAD_DIM**-0.5 if hh < 2 else 1.0
                qk[p, hh * 64 : hh * 64 + 32, cols] = ((u1 * c - u2 * s) * scale).astype(bf16)
                qk[p, hh * 64 + 32 : hh * 64 + 64, cols] = ((u2 * c + u1 * s) * scale).astype(bf16)
            qk[p, 256:384, cols] = t[256:384].astype(bf16)

    share_activation(xs, "ax", k == zh)
    shared_activation(xs, "ax", k != zh)
    for p in range(3):
        arrived(wq.at[p], f"cq{p}")
    slab_in(4, inner)
    slab_in(5, inner)
    slab_in(3, outer)
    xysend(3)
    with scope("qkvnear"):
        queries(zh)
    diag(2)
    slab_in(4, outer)
    xysend(4)
    share_activation(xs, "ax", k != zh)
    shared_activation(xs, "ax", k == zh)
    with scope("qkvfar"):
        queries(1 - zh)
    slab_in(5, outer)
    xysend(5)
    diag(3)

    @scoped
    def weight_done(u):
        done(u)
        o, w = GATHER[u]
        if u == 2:
            pieces = [(land.at[:, pl.ds(o, w)], wa.at[k], None)]
        elif u == 3:
            pieces = [(land.at[:, pl.ds(o, w)], wi.at[k, :, pl.ds(0, 640)], None)]
        elif u == 4:
            pieces = [(land.at[:, pl.ds(o, w)], wi.at[k, :, pl.ds(640, 512)], None)]
        else:
            pieces = [
                (land.at[:, pl.ds(o, w)], wm.at[:, pl.ds(0, 512)], lambda: k == 0),
                (land.at[:, pl.ds(o, w)], wm.at[:, pl.ds(640, 512)], lambda: k == 1),
            ]
        for src, dst, when in pieces:
            if when is None:
                local(src, dst, f"cw{u}")
            else:
                pl.when(when())(lambda src=src, dst=dst: local(src, dst, f"cw{u}") and None)
            send(src, dst, f"pw{u}", (pn, z), when=when)

    @scoped
    def weight_here(u):
        if u == 2:
            mine, theirs = [(wa.at[k], None)], [(wa.at[other], None)]
        elif u == 3:
            mine, theirs = [(wi.at[k, :, pl.ds(0, 640)], None)], [(wi.at[other, :, pl.ds(0, 640)], None)]
        elif u == 4:
            mine, theirs = [(wi.at[k, :, pl.ds(640, 512)], None)], [(wi.at[other, :, pl.ds(640, 512)], None)]
        else:
            low, high = wm.at[:, pl.ds(0, 512)], wm.at[:, pl.ds(640, 512)]
            mine, theirs = [(low, k == 0), (high, k == 1)], [(low, k == 1), (high, k == 0)]
        for group, name in ((mine, "cw"), (theirs, "pw")):
            for ref, when in group:
                if when is None:
                    arrived(ref, f"{name}{u}")
                else:
                    pl.when(when)(lambda ref=ref, name=name: arrived(ref, f"{name}{u}"))

    for h in range(6):
        rsem(f"e{h}")
        rsem(f"o{h}")
    first_send = count["send"]
    count["send"] += 6
    forward_steps = {
        0: lambda: (activation(dy_in, dys, "ay"), diag(4)),
        2: lambda: (weight_done(2), diag(5)),
        3: lambda: weight_done(3),
        4: lambda: (weight_done(4), weight_done(5)),
    }

    @pl.loop(0, 6)
    def _(h):
        p, hh = h // 2, lax.rem(h, 2)
        qrow, krow, vrow = (rows(at + hh * 64, 64) for at in (0, 128, 256))
        orow = rows(k * 384 + h * 64, 64)

        @pl.when(h >= 2)
        def _():
            pltpu.make_async_copy(probs.at[hh], keep.at[h - 2], rs_.at[names["e0"] + 2 * (h - 2)]).wait()

        s = dims(qk[p, krow, :], qk[p, qrow, :], 0, 0) + big[:, 0:1024]
        e = jnp.exp(s - jnp.max(s, 0, keepdims=True))
        r = 1.0 / jnp.sum(e, 0, keepdims=True)
        eb = e.astype(bf16)
        probs[hh] = eb
        otb[orow, :] = (times(qk[p, vrow, :], eb) * r).astype(bf16)
        rl[pl.ds(h, 1), :] = r
        pltpu.make_async_copy(probs.at[hh], keep.at[h], rs_.at[names["e0"] + 2 * h]).start()
        pltpu.make_async_remote_copy(
            src_ref=otb.at[orow, :], dst_ref=otb.at[orow, :], send_sem=sends.at[first_send + h],
            recv_sem=rs_.at[names["o0"] + 2 * h], device_id=(pn, z), device_id_type=MESH,
        ).start()
        for at, step in forward_steps.items():
            pl.when(h == at)(lambda step=step: step() and None)

    for h in range(6):
        drains.append((first_send + h, otb.at[pl.ds(0, 64), :], None))

    for u in range(2, 6):
        weight_here(u)
    arrived(spare, "cm")
    for h in range(6):
        arrived(otb.at[rows(other * 384 + h * 64, 64), :], f"o{h}")
    arrived(probs.at[0], "e4")
    arrived(probs.at[1], "e5")

    mine = rows(k * 512, 512)
    theirs = rows(other * 512, 512)
    my_lanes = lanes(k * 512, 512)
    ot_mine = otb[:, my_lanes]
    x1[:, 0:384] = xs[mine, 0:384].astype(f32) + dims(ot_mine, wa[0], 0, 0)
    x1[:, 384:768] = xs[mine, 384:768].astype(f32) + dims(ot_mine, wa[1], 0, 0)
    xx = x1[...]
    c = xx - jnp.mean(xx, -1, keepdims=True)
    n = c * lax.rsqrt(jnp.mean(c * c, -1, keepdims=True) + norm_eps)
    h2[mine, :] = (n * grow[1:2, :]).astype(bf16)
    send(h2.at[mine, :], h2.at[mine, :], "h2", (pn, z))
    share_activation(dys, "ay")
    for o, w in ((0, 512), (512, 512), (1024, 128)):
        cols = pl.ds(o, w)
        a = times(h2[mine, :], wi[0, :, cols])
        b = times(h2[mine, :], wi[1, :, cols])
        phi = 0.5 * (1.0 + lax.erf(a * 0.7071067811865476))
        gelu = a * phi
        e = times(dys[mine, :], wm[:, cols])
        hid[:, cols] = (gelu * b).astype(bf16)
        dgo[0, :, cols] = (e * (b * (phi + a * (jnp.exp(-0.5 * a * a) * 0.3989422804014327)))).astype(bf16)
        dgo[1, :, cols] = (e * gelu).astype(bf16)
    send(hid.at[:, lanes(other * 512, 640)], hidp, "hid", (pn, z))
    send(dgo.at[other], dgp, "dg", (pn, z))

    lo[...] = (x1[...] + dims(hid[...], wm[...], 1, 1)).astype(bf16)
    give_back(lo, lo_out, "alo")
    shared_activation(dys, "ay")
    arrived(hidp, "hid")
    t = (
        dims(dys[mine, :], hid[:, lanes(k * 512, 640)], 0, 0) + dims(dys[theirs, :], hidp[...], 0, 0)
    ).astype(bf16)

    @pl.when(k == 0)
    def _():
        grad[:, MLP : MLP + 512] = t[:, 0:512]
        grad[:, 0:128] = t[:, 512:640]

    @pl.when(k == 1)
    def _():
        grad[:, MLP : MLP + 512] = t[:, 128:640]

    s1("m")
    arrived(h2.at[theirs, :], "h2")
    arrived(dgp, "dg")
    for name, o, w in (("i0", 0, 640), ("i1", 640, 512)):
        cols = pl.ds(o, w)
        grad[:, IN + o : IN + o + w] = (
            dims(h2[mine, :], dgo[k, :, cols], 0, 0) + dims(h2[theirs, :], dgp[:, cols], 0, 0)
        ).astype(bf16)
        if name == "i0":
            s1(name)
    f2 = dims(dgo[0], wi[0], 1, 1) + dims(dgo[1], wi[1], 1, 1)
    xx = x1[...]
    c = xx - jnp.mean(xx, -1, keepdims=True)
    r2 = lax.rsqrt(jnp.mean(c * c, -1, keepdims=True) + norm_eps)
    n = c * r2
    grow[3:4, :] = jnp.sum(f2 * n, 0, keepdims=True)
    cc = f2 * grow[1:2, :]
    dx = dys[mine, :].astype(f32) + r2 * (
        cc - jnp.mean(cc, -1, keepdims=True) - n * jnp.mean(cc * n, -1, keepdims=True)
    )
    x1[...] = dx
    dx1b[...] = dx.astype(bf16)
    send(dx1b.at[:, lanes(other * 384, 384)], dx1bp, "dx1b", (pn, z))
    for part in range(2):
        which = other if part == 0 else k
        col = lanes(which * 384, 384)
        feat = rows(which * 384, 384)
        left = jnp.concatenate([wa[0, feat, :], wa[1, feat, :]], axis=1)
        t = dims(left, dx1b[...], 1, 1).astype(bf16)
        if part == 0:
            dot_send[...] = t
            send(dot_send, dot_own.at[:, my_lanes], "do", (pn, z))
        else:
            dot_own[:, my_lanes] = t
    local(keep.at[5], probs.at[1], "e5")
    local(keep.at[4], probs.at[0], "e4")

    s2("m")
    s1("i1")
    arrived(dx1bp, "dx1b")
    grad[:, ATTN : ATTN + 384] = (
        times(otb[:, my_lanes], dx1b[:, lanes(k * 384, 384)])
        + times(otb[:, lanes(other * 512, 512)], dx1bp[...])
    ).astype(bf16)
    arrived(dot_own.at[:, lanes(other * 512, 512)], "do")

    for h in range(6):
        rsem(f"b{h}")
    backward_steps = {
        4: lambda: (s2("i0"), s3("m")),
        3: lambda: (s2("i1"), s1("a"), s1("q2")),
        2: lambda: (s3("i0"), s4("m")),
        1: lambda: s3("i1"),
        0: lambda: (s2("a"), s4("i0")),
    }

    @pl.loop(0, 6)
    def _(turn):
        h = 5 - turn
        p, hh = h // 2, lax.rem(h, 2)
        qrow, krow, vrow = (rows(at + hh * 64, 64) for at in (0, 128, 256))
        arrived_at = rs_.at[names["e0"] + 2 * h]
        pltpu.make_async_copy(keep.at[h], probs.at[hh], arrived_at).wait()
        vt = qk[p, vrow, :]
        kt = qk[p, krow, :]
        for i in range(2):
            cols = slice(i * 512, i * 512 + 512)
            do = dot_own[rows(h * 64, 64), cols].astype(f32) * rl[pl.ds(h, 1), cols]
            delta = jnp.sum(do * otb[rows(k * 384 + h * 64, 64), cols].astype(f32), 0, keepdims=True)
            dob = do.astype(bf16)
            e = probs[hh, :, cols]
            ds = (e.astype(f32) * (dims(vt, dob, 0, 0) - delta)).astype(bf16)
            dk = dims(qk[p, qrow, cols], ds, 1, 1)
            dv = dims(dob, e, 1, 1)
            if i == 0:
                dkb[...] = dk
                dvb[...] = dv
            else:
                dkb[...] += dk
                dvb[...] += dv
            dq = times(kt, ds) * HEAD_DIM**-0.5
            c = cosr[:, cols]
            s = sinr[:, cols]
            qk[p, rows(hh * 64, 32), cols] = (dq[:32] * c + dq[32:] * s).astype(bf16)
            qk[p, rows(hh * 64 + 32, 32), cols] = (dq[32:] * c - dq[:32] * s).astype(bf16)

        @pl.when(h >= 2)
        def _():
            pltpu.make_async_copy(keep.at[h - 2], probs.at[hh], rs_.at[names["e0"] + 2 * (h - 2)]).start()

        d = dkb[...]
        c = cosr[...]
        s = sinr[...]
        qk[p, rows(128 + hh * 64, 32), :] = (d[:32] * c + d[32:] * s).astype(bf16)
        qk[p, rows(160 + hh * 64, 32), :] = (d[32:] * c - d[:32] * s).astype(bf16)
        qk[p, vrow, :] = dvb[...].astype(bf16)

        @pl.when(h == 4)
        def _():
            grad[:, lanes(PAIR + 384 * p, 384)] = dims(h1t[...], qk[p], 1, 1).astype(bf16)

        for at, step in backward_steps.items():
            pl.when(h == at)(lambda step=step: step() and None)

    def f1_part(cols):
        return times(wq[0], qk[0, :, cols]) + times(wq[1], qk[1, :, cols]) + times(wq[2], qk[2, :, cols])

    big[0:768, 0:512] = f1_part(lanes(other * 512, 512))
    send(big.at[pl.ds(0, 768), pl.ds(0, 512)], f1r, "f1", (pn, z))
    big[0:768, 512:1024] = f1_part(my_lanes)
    s2("q2")
    s4("i1")
    arrived(f1r, "f1")
    f1 = (big[0:768, 512:1024] + f1r[...]).T
    xx = xs[mine, :].astype(f32)
    c = xx - jnp.mean(xx, -1, keepdims=True)
    r1 = lax.rsqrt(jnp.mean(c * c, -1, keepdims=True) + norm_eps)
    n = c * r1
    grow[2:3, :] = jnp.sum(f1 * n, 0, keepdims=True)
    cc = f1 * grow[0:1, :]
    gi[...] = (
        x1[...] + r1 * (cc - jnp.mean(cc, -1, keepdims=True) - n * jnp.mean(cc * n, -1, keepdims=True))
    ).astype(bf16)
    send(grow, growp, "gr", (pn, z), when=lambda: k == 0)

    @pl.when(k == 1)
    def _():
        arrived(growp, "gr")
        two = jnp.concatenate([grow[2:4, :] + growp[2:4, :], jnp.zeros((126, 768), f32)], axis=0)
        grad[:, 0:128] = two.T.astype(bf16)

    s1("g")
    give_back(gi, gi_out, "agi", (0,))
    give_back(gi, gi_out, "agi", (1,), inner)
    for p in (1, 0):
        grad[:, PAIR + 384 * p : PAIR + 384 * p + 384] = dims(h1t[...], qk[p], 1, 1).astype(bf16)
        s1(f"q{p}")
        if p == 1:
            s3("a")
    s3("q2")
    s5("m")
    s4("a")
    s2("q1")
    s2("g")
    s4("q2")
    s5("i0")
    s2("q0")
    s5("i1")
    s3("q1")
    s3("g")
    s3("q0")
    give_back(gi, gi_out, "agi", (1,), outer)
    s5("a")
    s4("q1")
    s4("g")
    s4("q0")
    s5("q2")
    s5("q1")
    s5("g")
    s5("q0")
    for u in REDUCE:
        s6(u)
    given_back(lo_out, "alo")
    given_back(gi_out, "agi")
    drain_all()
    assert len(names) <= 160 and count["send"] <= 220 and len(packing) + len(small) <= 32


frequency = np.broadcast_to(
    (np.float32(rope_base) ** (-(np.arange(32, dtype=np.float32) * 2) / HEAD_DIM))[:, None], (32, 128)
).astype(np.float32)


def finish_kernel(
    lo_raw, gi_raw, gp_raw, lo, gi, o_qkv, o_attn, o_in, o_mlp, o_one, o_two,
    buf, gp, g_qkv, g_attn, g_in, g_mlp, g_one, g_two, sem,
):
    loads = [
        pltpu.make_async_copy(src, dst, sem.at[i])
        for i, (src, dst) in enumerate(((gp_raw, gp), (lo_raw, buf.at[0]), (gi_raw, buf.at[1])))
    ]
    for copy in loads:
        copy.start()
    pairs = ((buf.at[0], lo), (buf.at[1], gi), (g_qkv, o_qkv), (g_attn, o_attn), (g_in, o_in), (g_mlp, o_mlp), (g_one, o_one), (g_two, o_two))
    stores = [pltpu.make_async_copy(src, dst, sem.at[3 + i]) for i, (src, dst) in enumerate(pairs)]
    loads[0].wait()
    for c in range(2):
        for p in range(3):
            for t in range(3):
                o = 768 * t + 384 * c + 128 * p
                at = PAIR + 384 * p + 128 * t
                g_qkv[:, o : o + 128] = gp[c, :, at : at + 128]
        g_attn[:, 384 * c : 384 * c + 384] = gp[c, :, ATTN : ATTN + 384]
        g_in[:, 1152 * c : 1152 * c + 1152] = gp[c, :, IN : IN + 1152]
    g_mlp[:, 0:512] = gp[0, :, MLP : MLP + 512]
    g_mlp[:, 512:640] = gp[0, :, 0:128]
    g_mlp[:, 640:1152] = gp[1, :, MLP : MLP + 512]
    flat = jnp.concatenate([gp[1, :, 0:128], jnp.zeros((104, 128), f32)], axis=0).T
    g_one[...] = flat[0:1, 0:24]
    g_two[...] = flat[1:2, 0:24]
    for load, store in zip(loads[1:], stores[:2]):
        load.wait()
        store.start()
    for store in stores[2:]:
        store.start()
    for store in stores:
        store.wait()


def fast(layer_in, seg_start, out_grad, w_qkv, w_attn_out, w_in, w_mlp_out, norm_attn, norm_mlp):
    hbm = pl.BlockSpec(memory_space=pltpu.HBM)
    V = pltpu.VMEM
    outs = pl.pallas_call(
        step_kernel,
        name="layer",
        out_shape=[
            jax.ShapeDtypeStruct((2, 256, 768), bf16),
            jax.ShapeDtypeStruct((2, 256, 768), bf16),
            jax.ShapeDtypeStruct((2, 24, WIDTH), f32),
            jax.ShapeDtypeStruct((768, WIDTH), bf16),
            jax.ShapeDtypeStruct((6, 1024, 1024), bf16),
        ],
        in_specs=[hbm] * 10,
        out_specs=[hbm] * 5,
        scratch_shapes=[
            V((2, 24, WIDTH), bf16),
            V((8, 128), f32),
            V((2, 256), jnp.int32),
            V((1, 24), bf16),
            V((1, 24), bf16),
            V((32, 128), f32),
            V((1024, 768), bf16),
            V((1024, 768), bf16),
            V((1, 1024), jnp.int32),
            V((768, 1024), bf16),
            V((3, 768, 384), bf16),
            V((2, 768, 384), bf16),
            V((2, 768, 1152), bf16),
            V((768, 1152), bf16),
            V((768, 128), bf16),
            V((32, 1024), f32),
            V((32, 1024), f32),
            V((3, 384, 1024), bf16),
            V((1024, 1152), f32),
            V((2, 1024, 1024), bf16),
            V((768, 1024), bf16),
            V((8, 1024), f32),
            V((512, 768), f32),
            V((1024, 768), bf16),
            V((512, 1152), bf16),
            V((512, 640), bf16),
            V((2, 512, 1152), bf16),
            V((512, 1152), bf16),
            V((512, 768), bf16),
            V((512, 384), bf16),
            V((384, 512), bf16),
            V((384, 1024), bf16),
            V((768, 512), f32),
            V((512, 768), bf16),
            V((512, 768), bf16),
            V((768, WIDTH), bf16),
            V((8, 768), f32),
            V((8, 768), f32),
            V((64, 1024), f32),
            V((64, 1024), f32),
            V((2, 96, WIDTH), bf16),
            V((2, 96, WIDTH), bf16),
            V((96, WIDTH), bf16),
            V((96, WIDTH), bf16),
            V((2, 4, 24, WIDTH), bf16),
            V((2, 24, WIDTH), bf16),
            V((2, 2, 24, WIDTH), bf16),
            V((2, 24, WIDTH), bf16),
            V((2, 24, WIDTH), f32),
            pltpu.SemaphoreType.DMA((160,)),
            pltpu.SemaphoreType.DMA((32,)),
            pltpu.SemaphoreType.DMA((220,)),
        ],
        compiler_params=pltpu.CompilerParams(
            collective_id=0, has_side_effects=True, vmem_limit_bytes=67043328
        ),
    )(
        layer_in, out_grad, seg_start, w_qkv, w_attn_out, w_in, w_mlp_out,
        norm_attn[None], norm_mlp[None], frequency,
    )
    done = pl.pallas_call(
        finish_kernel,
        name="finish",
        out_shape=[
            jax.ShapeDtypeStruct((2, 256, 768), bf16),
            jax.ShapeDtypeStruct((2, 256, 768), bf16),
            jax.ShapeDtypeStruct((24, 2304), f32),
            jax.ShapeDtypeStruct((24, 768), f32),
            jax.ShapeDtypeStruct((24, 2304), f32),
            jax.ShapeDtypeStruct((24, 1152), f32),
            jax.ShapeDtypeStruct((1, 24), f32),
            jax.ShapeDtypeStruct((1, 24), f32),
        ],
        in_specs=[hbm, hbm, hbm],
        out_specs=[hbm] * 8,
        scratch_shapes=[
            V((2, 2, 256, 768), bf16),
            V((2, 24, WIDTH), f32),
            V((24, 2304), f32),
            V((24, 768), f32),
            V((24, 2304), f32),
            V((24, 1152), f32),
            V((1, 24), f32),
            V((1, 24), f32),
            pltpu.SemaphoreType.DMA((11,)),
        ],
    )(*outs[:3])
    return (*done[:6], done[6][0], done[7][0])


def normalize(values):
    centered = values - jnp.mean(values, axis=-1, keepdims=True)
    spread = jnp.mean(centered * centered, axis=-1, keepdims=True)
    return centered * lax.rsqrt(spread + norm_eps)


def rope_tables(positions):
    half_dim = HEAD_DIM // 2
    frequency = rope_base ** (-(jnp.arange(half_dim).astype(jnp.float32) * 2.0) / HEAD_DIM)
    angles = positions.astype(jnp.float32)[:, None] * frequency[None, :]
    angles = jnp.concatenate([angles, angles], axis=-1)
    return (jnp.cos(angles), jnp.sin(angles))


def turn_half(values):
    half_dim = values.shape[-1] // 2
    return jnp.concatenate([-values[..., half_dim:], values[..., :half_dim]], axis=-1)


def rotate(values, cosine_table, sine_table):
    return values * cosine_table[:, None, :] + turn_half(values) * sine_table[:, None, :]


def unrotate(values, cosine_table, sine_table):
    return values * cosine_table[:, None, :] - turn_half(values) * sine_table[:, None, :]


def product(left, right):
    return jnp.dot(left, right, preferred_element_type=jnp.float32)


def left_transposed(left, right):
    return lax.dot_general(
        left, right, (((0,), (0,)), ((), ())), preferred_element_type=jnp.float32
    )


def right_transposed(left, right):
    return lax.dot_general(
        left, right, (((1,), (1,)), ((), ())), preferred_element_type=jnp.float32
    )


def to_groups(array):
    row_count, head_count, head_size = array.shape
    return array.reshape(row_count, head_count // 4, 4, head_size).transpose(1, 0, 2, 3)


def from_groups(array):
    group_count, row_count, group_heads, head_size = array.shape
    return array.transpose(1, 0, 2, 3).reshape(row_count, group_count * group_heads, head_size)


def attend_group(group_in, same_doc):
    query_part, key_part, value_part = group_in
    scores = jnp.einsum(
        "qhd,khd->hqk", query_part, key_part, preferred_element_type=jnp.float32
    ) * HEAD_DIM ** (-0.5)
    masked = jnp.where(same_doc[None], scores, neg_large)
    highest = jnp.max(masked, axis=-1, keepdims=True)
    shifted = jnp.exp(masked - highest)
    totals = jnp.sum(shifted, axis=-1, keepdims=True)
    attn_prob = shifted / totals
    log_total = highest + jnp.log(totals)
    mixed_out = jnp.einsum(
        "hqk,khd->qhd",
        attn_prob.astype(jnp.bfloat16),
        value_part,
        preferred_element_type=jnp.float32,
    )
    return (mixed_out, log_total[..., 0])


def attend_back(group_in, same_doc):
    query_part, key_part, value_part, grad_part, log_total = group_in
    scores = jnp.einsum(
        "qhd,khd->hqk", query_part, key_part, preferred_element_type=jnp.float32
    ) * HEAD_DIM ** (-0.5)
    attn_prob = jnp.where(same_doc[None], jnp.exp(scores - log_total[..., None]), 0.0)
    grad_prob = jnp.einsum(
        "qhd,khd->hqk", grad_part, value_part, preferred_element_type=jnp.float32
    )
    inner_sum = jnp.sum(attn_prob * grad_prob, axis=-1, keepdims=True)
    grad_score = (attn_prob * (grad_prob - inner_sum)).astype(jnp.bfloat16)
    grad_query = jnp.einsum(
        "hqk,khd->qhd", grad_score, key_part, preferred_element_type=jnp.float32
    ) * HEAD_DIM ** (-0.5)
    grad_key = jnp.einsum(
        "hqk,qhd->khd", grad_score, query_part, preferred_element_type=jnp.float32
    ) * HEAD_DIM ** (-0.5)
    grad_value = jnp.einsum(
        "hqk,qhd->khd",
        attn_prob.astype(jnp.bfloat16),
        grad_part,
        preferred_element_type=jnp.float32,
    )
    return (grad_query, grad_key, grad_value)


def scaled_norm(values_in, gain_row):
    return normalize(values_in) * gain_row


def geglu(first_half, second_half):
    return jax.nn.gelu(first_half, approximate=False) * second_half


def local(layer_in, seg_start, out_grad, w_qkv, w_attn_out, w_in, w_mlp_out, norm_attn, norm_mlp):
    micro_count = layer_in.shape[0]
    span_len = layer_in.shape[1]
    model_width = layer_in.shape[2]
    ctx_rank = lax.axis_index("ctx")
    grad_sums = (
        jnp.zeros((model_width, 3 * model_width), jnp.float32),
        jnp.zeros((model_width, model_width), jnp.float32),
        jnp.zeros((model_width, 2 * FF), jnp.float32),
        jnp.zeros((model_width, FF), jnp.float32),
        jnp.zeros((model_width,), jnp.float32),
        jnp.zeros((model_width,), jnp.float32),
    )
    offsets = ctx_rank * span_len + jnp.arange(span_len, dtype=jnp.int32)
    outputs = []
    grad_inputs = []
    for micro_step in range(micro_count):
        gathered = (
            lax.all_gather(w_qkv, ("dp", "ctx"), axis=0, tiled=True),
            lax.all_gather(w_attn_out, ("dp", "ctx"), axis=0, tiled=True),
            lax.all_gather(w_in, ("dp", "ctx"), axis=0, tiled=True),
            lax.all_gather(w_mlp_out, ("dp", "ctx"), axis=0, tiled=True),
            lax.all_gather(norm_attn, ("dp", "ctx"), axis=0, tiled=True),
            lax.all_gather(norm_mlp, ("dp", "ctx"), axis=0, tiled=True),
        )
        qkv_full, attn_full, in_full, mlp_full, gain_attn, gain_mlp = gathered
        starts_here = seg_start[micro_step]
        hidden = layer_in[micro_step].astype(jnp.float32)
        cosine_table, sine_table = rope_tables(offsets - starts_here)
        normed, norm_back = jax.vjp(scaled_norm, hidden, gain_attn.astype(jnp.float32))
        normed_low = normed.astype(jnp.bfloat16)
        qkv_local = product(normed_low, qkv_full).reshape(span_len, 3, HEADS, HEAD_DIM)
        queries = rotate(qkv_local[:, 0], cosine_table, sine_table).astype(jnp.bfloat16)
        keys_here = rotate(qkv_local[:, 1], cosine_table, sine_table).astype(jnp.bfloat16)
        values_here = qkv_local[:, 2].astype(jnp.bfloat16)
        keys_all, values_all, starts_all = (
            lax.all_gather(keys_here, "ctx", axis=0, tiled=True),
            lax.all_gather(values_here, "ctx", axis=0, tiled=True),
            lax.all_gather(starts_here, "ctx", axis=0, tiled=True),
        )
        same_doc = starts_here[:, None] == starts_all[None, :]
        query_groups = to_groups(queries)
        key_groups = to_groups(keys_all)
        value_groups = to_groups(values_all)
        mixed_out, log_total = lax.map(
            lambda group_in: attend_group(group_in, same_doc),
            (query_groups, key_groups, value_groups),
        )
        attended = from_groups(mixed_out).reshape(span_len, model_width).astype(jnp.bfloat16)
        middle = hidden + product(attended, attn_full)
        normed_mlp, norm_mlp_back = jax.vjp(scaled_norm, middle, gain_mlp.astype(jnp.float32))
        normed_mlp_low = normed_mlp.astype(jnp.bfloat16)
        projected = product(normed_mlp_low, in_full)
        gated_out, geglu_back = jax.vjp(geglu, projected[:, :FF], projected[:, FF:])
        gated_low = gated_out.astype(jnp.bfloat16)
        result = middle + right_transposed(gated_low, mlp_full)
        outputs.append(result.astype(jnp.bfloat16))
        qkv_full, attn_full, in_full, mlp_full = (
            lax.all_gather(w_qkv, ("dp", "ctx"), axis=0, tiled=True),
            lax.all_gather(w_attn_out, ("dp", "ctx"), axis=0, tiled=True),
            lax.all_gather(w_in, ("dp", "ctx"), axis=0, tiled=True),
            lax.all_gather(w_mlp_out, ("dp", "ctx"), axis=0, tiled=True),
        )
        grad_out = out_grad[micro_step].astype(jnp.float32)
        grad_out_low = out_grad[micro_step]
        grad_mlp_weight = left_transposed(grad_out_low, gated_low)
        grad_gated = product(grad_out_low, mlp_full)
        grad_first, grad_second = geglu_back(grad_gated)
        grad_projected = jnp.concatenate([grad_first, grad_second], axis=1).astype(jnp.bfloat16)
        grad_in_weight = left_transposed(normed_mlp_low, grad_projected)
        grad_normed_mlp = right_transposed(grad_projected, in_full)
        grad_middle_norm, grad_gain_mlp = norm_mlp_back(grad_normed_mlp)
        grad_middle = grad_out + grad_middle_norm
        grad_middle_low = grad_middle.astype(jnp.bfloat16)
        grad_attn_weight = left_transposed(attended, grad_middle_low)
        grad_attended = (
            right_transposed(grad_middle_low, attn_full)
            .astype(jnp.bfloat16)
            .reshape(span_len, HEADS, HEAD_DIM)
        )
        grad_groups = to_groups(grad_attended)
        grad_query_groups, grad_key_groups, grad_value_groups = lax.map(
            lambda group_in: attend_back(group_in, same_doc),
            (query_groups, key_groups, value_groups, grad_groups, log_total),
        )
        keys_total = keys_all.shape[0]
        grad_keys, grad_values = (
            lax.psum_scatter(
                from_groups(grad_key_groups).reshape(keys_total, model_width).astype(jnp.bfloat16),
                "ctx",
                scatter_dimension=0,
                tiled=True,
            ).astype(jnp.float32),
            lax.psum_scatter(
                from_groups(grad_value_groups)
                .reshape(keys_total, model_width)
                .astype(jnp.bfloat16),
                "ctx",
                scatter_dimension=0,
                tiled=True,
            ).astype(jnp.float32),
        )
        grad_qkv = jnp.stack(
            [
                unrotate(from_groups(grad_query_groups), cosine_table, sine_table),
                unrotate(grad_keys.reshape(span_len, HEADS, HEAD_DIM), cosine_table, sine_table),
                grad_values.reshape(span_len, HEADS, HEAD_DIM),
            ],
            axis=1,
        )
        grad_qkv = grad_qkv.reshape(span_len, 3 * model_width).astype(jnp.bfloat16)
        grad_qkv_weight = left_transposed(normed_low, grad_qkv)
        grad_normed = right_transposed(grad_qkv, qkv_full)
        grad_hidden_norm, grad_gain_attn = norm_back(grad_normed)
        grad_inputs.append((grad_middle + grad_hidden_norm).astype(jnp.bfloat16))
        grad_sums = (
            grad_sums[0] + grad_qkv_weight,
            grad_sums[1] + grad_attn_weight,
            grad_sums[2] + grad_in_weight,
            grad_sums[3] + grad_mlp_weight,
            grad_sums[4] + grad_gain_attn,
            grad_sums[5] + grad_gain_mlp,
        )
    shares = (
        lax.psum_scatter(grad_sums[0], ("dp", "ctx"), scatter_dimension=0, tiled=True),
        lax.psum_scatter(grad_sums[1], ("dp", "ctx"), scatter_dimension=0, tiled=True),
        lax.psum_scatter(grad_sums[2], ("dp", "ctx"), scatter_dimension=0, tiled=True),
        lax.psum_scatter(grad_sums[3], ("dp", "ctx"), scatter_dimension=0, tiled=True),
        lax.psum_scatter(grad_sums[4], ("dp", "ctx"), scatter_dimension=0, tiled=True),
        lax.psum_scatter(grad_sums[5], ("dp", "ctx"), scatter_dimension=0, tiled=True),
    )
    return (
        jnp.stack(outputs),
        jnp.stack(grad_inputs),
        shares[0],
        shares[1],
        shares[2],
        shares[3],
        shares[4],
        shares[5],
    )


def solution(mesh):
    A = P(None, ("dp", "ctx"), None)
    S = P(None, ("dp", "ctx"))
    W = P(("dp", "ctx"), None)
    G = P(("dp", "ctx"))
    return jax.shard_map(
        fast if dict(mesh.shape) == {"dp": 8, "ctx": 4} else local,
        mesh=mesh,
        in_specs=(A, S, A, W, W, W, W, G, G),
        out_specs=(A, A, W, W, W, W, G, G),
        check_vma=False,
    )
```
